512 devices in a mesh: member: 2 (over y), gx: 16 (over x, core), gy: 16 (over z).
Axes of the slice: x: 8, y: 2, z: 16, core: 2. Of those that a mesh axis runs over, the one named last changes fastest.
The devices are a block of a 8x8x16 slice.
Arguments:
- perm: float32 [64, 128, 2048], P('member', 'gx', 'gy'), parts along dimension 0, may hold values from 0.2 to 5
- facies: int32 [64, 128, 2048], P('member', 'gx', 'gy'), parts along dimension 0, may hold values from 0 to 3
- facies_porosity: float32 [4], replicated, may hold values from 0.15 to 0.35
- facies_mobility: float32 [4], replicated, may hold values from 0.5 to 2
- pressure: float32 [64, 128, 2048], P('member', 'gx', 'gy'), parts along dimension 0, may hold values from -6 to 6
- saturation: float32 [64, 128, 2048], P('member', 'gx', 'gy'), parts along dimension 0, may hold values from 0.1 to 0.9
- basis: float32 [64, 128, 2048], P('member', 'gx', 'gy'), parts along dimension 0, may hold values from 0.75 to 1.33
- bx_map: int32 [256], P('member'), parts along dimension 0, may hold values from 0 to 15, as said below
- by_map: int32 [4096], P('member'), parts along dimension 0, may hold values from 0 to 255, as said below
- well_cells: int32 [1024], P('member'), parts along dimension 0, may hold values from 0 to 262143
- well_rates: float32 [1024], P('member'), parts along dimension 0, may hold values from -384 to 384
Outputs:
- new_pressure: float32 [64, 128, 2048], P('member', 'gx', 'gy'), parts along dimension 0
- new_saturation: float32 [64, 128, 2048], P('member', 'gx', 'gy'), parts along dimension 0
The draws below stay inside these ranges and needn't reach their ends.
There are 2 independent parts, one for each index of `member`. The reference program is written for one: setup_inputs(seed, part) draws one part's arguments, and reference() takes and returns one part's arrays. A program takes and returns all parts, laid end to end along the dimension named above; an argument that names none is the same for every part. Nothing has to cross between parts.
Inputs may be any that keep to these rules, and one draw needn't show every extreme that they name: `bx_map`: never falling; block 0 begins at position 0 and block k >= 1 begins at position 8 k + d with -2 <= d <= 2. `by_map`: never falling; block 0 begins at position 0 and block k >= 1 begins at position 8 k + d with -2 <= d <= 2.
All inputs are finite; a program needn't handle non-finite values.
Results may differ from the reference program's by a relative error of at most 0.0003.
Values sent between devices are 32-bit elements; how exact they have to be, the bound alone decides.
A program may use at most 64 MiB of HBM per device.

```python
import math
import jax
import jax.numpy as jnp
from jax import lax

NZ = 32
BX = 8
BY = 8
BZ = 4
JIT = 2
NSWEEP = 3
NSUB = 4
NFAC = 4
NX = 128
NY = 2048
NBX = 16
NBY = 256
NBZ = 8
WELLS = 512


def block_index(key, cells, blocks, length):
    shifts = jax.random.randint(key, (blocks - 1,), -JIT, JIT + 1, dtype=jnp.int32)
    starts = length * jnp.arange(1, blocks, dtype=jnp.int32) + shifts
    places = jnp.arange(cells, dtype=jnp.int32)
    return jnp.sum((places[:, None] >= starts[None, :]).astype(jnp.int32), axis=1).astype(jnp.int32)


def draw_bx_map(key, part):
    return block_index(jax.random.fold_in(key, 17), NX, NBX, BX)


def draw_by_map(key, part):
    return block_index(jax.random.fold_in(key, 29), NY, NBY, BY)


def place_ends(result, key, least, high):
    spot = [jax.random.randint(jax.random.fold_in(key, axis), (), 0, length) for axis, length in enumerate(result.shape)]
    widest = result.shape.index(max(result.shape))
    beside = spot[:widest] + [(spot[widest] + 1) % result.shape[widest]] + spot[widest + 1:]
    return result.at[tuple(spot)].set(least).at[tuple(beside)].set(high)


def level_of(rng, shape, split, least, largest):
    loudness = 1.0
    for dim, parts in split:
        heights = jax.random.uniform(jax.random.fold_in(jax.random.fold_in(rng, 6), dim), (parts,), jnp.float32, least / len(split), largest / len(split))
        loudness = loudness * jnp.repeat(jnp.exp(heights), shape[dim] // parts).reshape((-1,) + (1,) * (len(shape) - 1 - dim))
    return loudness


def scatter_about(key, dims, deviation, reach, shards=(), kind=jnp.bfloat16):
    factor_of = level_of(key, dims, shards, -0.22, 0.18) if shards else 1.0
    values = jax.random.normal(key, dims, jnp.float32) * deviation * factor_of
    return jnp.minimum(jnp.maximum(values, -reach), reach).astype(kind)


def setup_inputs(seed: int = 0, part: int = 0) -> dict:
    arg_keys = jax.random.split(jax.random.key(seed), 12)
    part_splits = jax.random.split(jax.random.fold_in(arg_keys[11], part), 12)
    return {
        "perm": jnp.clip(jnp.exp(math.log(5.0) - 3.218876 * jax.random.uniform(part_splits[0], (NZ, NX, NY), jnp.float32) ** level_of(part_splits[0], (NZ, NX, NY), ((1, 16), (2, 16)), -0.2, 0.2)), 0.2, 5.0),
        "facies": place_ends(jax.random.randint(part_splits[1], (NZ, NX, NY), 0, NFAC), jax.random.fold_in(part_splits[1], 1), 0, NFAC - 1).astype(jnp.int32),
        "facies_porosity": jnp.clip(jax.random.uniform(arg_keys[2], (NFAC,), jnp.float32, 0.15, 0.35), 0.15, 0.35),
        "facies_mobility": jnp.clip(jnp.exp(jax.random.uniform(arg_keys[3], (NFAC,), jnp.float32, math.log(0.5), math.log(2.0))), 0.5, 2.0),
        "pressure": scatter_about(part_splits[4], (NZ, NX, NY), 1.0, 6.0, ((1, 16), (2, 16)), jnp.float32),
        "saturation": jnp.clip(0.1 + 0.79999997 * jax.random.uniform(part_splits[5], (NZ, NX, NY), jnp.float32) ** level_of(part_splits[5], (NZ, NX, NY), ((1, 16), (2, 16)), -0.2, 0.2), 0.1, 0.9),
        "basis": jnp.clip(jnp.exp(math.log(1.33) - 0.57286105 * jax.random.uniform(part_splits[6], (NZ, NX, NY), jnp.float32) ** level_of(part_splits[6], (NZ, NX, NY), ((1, 16), (2, 16)), -0.2, 0.2)), 0.75, 1.33),
        "bx_map": draw_bx_map(jax.random.fold_in(jax.random.fold_in(arg_keys[11], part), 71), part),
        "by_map": draw_by_map(jax.random.fold_in(jax.random.fold_in(arg_keys[11], part), 71), part),
        "well_cells": place_ends(jax.random.randint(part_splits[9], (WELLS,), 0, NX * NY), jax.random.fold_in(part_splits[9], 1), 0, (NX * NY) - 1).astype(jnp.int32),
        "well_rates": scatter_about(part_splits[10], (WELLS,), (2 * NZ), 384.0, (), jnp.float32),
    }


viscosity_ratio = 4.0
vertical_factor = 0.1
storage_coefficient = 0.5
relaxation = 0.5
time_step = 0.005
highest = lax.Precision.HIGHEST


def lower(field, axis):
    return lax.slice_in_dim(field, 0, field.shape[axis] - 1, axis=axis)


def upper(field, axis):
    return lax.slice_in_dim(field, 1, field.shape[axis], axis=axis)


def pad_after(field, axis):
    widths = [(0, 1) if position == axis else (0, 0) for position in range(field.ndim)]
    return jnp.pad(field, widths)


def pad_before(field, axis):
    widths = [(1, 0) if position == axis else (0, 0) for position in range(field.ndim)]
    return jnp.pad(field, widths)


def harmonic(left, right):
    total = left + right
    return 2.0 * left * right / jnp.where(total > 0, total, 1.0)


def total_mobility(water_saturation):
    return water_saturation * water_saturation + (1.0 - water_saturation) * (1.0 - water_saturation) / viscosity_ratio


def fractional(water_saturation):
    wet = water_saturation * water_saturation
    return wet / (wet + (1.0 - water_saturation) * (1.0 - water_saturation) / viscosity_ratio)


def transmissibilities(mobility):
    return tuple((vertical_factor if axis == 0 else 1.0) * harmonic(lower(mobility, axis), upper(mobility, axis)) for axis in range(3))


def outflow(flows):
    total = 0.0
    for axis in range(3):
        total = total + pad_after(flows[axis], axis) - pad_before(flows[axis], axis)
    return total


def reference(perm, facies, facies_porosity, facies_mobility, pressure, saturation, basis, bx_map, by_map, well_cells, well_rates):
    porosity = facies_porosity[facies]
    mobility = perm * facies_mobility[facies] * total_mobility(saturation)
    trans = transmissibilities(mobility)
    column = jnp.zeros((NX * NY,), jnp.float32).at[well_cells].add(well_rates)
    source = jnp.broadcast_to((column / NZ).reshape(1, NX, NY), (NZ, NX, NY))
    pushes = tuple(trans[axis] * (lower(pressure, axis) - upper(pressure, axis)) for axis in range(3))
    residual = source - outflow(pushes)
    conductance = 0.0
    for axis in range(3):
        conductance = conductance + pad_after(trans[axis], axis) + pad_before(trans[axis], axis)
    cell_diagonal = basis * basis * (storage_coefficient * porosity + conductance)
    layer_blocks = jnp.arange(NZ, dtype=jnp.int32) // BZ
    same = ((layer_blocks[:-1] == layer_blocks[1:]).astype(jnp.float32).reshape(NZ - 1, 1, 1),
            (bx_map[:-1] == bx_map[1:]).astype(jnp.float32).reshape(1, NX - 1, 1),
            (by_map[:-1] == by_map[1:]).astype(jnp.float32).reshape(1, 1, NY - 1))
    couple = tuple(trans[axis] * lower(basis, axis) * upper(basis, axis) for axis in range(3))
    inner = 0.0
    for axis in range(3):
        inner = inner + pad_after(couple[axis] * same[axis], axis)
    onehot_x = (bx_map[:, None] == jnp.arange(NBX, dtype=jnp.int32)[None, :]).astype(jnp.float32)
    onehot_y = (by_map[:, None] == jnp.arange(NBY, dtype=jnp.int32)[None, :]).astype(jnp.float32)

    def to_blocks(field):
        stacked = field.reshape(NBZ, BZ, NX, NY).sum(axis=1)
        partial_sum = jnp.einsum('zab,ak->zkb', stacked, onehot_x, precision=highest)
        return jnp.einsum('zkb,bl->zkl', partial_sum, onehot_y, precision=highest)

    coarse_residual = to_blocks(basis * residual)
    coarse_diag = to_blocks(cell_diagonal - 2.0 * inner)
    crossing = []
    for axis in range(3):
        cut = couple[axis] * (1.0 - same[axis])
        crossing.append(to_blocks(pad_after(cut, axis)))
        crossing.append(to_blocks(pad_before(cut, axis)))

    def apply_coarse(estimate):
        applied = coarse_diag * estimate
        for axis in range(3):
            applied = applied - crossing[2 * axis] * pad_after(upper(estimate, axis), axis)
            applied = applied - crossing[2 * axis + 1] * pad_before(lower(estimate, axis), axis)
        return applied

    correction = relaxation * coarse_residual / coarse_diag
    for sweep in range(NSWEEP - 1):
        correction = correction + relaxation * (coarse_residual - apply_coarse(correction)) / coarse_diag
    fine_corr = jnp.einsum('zkl,ak->zal', correction, onehot_x, precision=highest)
    fine_corr = jnp.einsum('zal,bl->zab', fine_corr, onehot_y, precision=highest)
    fine_corr = jnp.repeat(fine_corr, BZ, axis=0)
    new_pressure = pressure + basis * fine_corr
    flows = tuple(trans[axis] * (lower(new_pressure, axis) - upper(new_pressure, axis)) for axis in range(3))
    water_saturation = saturation
    for substep in range(NSUB):
        frac = fractional(water_saturation)
        carried = tuple(jnp.where(flows[axis] > 0, lower(frac, axis), upper(frac, axis)) * flows[axis] for axis in range(3))
        change = jnp.maximum(source, 0.0) + jnp.minimum(source, 0.0) * frac - outflow(carried)
        water_saturation = water_saturation + time_step / porosity * change
    return new_pressure, water_saturation
```

```python
import jax
import jax.numpy as jnp
from jax import lax
from jax.experimental import pallas as pl
from jax.experimental.pallas import tpu as pltpu
from jax.sharding import PartitionSpec as P

NZ = 32
BX = 8
BY = 8
BZ = 4
NSWEEP = 3
NSUB = 4
NFAC = 4
NXL = 8
NYL = 128
EXT = NYL + 8
GROUPS = 4
ROWS_C = 24
REACH = 4

time_step = 0.005
MESH = pl.DeviceIdType.MESH
f32 = jnp.float32
bf16 = jnp.bfloat16
M, PR, B, S, PHI = range(5)


def iota(shape, dim):
    return lax.broadcasted_iota(jnp.int32, shape, dim)


def harmonic(left, right):
    total = left + right
    return 2.0 * left * right / jnp.where(total > 0, total, 1.0)


def split2(v):
    hi = v.astype(bf16)
    return hi, (v - hi.astype(f32)).astype(bf16)


def split3(v):
    hi = v.astype(bf16)
    rest = v - hi.astype(f32)
    mid = rest.astype(bf16)
    return hi, mid, (rest - mid.astype(f32)).astype(bf16)


def nn(a, b):
    return lax.dot_general(a, b, (((1,), (0,)), ((), ())), preferred_element_type=f32)


def nt(a, b):
    return lax.dot_general(a, b, (((1,), (1,)), ((), ())), preferred_element_type=f32)


def roll(v, shift, axis):
    return pltpu.roll(v, shift % v.shape[axis], axis)


def next_x(here, after):
    lane = iota(here.shape, 1)
    return jnp.where(lane < 96, roll(here, -32, 1), roll(after, -32, 1))


def prev_x(here, before):
    lane = iota(here.shape, 1)
    return jnp.where(lane >= 32, roll(here, 32, 1), roll(before, 32, 1))


def comm_kernel(
    sizes,
    perm, fac, pres, sat, bas, bymap, wells, rates, bxmap, fpor, fmob,
    fx_out, fy_out, fz_out, s_out, w_out, src_out, np_out,
    mob, por, newp, E, yh, xs, xr, ys, yr, ps, low, high,
    send_a, recv_a, send_h, recv_h, send_c, recv_c,
):
    n_gx, n_gy, full_y = sizes
    gx = lax.axis_index("gx")
    gy = lax.axis_index("gy")

    def there(dx, dy):
        ok = jnp.bool_(True)
        if dx:
            ok = ok & (gx + dx >= 0) & (gx + dx < n_gx)
        if dy:
            ok = ok & (gy + dy >= 0) & (gy + dy < n_gy)
        return ok

    def where_is(dx, dy):
        return {"gx": gx + dx, "gy": gy + dy}

    partners = [(dx, dy) for dx in range(-REACH, REACH + 1) for dy in (-1, 0, 1) if (dx, dy) != (0, 0)]

    at_edge = (gx < REACH) | (gx >= n_gx - REACH) | (gy == 0) | (gy == n_gy - 1)

    @pl.when(at_edge)
    def _():
        xr[...] = jnp.zeros_like(xr)
        yr[...] = jnp.zeros_like(yr)
        yh[...] = jnp.zeros_like(yh)
        ps[...] = jnp.zeros_like(ps)
        low[...] = jnp.zeros_like(low)
        high[...] = jnp.zeros_like(high)
        for f in range(5):
            E[f, 0] = jnp.zeros((EXT, 128), f32)
            E[f, 3] = jnp.zeros((EXT, 128), f32)

    barrier = pltpu.get_barrier_semaphore()
    for dx, dy in partners:
        @pl.when(there(dx, dy))
        def _(dx=dx, dy=dy):
            pl.semaphore_signal(barrier, inc=1, device_id=where_is(dx, dy), device_id_type=MESH)

    region = fac[...]
    s_nat = sat[...]
    fm = jnp.zeros(region.shape, f32)
    fp = jnp.zeros(region.shape, f32)
    for level in range(NFAC):
        fm = jnp.where(region == level, fmob[level], fm)
        fp = jnp.where(region == level, fpor[level], fp)
    mob[...] = perm[...] * fm * (s_nat * s_nat + (1.0 - s_nat) * (1.0 - s_nat) * 0.25)
    por[...] = fp

    def column(ref, x):
        return ref[pl.ds(x, NZ, NXL), :]

    own_edge = []
    for side, x in ((0, 0), (1, NXL - 1)):
        edge = [column(mob, x), column(pres, x), column(bas, x)]
        own_edge.append(edge)
        for k in range(3):
            xs[side, NZ * k : NZ * (k + 1), :] = edge[k]

    for f, ref in ((M, mob), (PR, pres), (B, bas), (S, sat), (PHI, por)):
        for g in (1, 2):
            block = jnp.concatenate([column(ref, 4 * (g - 1) + i) for i in range(4)], axis=0)
            E[f, g, 0:NYL, :] = block.T

    ys[...] = jnp.zeros_like(ys)
    for side, y in ((0, 0), (1, NYL - 1)):
        for k, f in enumerate((M, PR, B)):
            for g in (1, 2):
                ys[side, 2 * k + g - 1 : 2 * k + g, :] = E[f, g, y : y + 1, :]

    span_x = lax.min(gx, REACH) + lax.min(n_gx - 1 - gx, REACH) + 1
    span_y = lax.min(gy, 1) + lax.min(n_gy - 1 - gy, 1) + 1
    pl.semaphore_wait(barrier, span_x * span_y - 1)

    class Copy:
        def __init__(self, src, dst, sends, recvs, slot_out, slot_in, dx, dy):
            self.dx, self.dy = dx, dy
            self.copy = pltpu.make_async_remote_copy(
                src_ref=src, dst_ref=dst, send_sem=sends.at[slot_out], recv_sem=recvs.at[slot_in],
                device_id=where_is(dx, dy), device_id_type=MESH,
            )

        def start(self):
            pl.when(there(self.dx, self.dy))(lambda: self.copy.start())

        def wait_send(self):
            pl.when(there(self.dx, self.dy))(lambda: self.copy.wait_send())

        def wait_recv(self):
            pl.when(there(-self.dx, -self.dy))(lambda: self.copy.wait_recv())

    edges = [
        Copy(xs.at[1], xr.at[0], send_a, recv_a, 0, 0, 1, 0),
        Copy(xs.at[0], xr.at[1], send_a, recv_a, 1, 1, -1, 0),
        Copy(ys.at[1], yr.at[0], send_a, recv_a, 2, 2, 0, 1),
        Copy(ys.at[0], yr.at[1], send_a, recv_a, 3, 3, 0, -1),
    ]
    for copy in edges:
        copy.start()

    def halo_x(k, fields):
        return [
            Copy(E.at[fields, 2, 0:NYL], E.at[fields, 0, 0:NYL], send_h, recv_h, 2 * k, 2 * k, 1, 0),
            Copy(E.at[fields, 1, 0:NYL], E.at[fields, 3, 0:NYL], send_h, recv_h, 2 * k + 1, 2 * k + 1, -1, 0),
        ]

    up, down = slice(NYL - 8, NYL), slice(0, 8)
    everything = slice(0, 5)
    halo_early = halo_x(0, slice(0, 3))
    halo_late = halo_x(1, slice(3, 5))
    halo_y = [
        Copy(E.at[everything, 1:3, up], yh.at[0, everything, 1:3], send_h, recv_h, 4, 4, 0, 1),
        Copy(E.at[everything, 1:3, down], yh.at[1, everything, 1:3], send_h, recv_h, 5, 5, 0, -1),
        Copy(E.at[everything, 2, up], yh.at[0, everything, 0], send_h, recv_h, 6, 6, 1, 1),
        Copy(E.at[everything, 1, up], yh.at[0, everything, 3], send_h, recv_h, 7, 7, -1, 1),
        Copy(E.at[everything, 2, down], yh.at[1, everything, 0], send_h, recv_h, 8, 8, 1, -1),
        Copy(E.at[everything, 1, down], yh.at[1, everything, 3], send_h, recv_h, 9, 9, -1, -1),
    ]
    for copy in halo_early + halo_y:
        copy.start()

    well_y = wells[...] % full_y
    well_x = wells[...] // full_y
    n_wells = wells.shape[1]
    row = iota((EXT, 1), 0)
    y_here = gy * NYL + jnp.where(row < NYL + 4, row, row - EXT)
    hits_y = (y_here == well_y).astype(f32).astype(bf16)
    x_here = gx * NXL - 4 + iota((16, 1), 0)
    hits_x = jnp.where(x_here == well_x, rates[...], 0.0)
    col = nt(hits_y, jnp.concatenate(split3(hits_x), axis=0))
    col = (col[:, 0:16] + col[:, 16:32] + col[:, 32:48]) * (1.0 / NZ)
    lane = iota((16, 512), 1)
    spread = (lane // NZ == iota((16, 512), 0)).astype(f32).astype(bf16)
    src = nn(jnp.concatenate(split3(col), axis=1), jnp.concatenate([spread] * 3, axis=0))
    for g in range(GROUPS):
        src_out[g] = src[:, 128 * g : 128 * (g + 1)]

    blocks_y = NYL // BY
    map_own = bymap[pl.ds(gy, 1), :] - (gy * blocks_y - 4)
    map_up = bymap[pl.ds(lax.min(gy + 1, n_gy - 1), 1), :] - (gy * blocks_y - 4)
    map_down = bymap[pl.ds(lax.max(gy - 1, 0), 1), :] - (gy * blocks_y - 4)
    sum_y = (iota((ROWS_C, NYL), 0) == map_own).astype(f32).astype(bf16)
    sum_y = jnp.concatenate([sum_y, sum_y], axis=1)

    def column_of(values):
        return jnp.broadcast_to(values.astype(f32), (128, 128)).T

    by_row = column_of(map_own)
    by_up = column_of(map_up)[0:8]
    by_down = column_of(map_down)[120:128]
    by_ext = jnp.concatenate([by_row, jnp.where(iota((8, 128), 0) < 4, by_up, by_down)], axis=0)
    spread_y = (by_ext[:, 0:ROWS_C] == iota((EXT, ROWS_C), 1).astype(f32)).astype(f32).astype(bf16)
    same_y = (by_row == jnp.concatenate([by_row[1:], by_row[:1]], axis=0)).astype(f32)

    kx = [bxmap[lax.clamp(0, gx * NXL - 4 + i, n_gx * NXL - 1)] - gx for i in range(16)]

    def lanes_of(values, shape):
        which = iota(shape, 1) // NZ
        total = jnp.zeros(shape, jnp.int32)
        for i, value in enumerate(values):
            total = jnp.where(which == i, value, total)
        return total

    z_block = (iota((1, 256), 1) % NZ) // BZ
    target = (lanes_of(kx[4:12], (1, 256)) + 1) * 8 + z_block
    sum_xz = (iota((128, 256), 0) == target).astype(f32).astype(bf16)
    sum_xz = jnp.concatenate([sum_xz, sum_xz], axis=1)

    lane128 = iota((NYL, 128), 1)
    row128 = iota((NYL, 128), 0)
    z_of = lane128 % NZ
    m = [E[M, g, 0:NYL, :] for g in (1, 2)]
    p = [E[PR, g, 0:NYL, :] for g in (1, 2)]
    b = [E[B, g, 0:NYL, :] for g in (1, 2)]
    phi = [E[PHI, g, 0:NYL, :] for g in (1, 2)]
    own_src = [src[0:NYL, 128 * g : 128 * (g + 1)] for g in (1, 2)]
    same_x = [lanes_of([(kx[4 + 4 * g + i] == kx[5 + 4 * g + i]).astype(jnp.int32) for i in range(4)], (1, 128)) for g in (0, 1)]

    def nx_(v, g):
        return next_x(v[0], v[1]) if g == 0 else roll(v[1], -32, 1)

    def ny_(v):
        return roll(v, -1, 0)

    def nz_(v):
        return roll(v, -1, 1)

    tx = [harmonic(m[0], nx_(m, 0)), jnp.where(lane128 < 96, harmonic(m[1], nx_(m, 1)), 0.0)]
    ty = [jnp.where(row128 < NYL - 1, harmonic(v, ny_(v)), 0.0) for v in m]
    tz = [jnp.where(z_of < NZ - 1, 0.1 * harmonic(v, nz_(v)), 0.0) for v in m]
    qx = [tx[g] * (p[g] - nx_(p, g)) for g in (0, 1)]
    sums = []
    for g in (0, 1):
        qy = ty[g] * (p[g] - ny_(p[g]))
        qz = tz[g] * (p[g] - nz_(p[g]))
        in_x = prev_x(qx[g], qx[0]) if g == 1 else jnp.where(lane128 >= 32, roll(qx[0], 32, 1), 0.0)
        t_in_x = prev_x(tx[g], tx[0]) if g == 1 else jnp.where(lane128 >= 32, roll(tx[0], 32, 1), 0.0)
        out = qx[g] - in_x + qy - roll(qy, 1, 0) + qz - roll(qz, 1, 1)
        resid = b[g] * (own_src[g] - out)
        cond = tx[g] + t_in_x + ty[g] + roll(ty[g], 1, 0) + tz[g] + roll(tz[g], 1, 1)
        cx = tx[g] * b[g] * nx_(b, g)
        cy = ty[g] * b[g] * ny_(b[g])
        cz = tz[g] * b[g] * nz_(b[g])
        keep_x = same_x[g].astype(f32)
        keep_z = (z_of % BZ != BZ - 1).astype(f32)
        diag = b[g] * b[g] * (0.5 * phi[g] + cond) - 2.0 * (cx * keep_x + cy * same_y + cz * keep_z)
        sums.append((resid, diag, cz * (1.0 - keep_z), cx * (1.0 - keep_x), cy * (1.0 - same_y)))
    inner = []
    for q in range(5):
        hi, mid = split2(jnp.concatenate([sums[0][q], sums[1][q]], axis=1))
        inner.append(nn(sum_y, jnp.concatenate([hi, mid], axis=0)))

    kinds = 5
    z_row = iota((1, kinds * NZ), 1)
    kind = z_row // NZ
    k_low, k_high, k_next = kx[4], kx[11], kx[12]
    together = k_high == k_next
    q_of = lanes_of([0, 1, jnp.where(together, 1, 3), 0, 1], (1, kinds * NZ))
    k_of = lanes_of([k_high, k_high, k_high, k_low, k_low], (1, kinds * NZ))
    scale = jnp.where((kind == 2) & together, -2.0, 1.0)
    lane_to = q_of * 24 + (k_of + 1) * 8 + (z_row % NZ) // BZ
    sum_edge = jnp.where(iota((128, kinds * NZ), 0) == lane_to, scale, 0.0).astype(bf16)
    sum_edge = jnp.concatenate([sum_edge, sum_edge], axis=1)

    for copy in edges:
        copy.wait_recv()

    fields = []
    m0, p0, b0 = [xr[0, NZ * k : NZ * (k + 1), :] for k in range(3)]
    m1, p1, b1 = [xr[1, NZ * k : NZ * (k + 1), :] for k in range(3)]
    (om0, op0, ob0), (om1, op1, ob1) = own_edge
    t1 = harmonic(om1, m1)
    t0 = harmonic(om0, m0)
    fields = [
        -ob1 * t1 * (op1 - p1), ob1 * ob1 * t1, ob1 * b1 * t1,
        -ob0 * t0 * (op0 - p0), ob0 * ob0 * t0,
    ]
    hi, mid = split2(jnp.concatenate(fields, axis=0))
    edge_x = nt(sum_y, jnp.concatenate([hi, mid], axis=1))
    hi, mid = split2(edge_x)
    edge_x = nt(jnp.concatenate([hi, mid], axis=1), sum_edge)

    def wide(ref, side, k):
        return jnp.concatenate([ref[side, 2 * k : 2 * k + 1, :], ref[side, 2 * k + 1 : 2 * k + 2, :]], axis=1)

    um, up_, ub = [wide(yr, 1, k) for k in range(3)]
    dm, dp, db = [wide(yr, 0, k) for k in range(3)]
    om1, op1, ob1 = [wide(ys, 1, k) for k in range(3)]
    om0, op0, ob0 = [wide(ys, 0, k) for k in range(3)]
    t1 = harmonic(om1, um)
    t0 = harmonic(om0, dm)
    rows = iota((ROWS_C, 1), 0)
    r_high = by_row[NYL - 1 : NYL, 0:1].astype(jnp.int32)
    r_low = by_row[0:1, 0:1].astype(jnp.int32)
    r_next = by_up[0:1, 0:1].astype(jnp.int32)
    at_high = rows == r_high
    at_low = rows == r_low
    same = r_high == r_next
    couple = ob1 * ub * t1
    zero = jnp.zeros_like(couple)
    inner[0] = inner[0] + jnp.where(at_high, -ob1 * t1 * (op1 - up_), 0.0) + jnp.where(at_low, -ob0 * t0 * (op0 - dp), 0.0)
    inner[1] = (
        inner[1] + jnp.where(at_high, ob1 * ob1 * t1 - 2.0 * jnp.where(same, couple, zero), 0.0)
        + jnp.where(at_low, ob0 * ob0 * t0, 0.0)
    )
    inner[4] = inner[4] + jnp.where(at_high, jnp.where(same, zero, couple), 0.0)
    hi, mid = split2(jnp.concatenate(inner, axis=0))
    partial = nt(jnp.concatenate([hi, mid], axis=1), sum_xz)
    mine = edge_x
    for q in range(5):
        mine = mine + roll(partial[ROWS_C * q : ROWS_C * (q + 1)], 24 * q, 1)
    ps[REACH] = mine

    def slot(dx):
        return REACH + dx

    coarse = []
    for dx in (4, -4, 3, -3, 2, -2, 1, -1, 0):
        if dx:
            coarse.append(Copy(ps.at[slot(0)], ps.at[slot(-dx)], send_c, recv_c, slot(dx), slot(-dx), dx, 0))
        coarse.append(
            Copy(ps.at[slot(0), 16:24], low.at[slot(-dx)], send_c, recv_c, 9 + slot(dx), 9 + slot(-dx), dx, 1)
        )
        coarse.append(
            Copy(ps.at[slot(0), 0:8], high.at[slot(-dx)], send_c, recv_c, 18 + slot(dx), 18 + slot(-dx), dx, -1)
        )
    for copy in coarse:
        copy.start()
    for copy in halo_late:
        copy.start()

    target = (lanes_of(kx, (1, 512)) + 3) * 8 + (iota((1, 512), 1) % NZ) // BZ
    spread_xz = (iota((64, 512), 0) == target).astype(f32).astype(bf16)
    spread_xz = jnp.concatenate([spread_xz] * 3, axis=0)

    for copy in halo_early + halo_y + halo_late:
        copy.wait_recv()
    take_up = iota((8, 128), 0) < 4
    for f in range(5):
        for g in range(GROUPS):
            E[f, g, NYL:EXT, :] = jnp.where(take_up, yh[1, f, g], yh[0, f, g])

    z_ext = iota((EXT, 128), 1) % NZ
    for g in range(GROUPS):
        after = min(g + 1, GROUPS - 1)
        here = E[M, g]
        fx_out[g] = harmonic(here, next_x(here, E[M, after]))
        fy_out[g] = harmonic(here, roll(here, -1, 0))
        fz_out[g] = jnp.where(z_ext < NZ - 1, 0.1 * harmonic(here, roll(here, -1, 1)), 0.0)
        s_out[g] = E[S, g]
        phi_here = E[PHI, g]
        w_out[g] = time_step / jnp.where(phi_here > 0, phi_here, 1.0)

    for copy in coarse:
        copy.wait_recv()

    lane24 = iota((ROWS_C, 128), 1)
    system = [jnp.zeros((ROWS_C, 128), f32) for _ in range(5)]
    for dx in range(-REACH, REACH + 1):
        k = slot(dx)
        part = jnp.concatenate([ps[k, 0:8] + low[k], ps[k, 8:16], ps[k, 16:24] + high[k]], axis=0)
        first = (dx + 2) * 8
        take = (lane24 >= max(first, 0)) & (lane24 < min(first + 24, 56))
        for q in range(5):
            system[q] = system[q] + jnp.where(take, roll(part, first - 24 * q, 1), 0.0)
    resid, diag, cz, cx, cy = system
    diag = jnp.where(diag > 0, diag, 1.0)
    half = 0.5 / diag
    fixed = half * resid
    estimate = fixed
    for _ in range(NSWEEP - 1):
        flow = (
            cz * roll(estimate, -1, 1) + roll(cz * estimate, 1, 1)
            + cx * roll(estimate, -8, 1) + roll(cx * estimate, 8, 1)
            + cy * roll(estimate, -1, 0) + roll(cy * estimate, 1, 0)
        )
        estimate = 0.5 * estimate + fixed + half * flow
    row24 = iota((ROWS_C, 128), 0)
    wanted = (row24 >= 3) & (row24 < 21) & (lane24 >= 16) & (lane24 < 40)
    estimate = jnp.where(wanted, estimate, 0.0)[:, 0:64]
    spread1 = nn(jnp.concatenate(split3(estimate), axis=1), spread_xz)
    fine = nn(jnp.concatenate([spread_y] * 3, axis=1), jnp.concatenate(split3(spread1), axis=0))

    for g in range(GROUPS):
        newp[g] = E[PR, g] + E[B, g] * fine[:, 128 * g : 128 * (g + 1)]
    for g in range(GROUPS):
        after = min(g + 1, GROUPS - 1)
        here = newp[g]
        fx_out[g] = fx_out[g] * (here - next_x(here, newp[after]))
        fy_out[g] = fy_out[g] * (here - roll(here, -1, 0))
        fz_out[g] = fz_out[g] * (here - roll(here, -1, 1))
        if g in (1, 2):
            np_out[g - 1] = here[0:NYL]

    for copy in edges + halo_early + halo_late + halo_y + coarse:
        copy.wait_send()


def transport_kernel(fx, fy, fz, s_in, w, src, np_in, np_out, s_out, s, out_x):
    for g in range(GROUPS):
        s[g] = s_in[g]
    for step in range(NSUB):
        last = step == NSUB - 1
        frac = []
        for g in range(GROUPS):
            v = s[g]
            wet = v * v
            frac.append(wet / (wet + (1.0 - v) * (1.0 - v) * 0.25))
        carried = []
        for g in range(GROUPS):
            flow = fx[g]
            after = frac[min(g + 1, GROUPS - 1)]
            carried.append(jnp.where(flow > 0, frac[g], next_x(frac[g], after)) * flow)
        for g in range(GROUPS):
            if last and g in (0, 3):
                continue
            flow = fy[g]
            cy = jnp.where(flow > 0, frac[g], roll(frac[g], -1, 0)) * flow
            flow = fz[g]
            cz = jnp.where(flow > 0, frac[g], roll(frac[g], -1, 1)) * flow
            cx = carried[g]
            out = cx - prev_x(cx, carried[max(g - 1, 0)]) + cy - roll(cy, 1, 0) + cz - roll(cz, 1, 1)
            source = src[g]
            change = jnp.maximum(source, 0.0) + jnp.minimum(source, 0.0) * frac[g] - out
            s[g] = s[g] + w[g] * change
    for g in (1, 2):
        for block, dst in ((s[g, 0:NYL, :], s_out), (np_in[g - 1], np_out)):
            back = block.T
            for i in range(4):
                dst[pl.ds(4 * (g - 1) + i, NZ, NXL), :] = back[NZ * i : NZ * (i + 1)]


def solution(mesh):
    n_gx, n_gy = mesh.shape["gx"], mesh.shape["gy"]
    vmem = pl.BlockSpec(memory_space=pltpu.VMEM)
    smem = pl.BlockSpec(memory_space=pltpu.SMEM)

    def body(perm, facies, fpor, fmob, pressure, saturation, basis, bx_map, by_map, well_cells, well_rates):
        assert pressure.shape == (NZ, NXL, NYL)
        flat = lambda a: a.reshape(NZ * NXL, NYL)
        sizes = (n_gx, n_gy, by_map.shape[0])
        wide = jax.ShapeDtypeStruct((GROUPS, EXT, 128), f32)
        own = jax.ShapeDtypeStruct((2, NYL, 128), f32)
        results = pl.pallas_call(
            lambda *refs: comm_kernel(sizes, *refs),
            name="exchange",
            out_shape=[wide] * 6 + [own],
            in_specs=[vmem] * 8 + [smem] * 3,
            out_specs=[vmem] * 7,
            scratch_shapes=[
                pltpu.VMEM((NZ * NXL, NYL), f32),
                pltpu.VMEM((NZ * NXL, NYL), f32),
                pltpu.VMEM((GROUPS, EXT, 128), f32),
                pltpu.VMEM((5, GROUPS, EXT, 128), f32),
                pltpu.VMEM((2, 5, GROUPS, 8, 128), f32),
                pltpu.VMEM((2, 3 * NZ, NYL), f32),
                pltpu.VMEM((2, 3 * NZ, NYL), f32),
                pltpu.VMEM((2, 8, 128), f32),
                pltpu.VMEM((2, 8, 128), f32),
                pltpu.VMEM((2 * REACH + 1, ROWS_C, 128), f32),
                pltpu.VMEM((2 * REACH + 1, 8, 128), f32),
                pltpu.VMEM((2 * REACH + 1, 8, 128), f32),
                pltpu.SemaphoreType.DMA((4,)),
                pltpu.SemaphoreType.DMA((4,)),
                pltpu.SemaphoreType.DMA((10,)),
                pltpu.SemaphoreType.DMA((10,)),
                pltpu.SemaphoreType.DMA((27,)),
                pltpu.SemaphoreType.DMA((27,)),
            ],
            compiler_params=pltpu.CompilerParams(collective_id=0, has_side_effects=True),
        )(
            flat(perm), flat(facies), flat(pressure), flat(saturation), flat(basis),
            by_map.reshape(n_gy, NYL), well_cells.reshape(1, -1), well_rates.reshape(1, -1),
            bx_map, fpor, fmob,
        )
        shape = jax.ShapeDtypeStruct((NZ * NXL, NYL), f32)
        new_pressure, water = pl.pallas_call(
            transport_kernel,
            name="transport",
            out_shape=[shape, shape],
            in_specs=[vmem] * 7,
            out_specs=[vmem] * 2,
            scratch_shapes=[pltpu.VMEM((GROUPS, EXT, 128), f32), pltpu.VMEM((GROUPS, EXT, 128), f32)],
        )(*results)
        return new_pressure.reshape(pressure.shape), water.reshape(pressure.shape)

    cells = P("member", "gx", "gy")
    return jax.shard_map(
        body,
        mesh=mesh,
        in_specs=(cells, cells, P(), P(), cells, cells, cells, P("member"), P("member"), P("member"), P("member")),
        out_specs=(cells, cells),
        check_vma=False,
    )
```

```python
import jax
import jax.numpy as jnp
from jax import lax
from jax.experimental import pallas as pl
from jax.experimental.pallas import tpu as pltpu
from jax.sharding import PartitionSpec as P

NZ = 32
BX = 8
BY = 8
BZ = 4
NSWEEP = 3
NSUB = 4
NFAC = 4
NXL = 8
NYL = 128
EXT = NYL + 8
GROUPS = 4
ROWS_C = 24
REACH = 4

time_step = 0.005
f32 = jnp.float32
bf16 = jnp.bfloat16
M, PR, B, S, PHI = range(5)


def iota(shape, dim):
    return lax.broadcasted_iota(jnp.int32, shape, dim)


def harmonic(left, right):
    total = left + right
    return 2.0 * left * right / jnp.where(total > 0, total, 1.0)


def split2(v):
    hi = v.astype(bf16)
    return hi, (v - hi.astype(f32)).astype(bf16)


def split3(v):
    hi = v.astype(bf16)
    rest = v - hi.astype(f32)
    mid = rest.astype(bf16)
    return hi, mid, (rest - mid.astype(f32)).astype(bf16)


def nn(a, b):
    return lax.dot_general(a, b, (((1,), (0,)), ((), ())), preferred_element_type=f32)


def nt(a, b):
    return lax.dot_general(a, b, (((1,), (1,)), ((), ())), preferred_element_type=f32)


def roll(v, shift, axis):
    return pltpu.roll(v, shift % v.shape[axis], axis)


def next_x(here, after):
    lane = iota(here.shape, 1)
    return jnp.where(lane < 96, roll(here, -32, 1), roll(after, -32, 1))


def prev_x(here, before):
    lane = iota(here.shape, 1)
    return jnp.where(lane >= 32, roll(here, 32, 1), roll(before, 32, 1))


def comm_kernel(
    sizes,
    perm_h, fac_h, pres_h, sat_h, bas_h, bymap_h, wells_h, rates_h, bxmap_h, fpor_h, fmob_h,
    tx_out, ty_out, tz_out, s_out, w_out, src_out, newp,
    perm, fac, pres, sat, bas, bymap, wells, rates, bxmap, fpor, fmob, in_sem,
    mob, por, E, yh, xs, xr, ys, yr, ps, low, high,
    send_a, recv_a, send_h, recv_h, send_c, recv_c,
):
    n_gx, n_gy, full_y = sizes
    gx = lax.axis_index("gx")
    gy = lax.axis_index("gy")

    def there(dx, dy):
        ok = jnp.bool_(True)
        if dx:
            ok = ok & (gx + dx >= 0) & (gx + dx < n_gx)
        if dy:
            ok = ok & (gy + dy >= 0) & (gy + dy < n_gy)
        return ok

    def where_is(dx, dy):
        return {"gx": gx + dx, "gy": gy + dy}

    partners = [(dx, dy) for dx in range(-REACH, REACH + 1) for dy in (-1, 0, 1) if (dx, dy) != (0, 0)]
    partners.sort(key=lambda d: abs(d[0]) + abs(d[1]))
    inputs = [
        pltpu.make_async_copy(src, dst, in_sem.at[i])
        for i, (src, dst) in enumerate(zip(
            (sat_h, fac_h, perm_h, fpor_h, fmob_h, pres_h, bas_h, bxmap_h, bymap_h, wells_h, rates_h),
            (sat, fac, perm, fpor, fmob, pres, bas, bxmap, bymap, wells, rates),
        ))
    ]
    for copy in inputs:
        copy.start()

    at_edge = (gx < REACH) | (gx >= n_gx - REACH) | (gy == 0) | (gy == n_gy - 1)

    @pl.when(at_edge)
    def _():
        ps[...] = jnp.zeros_like(ps)
        low[...] = jnp.zeros_like(low)
        high[...] = jnp.zeros_like(high)
        yh[...] = jnp.zeros_like(yh)
        yr[...] = jnp.zeros_like(yr)

    @pl.when(gx == 0)
    def _():
        xr[0] = jnp.zeros(xr.shape[1:], f32)
        for f in range(5):
            E[f, 0] = jnp.zeros((EXT, 128), f32)

    @pl.when(gx == n_gx - 1)
    def _():
        xr[1] = jnp.zeros(xr.shape[1:], f32)
        for f in range(5):
            E[f, 3] = jnp.zeros((EXT, 128), f32)

    barrier = pltpu.get_barrier_semaphore()
    for dx, dy in partners:
        @pl.when(there(dx, dy))
        def _(dx=dx, dy=dy):
            pl.semaphore_signal(barrier, inc=1, device_id=where_is(dx, dy), device_id_type=pl.DeviceIdType.MESH)

    for i in (0, 1, 2, 3, 4):
        inputs[i].wait()

    region = fac[...]
    s_nat = sat[...]
    fm = jnp.zeros(region.shape, f32)
    fp = jnp.zeros(region.shape, f32)
    for level in range(NFAC):
        fm = jnp.where(region == level, fmob[level], fm)
        fp = jnp.where(region == level, fpor[level], fp)
    mob[...] = perm[...] * fm * (s_nat * s_nat + (1.0 - s_nat) * (1.0 - s_nat) * 0.25)
    por[...] = fp

    def column(ref, x):
        return ref[pl.ds(x, NZ, NXL), :]

    for i in (5, 6):
        inputs[i].wait()

    own_edge = []
    for side, x in ((0, 0), (1, NXL - 1)):
        edge = [column(mob, x), column(pres, x), column(bas, x)]
        own_edge.append(edge)
        for k in range(3):
            xs[side, NZ * k : NZ * (k + 1), :] = edge[k]

    span_x = lax.min(gx, REACH) + lax.min(n_gx - 1 - gx, REACH) + 1
    span_y = lax.min(gy, 1) + lax.min(n_gy - 1 - gy, 1) + 1
    pl.semaphore_wait(barrier, span_x * span_y - 1)

    class Copy:
        def __init__(self, src, dst, sends, recvs, slot_out, slot_in, dx, dy):
            self.dx, self.dy = dx, dy
            self.copy = pltpu.make_async_remote_copy(
                src_ref=src, dst_ref=dst, send_sem=sends.at[slot_out], recv_sem=recvs.at[slot_in],
                device_id=where_is(dx, dy), device_id_type=pl.DeviceIdType.MESH,
            )

        def start(self):
            pl.when(there(self.dx, self.dy))(lambda: self.copy.start())

        def wait_send(self):
            pl.when(there(self.dx, self.dy))(lambda: self.copy.wait_send())

        def wait_recv(self):
            pl.when(there(-self.dx, -self.dy))(lambda: self.copy.wait_recv())

    edges = [
        Copy(xs.at[1], xr.at[0], send_a, recv_a, 0, 0, 1, 0),
        Copy(xs.at[0], xr.at[1], send_a, recv_a, 1, 1, -1, 0),
        Copy(ys.at[1], yr.at[0], send_a, recv_a, 2, 2, 0, 1),
        Copy(ys.at[0], yr.at[1], send_a, recv_a, 3, 3, 0, -1),
    ]
    for copy in edges[:2]:
        copy.start()

    def turn(pairs):
        for f, ref in pairs:
            for g in (1, 2):
                block = jnp.concatenate([column(ref, 4 * (g - 1) + i) for i in range(4)], axis=0)
                E[f, g, 0:NYL, :] = block.T

    turn(((M, mob), (PR, pres), (B, bas)))

    ys[...] = jnp.zeros_like(ys)
    for side, y in ((0, 0), (1, NYL - 1)):
        for k, f in enumerate((M, PR, B)):
            for g in (1, 2):
                ys[side, 2 * k + g - 1 : 2 * k + g, :] = E[f, g, y : y + 1, :]
    for copy in edges[2:]:
        copy.start()
    turn(((S, sat), (PHI, por)))

    def halo_x(k, fields):
        return [
            Copy(E.at[fields, 2, 0:NYL], E.at[fields, 0, 0:NYL], send_h, recv_h, 2 * k, 2 * k, 1, 0),
            Copy(E.at[fields, 1, 0:NYL], E.at[fields, 3, 0:NYL], send_h, recv_h, 2 * k + 1, 2 * k + 1, -1, 0),
        ]

    up, down = slice(NYL - 8, NYL), slice(0, 8)
    everything = slice(0, 5)
    halo_early = halo_x(0, slice(0, 3))
    halo_late = halo_x(1, slice(3, 5))
    halo_y = [
        Copy(E.at[everything, 1:3, up], yh.at[0, everything, 1:3], send_h, recv_h, 4, 4, 0, 1),
        Copy(E.at[everything, 1:3, down], yh.at[1, everything, 1:3], send_h, recv_h, 5, 5, 0, -1),
        Copy(E.at[everything, 2, up], yh.at[0, everything, 0], send_h, recv_h, 6, 6, 1, 1),
        Copy(E.at[everything, 1, up], yh.at[0, everything, 3], send_h, recv_h, 7, 7, -1, 1),
        Copy(E.at[everything, 2, down], yh.at[1, everything, 0], send_h, recv_h, 8, 8, 1, -1),
        Copy(E.at[everything, 1, down], yh.at[1, everything, 3], send_h, recv_h, 9, 9, -1, -1),
    ]
    for copy in halo_early + halo_y:
        copy.start()
    for i in (7, 8, 9, 10):
        inputs[i].wait()

    well_y = wells[...] % full_y
    well_x = wells[...] // full_y
    n_wells = wells.shape[1]
    row = iota((EXT, 1), 0)
    y_here = gy * NYL + jnp.where(row < NYL + 4, row, row - EXT)
    hits_y = (y_here == well_y).astype(f32).astype(bf16)
    x_here = gx * NXL - 4 + iota((16, 1), 0)
    hits_x = jnp.where(x_here == well_x, rates[...], 0.0)
    col = nt(hits_y, jnp.concatenate(split3(hits_x), axis=0))
    col = (col[:, 0:16] + col[:, 16:32] + col[:, 32:48]) * (1.0 / NZ)
    lane = iota((16, 512), 1)
    spread = (lane // NZ == iota((16, 512), 0)).astype(f32).astype(bf16)
    src = nn(jnp.concatenate(split3(col), axis=1), jnp.concatenate([spread] * 3, axis=0))
    for g in range(GROUPS):
        src_out[g] = src[:, 128 * g : 128 * (g + 1)]

    blocks_y = NYL // BY
    map_own = bymap[pl.ds(gy, 1), :] - (gy * blocks_y - 4)
    map_up = bymap[pl.ds(lax.min(gy + 1, n_gy - 1), 1), :] - (gy * blocks_y - 4)
    map_down = bymap[pl.ds(lax.max(gy - 1, 0), 1), :] - (gy * blocks_y - 4)
    sum_y = (iota((ROWS_C, NYL), 0) == map_own).astype(f32).astype(bf16)
    sum_y = jnp.concatenate([sum_y, sum_y], axis=1)

    def column_of(values):
        return jnp.broadcast_to(values.astype(f32), (128, 128)).T

    by_row = column_of(map_own)
    by_up = column_of(map_up)[0:8]
    by_down = column_of(map_down)[120:128]
    by_ext = jnp.concatenate([by_row, jnp.where(iota((8, 128), 0) < 4, by_up, by_down)], axis=0)
    spread_y = (by_ext[:, 0:ROWS_C] == iota((EXT, ROWS_C), 1).astype(f32)).astype(f32).astype(bf16)
    same_y = (by_row == jnp.concatenate([by_row[1:], by_row[:1]], axis=0)).astype(f32)

    kx = [bxmap[lax.clamp(0, gx * NXL - 4 + i, n_gx * NXL - 1)] - gx for i in range(16)]

    def lanes_of(values, shape):
        which = iota(shape, 1) // NZ
        total = jnp.zeros(shape, jnp.int32)
        for i, value in enumerate(values):
            total = jnp.where(which == i, value, total)
        return total

    z_block = (iota((1, 256), 1) % NZ) // BZ
    target = (lanes_of(kx[4:12], (1, 256)) + 1) * 8 + z_block
    sum_xz = (iota((128, 256), 0) == target).astype(f32).astype(bf16)
    sum_xz = jnp.concatenate([sum_xz, sum_xz], axis=1)

    lane128 = iota((NYL, 128), 1)
    row128 = iota((NYL, 128), 0)
    z_of = lane128 % NZ
    m = [E[M, g, 0:NYL, :] for g in (1, 2)]
    p = [E[PR, g, 0:NYL, :] for g in (1, 2)]
    b = [E[B, g, 0:NYL, :] for g in (1, 2)]
    phi = [E[PHI, g, 0:NYL, :] for g in (1, 2)]
    own_src = [src[0:NYL, 128 * g : 128 * (g + 1)] for g in (1, 2)]
    same_x = [lanes_of([(kx[4 + 4 * g + i] == kx[5 + 4 * g + i]).astype(jnp.int32) for i in range(4)], (1, 128)) for g in (0, 1)]

    def nx_(v, g):
        return next_x(v[0], v[1]) if g == 0 else roll(v[1], -32, 1)

    def ny_(v):
        return roll(v, -1, 0)

    def nz_(v):
        return roll(v, -1, 1)

    tx = [harmonic(m[0], nx_(m, 0)), jnp.where(lane128 < 96, harmonic(m[1], nx_(m, 1)), 0.0)]
    ty = [jnp.where(row128 < NYL - 1, harmonic(v, ny_(v)), 0.0) for v in m]
    tz = [jnp.where(z_of < NZ - 1, 0.1 * harmonic(v, nz_(v)), 0.0) for v in m]
    qx = [tx[g] * (p[g] - nx_(p, g)) for g in (0, 1)]
    sums = []
    for g in (0, 1):
        qy = ty[g] * (p[g] - ny_(p[g]))
        qz = tz[g] * (p[g] - nz_(p[g]))
        in_x = prev_x(qx[g], qx[0]) if g == 1 else jnp.where(lane128 >= 32, roll(qx[0], 32, 1), 0.0)
        t_in_x = prev_x(tx[g], tx[0]) if g == 1 else jnp.where(lane128 >= 32, roll(tx[0], 32, 1), 0.0)
        out = qx[g] - in_x + qy - roll(qy, 1, 0) + qz - roll(qz, 1, 1)
        resid = b[g] * (own_src[g] - out)
        cond = tx[g] + t_in_x + ty[g] + roll(ty[g], 1, 0) + tz[g] + roll(tz[g], 1, 1)
        cx = tx[g] * b[g] * nx_(b, g)
        cy = ty[g] * b[g] * ny_(b[g])
        cz = tz[g] * b[g] * nz_(b[g])
        keep_x = same_x[g].astype(f32)
        keep_z = (z_of % BZ != BZ - 1).astype(f32)
        diag = b[g] * b[g] * (0.5 * phi[g] + cond) - 2.0 * (cx * keep_x + cy * same_y + cz * keep_z)
        sums.append((resid, diag, cz * (1.0 - keep_z), cx * (1.0 - keep_x), cy * (1.0 - same_y)))
    inner = []
    for q in range(5):
        hi, mid = split2(jnp.concatenate([sums[0][q], sums[1][q]], axis=1))
        inner.append(nn(sum_y, jnp.concatenate([hi, mid], axis=0)))

    kinds = 5
    z_row = iota((1, kinds * NZ), 1)
    kind = z_row // NZ
    k_low, k_high, k_next = kx[4], kx[11], kx[12]
    together = k_high == k_next
    q_of = lanes_of([0, 1, jnp.where(together, 1, 3), 0, 1], (1, kinds * NZ))
    k_of = lanes_of([k_high, k_high, k_high, k_low, k_low], (1, kinds * NZ))
    scale = jnp.where((kind == 2) & together, -2.0, 1.0)
    lane_to = q_of * 24 + (k_of + 1) * 8 + (z_row % NZ) // BZ
    sum_edge = jnp.where(iota((128, kinds * NZ), 0) == lane_to, scale, 0.0).astype(bf16)
    sum_edge = jnp.concatenate([sum_edge, sum_edge], axis=1)

    for copy in edges:
        copy.wait_recv()

    fields = []
    m0, p0, b0 = [xr[0, NZ * k : NZ * (k + 1), :] for k in range(3)]
    m1, p1, b1 = [xr[1, NZ * k : NZ * (k + 1), :] for k in range(3)]
    (om0, op0, ob0), (om1, op1, ob1) = own_edge
    t1 = harmonic(om1, m1)
    t0 = harmonic(om0, m0)
    fields = [
        -ob1 * t1 * (op1 - p1), ob1 * ob1 * t1, ob1 * b1 * t1,
        -ob0 * t0 * (op0 - p0), ob0 * ob0 * t0,
    ]
    hi, mid = split2(jnp.concatenate(fields, axis=0))
    edge_x = nt(sum_y, jnp.concatenate([hi, mid], axis=1))
    hi, mid = split2(edge_x)
    edge_x = nt(jnp.concatenate([hi, mid], axis=1), sum_edge)

    def wide(ref, side, k):
        return jnp.concatenate([ref[side, 2 * k : 2 * k + 1, :], ref[side, 2 * k + 1 : 2 * k + 2, :]], axis=1)

    um, up_, ub = [wide(yr, 1, k) for k in range(3)]
    dm, dp, db = [wide(yr, 0, k) for k in range(3)]
    om1, op1, ob1 = [wide(ys, 1, k) for k in range(3)]
    om0, op0, ob0 = [wide(ys, 0, k) for k in range(3)]
    t1 = harmonic(om1, um)
    t0 = harmonic(om0, dm)
    rows = iota((ROWS_C, 1), 0)
    r_high = by_row[NYL - 1 : NYL, 0:1].astype(jnp.int32)
    r_low = by_row[0:1, 0:1].astype(jnp.int32)
    r_next = by_up[0:1, 0:1].astype(jnp.int32)
    at_high = rows == r_high
    at_low = rows == r_low
    same = r_high == r_next
    couple = ob1 * ub * t1
    zero = jnp.zeros_like(couple)
    inner[0] = inner[0] + jnp.where(at_high, -ob1 * t1 * (op1 - up_), 0.0) + jnp.where(at_low, -ob0 * t0 * (op0 - dp), 0.0)
    inner[1] = (
        inner[1] + jnp.where(at_high, ob1 * ob1 * t1 - 2.0 * jnp.where(same, couple, zero), 0.0)
        + jnp.where(at_low, ob0 * ob0 * t0, 0.0)
    )
    inner[4] = inner[4] + jnp.where(at_high, jnp.where(same, zero, couple), 0.0)
    hi, mid = split2(jnp.concatenate(inner, axis=0))
    partial = nt(jnp.concatenate([hi, mid], axis=1), sum_xz)
    mine = edge_x
    for q in range(5):
        mine = mine + roll(partial[ROWS_C * q : ROWS_C * (q + 1)], 24 * q, 1)
    ps[REACH] = mine

    def slot(dx):
        return REACH + dx

    coarse = []
    for dx in (4, -4, 3, -3, 2, -2, 1, -1, 0):
        if dx:
            coarse.append(Copy(ps.at[slot(0)], ps.at[slot(-dx)], send_c, recv_c, slot(dx), slot(-dx), dx, 0))
        coarse.append(
            Copy(ps.at[slot(0), 16:24], low.at[slot(-dx)], send_c, recv_c, 9 + slot(dx), 9 + slot(-dx), dx, 1)
        )
        coarse.append(
            Copy(ps.at[slot(0), 0:8], high.at[slot(-dx)], send_c, recv_c, 18 + slot(dx), 18 + slot(-dx), dx, -1)
        )
    for copy in coarse:
        copy.start()
    for copy in halo_late:
        copy.start()

    target = (lanes_of(kx, (1, 512)) + 3) * 8 + (iota((1, 512), 1) % NZ) // BZ
    spread_xz = (iota((64, 512), 0) == target).astype(f32).astype(bf16)
    spread_xz = jnp.concatenate([spread_xz] * 3, axis=0)

    for copy in halo_early + halo_y + halo_late:
        copy.wait_recv()
    take_up = iota((8, 128), 0) < 4
    for f in range(5):
        for g in range(GROUPS):
            E[f, g, NYL:EXT, :] = jnp.where(take_up, yh[1, f, g], yh[0, f, g])

    z_ext = iota((EXT, 128), 1) % NZ
    for g in range(GROUPS):
        after = min(g + 1, GROUPS - 1)
        here = E[M, g]
        tx_out[g] = harmonic(here, next_x(here, E[M, after]))
        ty_out[g] = harmonic(here, roll(here, -1, 0))
        tz_out[g] = jnp.where(z_ext < NZ - 1, 0.1 * harmonic(here, roll(here, -1, 1)), 0.0)
        s_out[g] = E[S, g]
        phi_here = E[PHI, g]
        w_out[g] = time_step / jnp.where(phi_here > 0, phi_here, 1.0)

    for copy in coarse:
        copy.wait_recv()

    lane24 = iota((ROWS_C, 128), 1)
    system = [jnp.zeros((ROWS_C, 128), f32) for _ in range(5)]
    for dx in range(-REACH, REACH + 1):
        k = slot(dx)
        part = jnp.concatenate([ps[k, 0:8] + low[k], ps[k, 8:16], ps[k, 16:24] + high[k]], axis=0)
        first = (dx + 2) * 8
        take = (lane24 >= max(first, 0)) & (lane24 < min(first + 24, 56))
        for q in range(5):
            system[q] = system[q] + jnp.where(take, roll(part, first - 24 * q, 1), 0.0)
    resid, diag, cz, cx, cy = system
    diag = jnp.where(diag > 0, diag, 1.0)
    half = 0.5 / diag
    fixed = half * resid
    estimate = fixed
    for _ in range(NSWEEP - 1):
        flow = (
            cz * roll(estimate, -1, 1) + roll(cz * estimate, 1, 1)
            + cx * roll(estimate, -8, 1) + roll(cx * estimate, 8, 1)
            + cy * roll(estimate, -1, 0) + roll(cy * estimate, 1, 0)
        )
        estimate = 0.5 * estimate + fixed + half * flow
    row24 = iota((ROWS_C, 128), 0)
    wanted = (row24 >= 3) & (row24 < 21) & (lane24 >= 16) & (lane24 < 40)
    estimate = jnp.where(wanted, estimate, 0.0)[:, 0:64]
    spread1 = nn(jnp.concatenate(split3(estimate), axis=1), spread_xz)
    fine = nn(jnp.concatenate([spread_y] * 3, axis=1), jnp.concatenate(split3(spread1), axis=0))

    for g in range(GROUPS):
        newp[g] = E[PR, g] + E[B, g] * fine[:, 128 * g : 128 * (g + 1)]
    for copy in edges + halo_early + halo_late + halo_y + coarse:
        copy.wait_send()


def transport_kernel(tx, ty, tz, s_in, w_in, src, newp, np_out, s_out, s, F, fx, C):
    first, last_row = 8, 8 + EXT - 1

    def flows(g):
        after = min(g + 1, GROUPS - 1)
        return newp[g] - next_x(newp[g], newp[after])

    for g in range(GROUPS):
        fx[g] = tx[g] * flows(g)
    for g in range(GROUPS):
        here = newp[g]
        w = w_in[g]
        source = src[g]
        fx_up = fx[g]
        fx_down = prev_x(fx_up, fx[max(g - 1, 0)])
        fy_up = ty[g] * (here - roll(here, -1, 0))
        fy_down = roll(fy_up, 1, 0)
        fz_up = tz[g] * (here - roll(here, -1, 1))
        fz_down = roll(fz_up, 1, 1)
        C[0, g] = w * jnp.maximum(source, 0.0)
        leaves = jnp.minimum(source, 0.0)
        for k, (up, down) in enumerate(((fx_up, fx_down), (fy_up, fy_down), (fz_up, fz_down))):
            from_up = jnp.maximum(-up, 0.0)
            from_down = jnp.maximum(down, 0.0)
            C[2 + 2 * k, g] = w * from_up
            C[3 + 2 * k, g] = w * from_down
            leaves = leaves - (up + from_up) + (down - from_down)
        C[1, g] = w * leaves

    for step in range(NSUB):
        groups = (1, 2) if step == NSUB - 1 else range(GROUPS)
        for g in range(GROUPS):
            v = s_in[g] if step == 0 else s[g]
            wet = v * v
            f = wet / (wet + (1.0 - v) * (1.0 - v) * 0.25)
            F[g, first : first + EXT] = f
            F[g, first - 1 : first] = f[EXT - 1 : EXT]
            F[g, last_row + 1 : last_row + 2] = f[0:1]
        for g in groups:
            f = F[g, first : first + EXT]
            f_after = F[min(g + 1, GROUPS - 1), first : first + EXT]
            f_before = F[max(g - 1, 0), first : first + EXT]
            v = s_in[g] if step == 0 else s[g]
            v = v + C[0, g] + C[1, g] * f
            v = v + C[4, g] * F[g, first + 1 : first + 1 + EXT] + C[5, g] * F[g, first - 1 : first - 1 + EXT]
            v = v + C[2, g] * next_x(f, f_after) + C[3, g] * prev_x(f, f_before)
            v = v + C[6, g] * roll(f, -1, 1) + C[7, g] * roll(f, 1, 1)
            s[g] = v
    for g in (1, 2):
        for block, dst in ((s[g, 0:NYL, :], s_out), (newp[g, 0:NYL, :], np_out)):
            back = block.T
            for i in range(4):
                dst[pl.ds(4 * (g - 1) + i, NZ, NXL), :] = back[NZ * i : NZ * (i + 1)]


def solution(mesh):
    n_gx, n_gy = mesh.shape["gx"], mesh.shape["gy"]
    vmem = pl.BlockSpec(memory_space=pltpu.VMEM)

    def body(perm, facies, fpor, fmob, pressure, saturation, basis, bx_map, by_map, well_cells, well_rates):
        assert pressure.shape == (NZ, NXL, NYL)
        flat = lambda a: a.reshape(NZ * NXL, NYL)
        sizes = (n_gx, n_gy, by_map.shape[0])
        wide = pltpu.VMEM((GROUPS, EXT, 128), f32)
        cells_in = lambda kind=f32: pltpu.VMEM((NZ * NXL, NYL), kind)
        anywhere = pl.BlockSpec(memory_space=pl.ANY)
        results = pl.pallas_call(
            lambda *refs: comm_kernel(sizes, *refs),
            name="exchange",
            out_shape=[wide] * 7,
            in_specs=[anywhere] * 11,
            out_specs=[vmem] * 7,
            scratch_shapes=[
                cells_in(), cells_in(jnp.int32), cells_in(), cells_in(), cells_in(),
                pltpu.VMEM((n_gy, NYL), jnp.int32),
                pltpu.VMEM((1, well_cells.shape[0]), jnp.int32),
                pltpu.VMEM((1, well_cells.shape[0]), f32),
                pltpu.SMEM(bx_map.shape, jnp.int32),
                pltpu.SMEM(fpor.shape, f32),
                pltpu.SMEM(fmob.shape, f32),
                pltpu.SemaphoreType.DMA((11,)),
                cells_in(),
                cells_in(),
                pltpu.VMEM((5, GROUPS, EXT, 128), f32),
                pltpu.VMEM((2, 5, GROUPS, 8, 128), f32),
                pltpu.VMEM((2, 3 * NZ, NYL), f32),
                pltpu.VMEM((2, 3 * NZ, NYL), f32),
                pltpu.VMEM((2, 8, 128), f32),
                pltpu.VMEM((2, 8, 128), f32),
                pltpu.VMEM((2 * REACH + 1, ROWS_C, 128), f32),
                pltpu.VMEM((2 * REACH + 1, 8, 128), f32),
                pltpu.VMEM((2 * REACH + 1, 8, 128), f32),
                pltpu.SemaphoreType.DMA((4,)),
                pltpu.SemaphoreType.DMA((4,)),
                pltpu.SemaphoreType.DMA((10,)),
                pltpu.SemaphoreType.DMA((10,)),
                pltpu.SemaphoreType.DMA((27,)),
                pltpu.SemaphoreType.DMA((27,)),
            ],
            compiler_params=pltpu.CompilerParams(collective_id=0, has_side_effects=True),
        )(
            flat(perm), flat(facies), flat(pressure), flat(saturation), flat(basis),
            by_map.reshape(n_gy, NYL), well_cells.reshape(1, -1), well_rates.reshape(1, -1),
            bx_map, fpor, fmob,
        )
        shape = jax.ShapeDtypeStruct((NZ * NXL, NYL), f32)
        new_pressure, water = pl.pallas_call(
            transport_kernel,
            name="transport",
            out_shape=[shape, shape],
            in_specs=[vmem] * 7,
            out_specs=[vmem] * 2,
            scratch_shapes=[
                pltpu.VMEM((GROUPS, EXT, 128), f32),
                pltpu.VMEM((GROUPS, EXT + 16, 128), f32),
                pltpu.VMEM((GROUPS, EXT, 128), f32),
                pltpu.VMEM((8, GROUPS, EXT, 128), f32),
            ],
        )(*[pltpu.with_memory_space_constraint(r, pltpu.VMEM) for r in results])
        return new_pressure.reshape(pressure.shape), water.reshape(pressure.shape)

    cells = P("member", "gx", "gy")
    return jax.shard_map(
        body,
        mesh=mesh,
        in_specs=(cells, cells, P(), P(), cells, cells, cells, P("member"), P("member"), P("member"), P("member")),
        out_specs=(cells, cells),
        check_vma=False,
    )
```

```python
import jax
import jax.numpy as jnp
from jax import lax
from jax.experimental import pallas as pl
from jax.experimental.pallas import tpu as pltpu
from jax.sharding import PartitionSpec as P

NZ = 32
BX = 8
BY = 8
BZ = 4
NSWEEP = 3
NSUB = 4
NFAC = 4
NXL = 8
NYL = 128
EXT = NYL + 8
GROUPS = 4
ROWS_C = 24
REACH = 4

time_step = 0.005
f32 = jnp.float32
bf16 = jnp.bfloat16
M, PR, B, S, PHI = range(5)


def iota(shape, dim):
    return lax.broadcasted_iota(jnp.int32, shape, dim)


def harmonic(left, right):
    total = left + right
    return 2.0 * left * right / jnp.where(total > 0, total, 1.0)


def split2(v):
    hi = v.astype(bf16)
    return hi, (v - hi.astype(f32)).astype(bf16)


def split3(v):
    hi = v.astype(bf16)
    rest = v - hi.astype(f32)
    mid = rest.astype(bf16)
    return hi, mid, (rest - mid.astype(f32)).astype(bf16)


def nn(a, b):
    return lax.dot_general(a, b, (((1,), (0,)), ((), ())), preferred_element_type=f32)


def nt(a, b):
    return lax.dot_general(a, b, (((1,), (1,)), ((), ())), preferred_element_type=f32)


def roll(v, shift, axis):
    return pltpu.roll(v, shift % v.shape[axis], axis)


def next_x(here, after):
    lane = iota(here.shape, 1)
    return jnp.where(lane < 96, roll(here, -32, 1), roll(after, -32, 1))


def prev_x(here, before):
    lane = iota(here.shape, 1)
    return jnp.where(lane >= 32, roll(here, 32, 1), roll(before, 32, 1))


def fetch_properties(perm, fac, sat, fpor, fmob, mob, por):
    region = fac[...]
    s_nat = sat[...]
    fm = jnp.zeros(region.shape, f32)
    fp = jnp.zeros(region.shape, f32)
    for level in range(NFAC):
        fm = jnp.where(region == level, fmob[level], fm)
        fp = jnp.where(region == level, fpor[level], fp)
    mob[...] = perm[...] * fm * (s_nat * s_nat + (1.0 - s_nat) * (1.0 - s_nat) * 0.25)
    por[...] = fp


def turned(ref, g):
    block = jnp.concatenate([ref[pl.ds(4 * (g - 1) + i, NZ, NXL), :] for i in range(4)], axis=0)
    return block.T


def edge_rows(ref, x):
    return jnp.concatenate([ref[pl.ds(x + NXL * i, NZ // BZ, NXL * BZ), :] for i in range(BZ)], axis=0)


class Copy:
    def __init__(self, src, dst, send, recv, target, goes, comes):
        self.goes, self.comes = goes, comes
        self.copy = pltpu.make_async_remote_copy(
            src_ref=src, dst_ref=dst, send_sem=send, recv_sem=recv, device_id=target, device_id_type=pl.DeviceIdType.MESH
        )

    def start(self):
        pl.when(self.goes)(lambda: self.copy.start())

    def wait_send(self):
        pl.when(self.goes)(lambda: self.copy.wait_send())

    def wait_recv(self):
        pl.when(self.comes)(lambda: self.copy.wait_recv())


def pair_kernel(
    n_gx, perm_h, fac_h, pres_h, sat_h, bas_h, fpor_h, fmob_h, block_out, edge_out,
    perm, fac, pres, sat, bas, fpor, fmob, in_sem, mob, por, block, edge, block_in, edge_in, send, recv,
):
    gx = lax.axis_index("gx")
    odd = gx % 2 == 1
    partner = jnp.where(odd, gx + 1, gx - 1)
    linked = (partner >= 0) & (partner < n_gx)
    barrier = pltpu.get_barrier_semaphore()

    @pl.when(jnp.logical_not(linked))
    def _():
        block_out[...] = jnp.zeros_like(block_out)
        edge_out[...] = jnp.zeros_like(edge_out)

    @pl.when(linked)
    def _():
        inputs = [
            pltpu.make_async_copy(src, dst, in_sem.at[i])
            for i, (src, dst) in enumerate(zip(
                (sat_h, fac_h, perm_h, fpor_h, fmob_h, pres_h, bas_h), (sat, fac, perm, fpor, fmob, pres, bas)
            ))
        ]
        for copy in inputs:
            copy.start()
        pl.semaphore_signal(barrier, inc=1, device_id={"gx": partner}, device_id_type=pl.DeviceIdType.MESH)
        for copy in inputs:
            copy.wait()
        fetch_properties(perm, fac, sat, fpor, fmob, mob, por)

        def fill(g, x):
            for f, ref in ((M, mob), (PR, pres), (B, bas), (S, sat), (PHI, por)):
                block[f] = turned(ref, g)
            for k, ref in enumerate((mob, pres, bas)):
                edge[NZ * k : NZ * (k + 1)] = edge_rows(ref, x)

        pl.when(odd)(lambda: fill(2, NXL - 1))
        pl.when(jnp.logical_not(odd))(lambda: fill(1, 0))
        pl.semaphore_wait(barrier, 1)
        copies = [
            pltpu.make_async_remote_copy(
                src_ref=src, dst_ref=dst, send_sem=send.at[i], recv_sem=recv.at[i],
                device_id={"gx": partner}, device_id_type=pl.DeviceIdType.MESH,
            )
            for i, (src, dst) in enumerate(((edge, edge_in), (block, block_in)))
        ]
        for copy in copies:
            copy.start()
        for copy in copies:
            copy.wait()
        block_out[...] = block_in[...]
        edge_out[...] = edge_in[...]


def comm_kernel(
    sizes,
    perm, fac, pres, sat, bas, block_in, edge_in, bymap_h, wells_h, rates_h, bxmap_h, fpor_h, fmob_h,
    tx_out, ty_out, tz_out, s_out, w_out, src_out, newp,
    bymap, wells, rates, bxmap, fpor, fmob, in_sem,
    mob, por, E, yh, xs, xr, ys, yr, ps, low, high,
    send_a, recv_a, send_h, recv_h, send_c, recv_c,
):
    n_gx, n_gy, full_y = sizes
    gx = lax.axis_index("gx")
    gy = lax.axis_index("gy")
    odd = gx % 2 == 1
    even = jnp.logical_not(odd)

    def there(dx, dy):
        ok = jnp.bool_(True)
        if dx:
            ok = ok & (gx + dx >= 0) & (gx + dx < n_gx)
        if dy:
            ok = ok & (gy + dy >= 0) & (gy + dy < n_gy)
        return ok

    def where_is(dx, dy):
        return {"gx": gx + dx, "gy": gy + dy}

    partners = [(dx, dy) for dx in range(-REACH, REACH + 1) for dy in (-1, 0, 1) if (dx, dy) != (0, 0)]
    partners.sort(key=lambda d: abs(d[0]) + abs(d[1]))

    inputs = [
        pltpu.make_async_copy(src, dst, in_sem.at[i])
        for i, (src, dst) in enumerate(zip(
            (fpor_h, fmob_h, bxmap_h, bymap_h, wells_h, rates_h), (fpor, fmob, bxmap, bymap, wells, rates)
        ))
    ]
    for copy in inputs:
        copy.start()

    at_edge = (gx < REACH) | (gx >= n_gx - REACH) | (gy == 0) | (gy == n_gy - 1)

    @pl.when(at_edge)
    def _():
        ps[...] = jnp.zeros_like(ps)
        low[...] = jnp.zeros_like(low)
        high[...] = jnp.zeros_like(high)
        yh[...] = jnp.zeros_like(yh)
        yr[...] = jnp.zeros_like(yr)

    barrier = pltpu.get_barrier_semaphore()
    for dx, dy in partners:
        @pl.when(there(dx, dy))
        def _(dx=dx, dy=dy):
            pl.semaphore_signal(barrier, inc=1, device_id=where_is(dx, dy), device_id_type=pl.DeviceIdType.MESH)

    for copy in inputs[:2]:
        copy.wait()
    fetch_properties(perm, fac, sat, fpor, fmob, mob, por)

    def turn(pairs):
        for f, ref in pairs:
            for g in (1, 2):
                E[f, g, 0:NYL, :] = turned(ref, g)

    turn(((M, mob), (PR, pres), (B, bas)))
    ys[...] = jnp.zeros_like(ys)
    for side, y in ((0, 0), (1, NYL - 1)):
        for k, f in enumerate((M, PR, B)):
            for g in (1, 2):
                ys[side, 2 * k + g - 1 : 2 * k + g, :] = E[f, g, y : y + 1, :]
    own_edge = []
    for x in (0, NXL - 1):
        own_edge.append([edge_rows(ref, x) for ref in (mob, pres, bas)])
    for k in range(3):
        xs[NZ * k : NZ * (k + 1)] = jnp.where(odd, own_edge[0][k], own_edge[1][k])

    span_x = lax.min(gx, REACH) + lax.min(n_gx - 1 - gx, REACH) + 1
    span_y = lax.min(gy, 1) + lax.min(n_gy - 1 - gy, 1) + 1
    pl.semaphore_wait(barrier, span_x * span_y - 1)

    def to(src, dst, sends, recvs, slot_out, slot_in, dx, dy):
        return Copy(src, dst, sends.at[slot_out], recvs.at[slot_in], where_is(dx, dy), there(dx, dy), there(-dx, -dy))

    mate = {"gx": jnp.where(odd, gx - 1, gx + 1)}
    always = jnp.bool_(True)
    edges = [
        to(ys.at[1], yr.at[0], send_a, recv_a, 2, 2, 0, 1),
        to(ys.at[0], yr.at[1], send_a, recv_a, 3, 3, 0, -1),
        Copy(xs, xr, send_a.at[0], recv_a.at[0], mate, always, always),
    ]
    for copy in edges:
        copy.start()
    turn(((S, sat), (PHI, por)))

    up, down = slice(NYL - 8, NYL), slice(0, 8)
    every = slice(0, 5)
    halo = [
        to(E.at[every, 1:3, up], yh.at[0, every, 1:3], send_h, recv_h, 4, 4, 0, 1),
        to(E.at[every, 1:3, down], yh.at[1, every, 1:3], send_h, recv_h, 5, 5, 0, -1),
        to(E.at[every, 2, up], yh.at[0, every, 0], send_h, recv_h, 6, 6, 1, 1),
        to(E.at[every, 1, up], yh.at[0, every, 3], send_h, recv_h, 7, 7, -1, 1),
        to(E.at[every, 2, down], yh.at[1, every, 0], send_h, recv_h, 8, 8, 1, -1),
        to(E.at[every, 1, down], yh.at[1, every, 3], send_h, recv_h, 9, 9, -1, -1),
        Copy(E.at[every, 2, 0:NYL], E.at[every, 0, 0:NYL], send_h.at[0], recv_h.at[0], mate, even, odd),
        Copy(E.at[every, 1, 0:NYL], E.at[every, 3, 0:NYL], send_h.at[1], recv_h.at[1], mate, odd, even),
    ]
    for copy in halo:
        copy.start()
    for copy in inputs[2:]:
        copy.wait()

    @pl.when(even)
    def _():
        E[every, 0, 0:NYL] = block_in[...]

    @pl.when(odd)
    def _():
        E[every, 3, 0:NYL] = block_in[...]

    well_y = wells[...] % full_y
    well_x = wells[...] // full_y
    n_wells = wells.shape[1]
    row = iota((EXT, 1), 0)
    y_here = gy * NYL + jnp.where(row < NYL + 4, row, row - EXT)
    hits_y = (y_here == well_y).astype(f32).astype(bf16)
    x_here = gx * NXL - 4 + iota((16, 1), 0)
    hits_x = jnp.where(x_here == well_x, rates[...], 0.0)
    col = nt(hits_y, jnp.concatenate(split3(hits_x), axis=0))
    col = (col[:, 0:16] + col[:, 16:32] + col[:, 32:48]) * (1.0 / NZ)
    lane = iota((16, 512), 1)
    spread = (lane // NZ == iota((16, 512), 0)).astype(f32).astype(bf16)
    src = nn(jnp.concatenate(split3(col), axis=1), jnp.concatenate([spread] * 3, axis=0))
    for g in range(GROUPS):
        src_out[g] = src[:, 128 * g : 128 * (g + 1)]

    blocks_y = NYL // BY
    map_own = bymap[pl.ds(gy, 1), :] - (gy * blocks_y - 4)
    map_up = bymap[pl.ds(lax.min(gy + 1, n_gy - 1), 1), :] - (gy * blocks_y - 4)
    map_down = bymap[pl.ds(lax.max(gy - 1, 0), 1), :] - (gy * blocks_y - 4)
    sum_y = (iota((ROWS_C, NYL), 0) == map_own).astype(f32).astype(bf16)
    sum_y = jnp.concatenate([sum_y, sum_y], axis=1)

    def column_of(values):
        return jnp.broadcast_to(values.astype(f32), (128, 128)).T

    by_row = column_of(map_own)
    by_up = column_of(map_up)[0:8]
    by_down = column_of(map_down)[120:128]
    by_ext = jnp.concatenate([by_row, jnp.where(iota((8, 128), 0) < 4, by_up, by_down)], axis=0)
    spread_y = (by_ext[:, 0:ROWS_C] == iota((EXT, ROWS_C), 1).astype(f32)).astype(f32).astype(bf16)
    same_y = (by_row == jnp.concatenate([by_row[1:], by_row[:1]], axis=0)).astype(f32)

    kx = [bxmap[lax.clamp(0, gx * NXL - 4 + i, n_gx * NXL - 1)] - gx for i in range(16)]

    def lanes_of(values, shape):
        which = iota(shape, 1) // NZ
        total = jnp.zeros(shape, jnp.int32)
        for i, value in enumerate(values):
            total = jnp.where(which == i, value, total)
        return total

    z_block = (iota((1, 256), 1) % NZ) // BZ
    target = (lanes_of(kx[4:12], (1, 256)) + 1) * 8 + z_block
    sum_xz = (iota((128, 256), 0) == target).astype(f32).astype(bf16)
    sum_xz = jnp.concatenate([sum_xz, sum_xz], axis=1)

    lane128 = iota((NYL, 128), 1)
    row128 = iota((NYL, 128), 0)
    z_of = lane128 % NZ
    m = [E[M, g, 0:NYL, :] for g in (1, 2)]
    p = [E[PR, g, 0:NYL, :] for g in (1, 2)]
    b = [E[B, g, 0:NYL, :] for g in (1, 2)]
    phi = [E[PHI, g, 0:NYL, :] for g in (1, 2)]
    own_src = [src[0:NYL, 128 * g : 128 * (g + 1)] for g in (1, 2)]
    same_x = [lanes_of([(kx[4 + 4 * g + i] == kx[5 + 4 * g + i]).astype(jnp.int32) for i in range(4)], (1, 128)) for g in (0, 1)]

    def nx_(v, g):
        return next_x(v[0], v[1]) if g == 0 else roll(v[1], -32, 1)

    def ny_(v):
        return roll(v, -1, 0)

    def nz_(v):
        return roll(v, -1, 1)

    tx = [harmonic(m[0], nx_(m, 0)), jnp.where(lane128 < 96, harmonic(m[1], nx_(m, 1)), 0.0)]
    ty = [jnp.where(row128 < NYL - 1, harmonic(v, ny_(v)), 0.0) for v in m]
    tz = [jnp.where(z_of < NZ - 1, 0.1 * harmonic(v, nz_(v)), 0.0) for v in m]
    qx = [tx[g] * (p[g] - nx_(p, g)) for g in (0, 1)]
    sums = []
    for g in (0, 1):
        qy = ty[g] * (p[g] - ny_(p[g]))
        qz = tz[g] * (p[g] - nz_(p[g]))
        in_x = prev_x(qx[g], qx[0]) if g == 1 else jnp.where(lane128 >= 32, roll(qx[0], 32, 1), 0.0)
        t_in_x = prev_x(tx[g], tx[0]) if g == 1 else jnp.where(lane128 >= 32, roll(tx[0], 32, 1), 0.0)
        out = qx[g] - in_x + qy - roll(qy, 1, 0) + qz - roll(qz, 1, 1)
        resid = b[g] * (own_src[g] - out)
        cond = tx[g] + t_in_x + ty[g] + roll(ty[g], 1, 0) + tz[g] + roll(tz[g], 1, 1)
        cx = tx[g] * b[g] * nx_(b, g)
        cy = ty[g] * b[g] * ny_(b[g])
        cz = tz[g] * b[g] * nz_(b[g])
        keep_x = same_x[g].astype(f32)
        keep_z = (z_of % BZ != BZ - 1).astype(f32)
        diag = b[g] * b[g] * (0.5 * phi[g] + cond) - 2.0 * (cx * keep_x + cy * same_y + cz * keep_z)
        sums.append((resid, diag, cz * (1.0 - keep_z), cx * (1.0 - keep_x), cy * (1.0 - same_y)))
    inner = []
    for q in range(5):
        hi, mid = split2(jnp.concatenate([sums[0][q], sums[1][q]], axis=1))
        inner.append(nn(sum_y, jnp.concatenate([hi, mid], axis=0)))

    k_low, k_high, k_next = kx[4], kx[11], kx[12]
    together = k_high == k_next
    for copy in edges:
        copy.wait_recv()

    from_mate = [xr[NZ * k : NZ * (k + 1)] for k in range(3)]
    from_link = [edge_in[NZ * k : NZ * (k + 1)] for k in range(3)]
    m0, p0, b0 = [jnp.where(odd, v, w) for v, w in zip(from_mate, from_link)]
    m1, p1, b1 = [jnp.where(odd, w, v) for v, w in zip(from_mate, from_link)]
    (om0, op0, ob0), (om1, op1, ob1) = own_edge
    t1 = harmonic(om1, m1)
    t0 = harmonic(om0, m0)

    def layers(v):
        return v[0:8] + v[8:16] + v[16:24] + v[24:32]

    r1, d1, c1 = layers(-ob1 * t1 * (op1 - p1)), layers(ob1 * ob1 * t1), layers(ob1 * b1 * t1)
    r0, d0 = layers(-ob0 * t0 * (op0 - p0)), layers(ob0 * ob0 * t0)
    nothing = jnp.zeros((8, 128), f32)
    d1 = d1 - 2.0 * jnp.where(together, c1, nothing)
    c1 = jnp.where(together, nothing, c1)
    placed = []
    for high_part, low_part in ((r1, r0), (d1, d0), (nothing, nothing), (c1, nothing), (nothing, nothing)):
        for k in (-1, 0, 1):
            placed.append(jnp.where(k_high == k, high_part, nothing) + jnp.where(k_low == k, low_part, nothing))
    hi, mid = split2(jnp.concatenate(placed + [nothing], axis=0))
    mine = nt(sum_y, jnp.concatenate([hi, mid], axis=1))

    def wide(ref, side, k):
        return jnp.concatenate([ref[side, 2 * k : 2 * k + 1, :], ref[side, 2 * k + 1 : 2 * k + 2, :]], axis=1)

    um, up_, ub = [wide(yr, 1, k) for k in range(3)]
    dm, dp, db = [wide(yr, 0, k) for k in range(3)]
    om1, op1, ob1 = [wide(ys, 1, k) for k in range(3)]
    om0, op0, ob0 = [wide(ys, 0, k) for k in range(3)]
    t1 = harmonic(om1, um)
    t0 = harmonic(om0, dm)
    rows = iota((ROWS_C, 1), 0)
    r_high = by_row[NYL - 1 : NYL, 0:1].astype(jnp.int32)
    r_low = by_row[0:1, 0:1].astype(jnp.int32)
    r_next = by_up[0:1, 0:1].astype(jnp.int32)
    at_high = rows == r_high
    at_low = rows == r_low
    same = r_high == r_next
    couple = ob1 * ub * t1
    zero = jnp.zeros_like(couple)
    inner[0] = inner[0] + jnp.where(at_high, -ob1 * t1 * (op1 - up_), 0.0) + jnp.where(at_low, -ob0 * t0 * (op0 - dp), 0.0)
    inner[1] = (
        inner[1] + jnp.where(at_high, ob1 * ob1 * t1 - 2.0 * jnp.where(same, couple, zero), 0.0)
        + jnp.where(at_low, ob0 * ob0 * t0, 0.0)
    )
    inner[4] = inner[4] + jnp.where(at_high, jnp.where(same, zero, couple), 0.0)
    hi, mid = split2(jnp.concatenate(inner, axis=0))
    partial = nt(jnp.concatenate([hi, mid], axis=1), sum_xz)
    for q in range(5):
        mine = mine + roll(partial[ROWS_C * q : ROWS_C * (q + 1)], 24 * q, 1)
    ps[REACH] = mine

    def slot(dx):
        return REACH + dx

    coarse = {}
    for dx in range(-REACH, REACH + 1):
        if dx:
            coarse[dx, 0] = to(ps.at[slot(0)], ps.at[slot(-dx)], send_c, recv_c, slot(dx), slot(-dx), dx, 0)
        coarse[dx, 1] = to(
            ps.at[slot(0), 16:24], low.at[slot(-dx)], send_c, recv_c, 9 + slot(dx), 9 + slot(-dx), dx, 1
        )
        coarse[dx, -1] = to(
            ps.at[slot(0), 0:8], high.at[slot(-dx)], send_c, recv_c, 18 + slot(dx), 18 + slot(-dx), dx, -1
        )
    for dx in (4, -4, 3, -3, 2, -2, 1, -1, 0):
        for dy in (1, -1, 0):
            if (dx, dy) in coarse:
                coarse[dx, dy].start()

    target = (lanes_of(kx, (1, 512)) + 3) * 8 + (iota((1, 512), 1) % NZ) // BZ
    spread_xz = (iota((64, 512), 0) == target).astype(f32).astype(bf16)
    spread_xz = jnp.concatenate([spread_xz] * 3, axis=0)

    for copy in halo:
        copy.wait_recv()
    take_up = iota((8, 128), 0) < 4
    for f in range(5):
        for g in range(GROUPS):
            E[f, g, NYL:EXT, :] = jnp.where(take_up, yh[1, f, g], yh[0, f, g])

    z_ext = iota((EXT, 128), 1) % NZ
    for g in range(GROUPS):
        after = min(g + 1, GROUPS - 1)
        here = E[M, g]
        tx_out[g] = harmonic(here, next_x(here, E[M, after]))
        ty_out[g] = harmonic(here, roll(here, -1, 0))
        tz_out[g] = jnp.where(z_ext < NZ - 1, 0.1 * harmonic(here, roll(here, -1, 1)), 0.0)
        s_out[g] = E[S, g]
        phi_here = E[PHI, g]
        w_out[g] = time_step / jnp.where(phi_here > 0, phi_here, 1.0)

    lane24 = iota((ROWS_C, 128), 1)
    system = [jnp.zeros((ROWS_C, 128), f32) for _ in range(5)]
    for dx in sorted(range(-REACH, REACH + 1), key=abs):
        for dy in (-1, 0, 1):
            if (dx, dy) in coarse:
                coarse[-dx, -dy].wait_recv()
        k = slot(dx)
        part = jnp.concatenate([ps[k, 0:8] + low[k], ps[k, 8:16], ps[k, 16:24] + high[k]], axis=0)
        first = (dx + 2) * 8
        take = (lane24 >= max(first, 0)) & (lane24 < min(first + 24, 56))
        for q in range(5):
            system[q] = system[q] + jnp.where(take, roll(part, first - 24 * q, 1), 0.0)
    resid, diag, cz, cx, cy = system
    diag = jnp.where(diag > 0, diag, 1.0)
    half = 0.5 / diag
    fixed = half * resid
    estimate = fixed
    for _ in range(NSWEEP - 1):
        flow = (
            cz * roll(estimate, -1, 1) + roll(cz * estimate, 1, 1)
            + cx * roll(estimate, -8, 1) + roll(cx * estimate, 8, 1)
            + cy * roll(estimate, -1, 0) + roll(cy * estimate, 1, 0)
        )
        estimate = 0.5 * estimate + fixed + half * flow
    row24 = iota((ROWS_C, 128), 0)
    wanted = (row24 >= 3) & (row24 < 21) & (lane24 >= 16) & (lane24 < 40)
    estimate = jnp.where(wanted, estimate, 0.0)[:, 0:64]
    spread1 = nn(jnp.concatenate(split3(estimate), axis=1), spread_xz)
    fine = nn(jnp.concatenate([spread_y] * 3, axis=1), jnp.concatenate(split3(spread1), axis=0))

    for g in range(GROUPS):
        newp[g] = E[PR, g] + E[B, g] * fine[:, 128 * g : 128 * (g + 1)]
    for copy in edges + halo + list(coarse.values()):
        copy.wait_send()


def transport_kernel(tx, ty, tz, s_in, w_in, src, newp, np_out, s_out, s, F, C, np_nat, s_nat, sem):
    first, last_row = 8, 8 + EXT - 1
    lane = iota((EXT, 128), 1)

    def to_next(rolled, g):
        return jnp.where(lane < 96, rolled[g], rolled[min(g + 1, GROUPS - 1)])

    def to_prev(rolled, g):
        return jnp.where(lane >= 32, rolled[g], rolled[max(g - 1, 0)])

    def put(block, g, dst):
        back = block.T
        for i in range(4):
            dst[pl.ds(4 * (g - 1) + i, NZ, NXL), :] = back[NZ * i : NZ * (i + 1)]

    for g in (1, 2):
        put(newp[g, 0:NYL, :], g, np_nat)
    np_copy = pltpu.make_async_copy(np_nat, np_out, sem.at[0])
    np_copy.start()

    rolled = [roll(newp[g], -32, 1) for g in range(GROUPS)]
    fx = [tx[g] * (newp[g] - to_next(rolled, g)) for g in range(GROUPS)]
    rolled = [roll(v, 32, 1) for v in fx]
    for g in range(GROUPS):
        here = newp[g]
        w = w_in[g]
        source = src[g]
        fx_up = fx[g]
        fx_down = to_prev(rolled, g)
        fy_up = ty[g] * (here - roll(here, -1, 0))
        fy_down = roll(fy_up, 1, 0)
        fz_up = tz[g] * (here - roll(here, -1, 1))
        fz_down = roll(fz_up, 1, 1)
        C[0, g] = w * jnp.maximum(source, 0.0)
        leaves = jnp.minimum(source, 0.0)
        for k, (up, down) in enumerate(((fx_up, fx_down), (fy_up, fy_down), (fz_up, fz_down))):
            from_up = jnp.maximum(-up, 0.0)
            from_down = jnp.maximum(down, 0.0)
            C[2 + 2 * k, g] = w * from_up
            C[3 + 2 * k, g] = w * from_down
            leaves = leaves - (up + from_up) + (down - from_down)
        C[1, g] = w * leaves

    for step in range(NSUB):
        last = step == NSUB - 1
        for g in range(GROUPS):
            v = s_in[g] if step == 0 else s[g]
            wet = v * v
            f = wet / (wet + (1.0 - v) * (1.0 - v) * 0.25)
            F[g, first : first + EXT] = f
            F[g, first - 1 : first] = f[EXT - 1 : EXT]
            F[g, last_row + 1 : last_row + 2] = f[0:1]
        ups = [roll(F[g, first : first + EXT], -32, 1) if g or not last else None for g in range(GROUPS)]
        downs = [roll(F[g, first : first + EXT], 32, 1) if g < 3 or not last else None for g in range(GROUPS)]
        for g in (1, 2) if last else range(GROUPS):
            f = F[g, first : first + EXT]
            v = s_in[g] if step == 0 else s[g]
            v = v + C[0, g] + C[1, g] * f
            v = v + C[4, g] * F[g, first + 1 : first + 1 + EXT] + C[5, g] * F[g, first - 1 : first - 1 + EXT]
            v = v + C[2, g] * to_next(ups, g) + C[3, g] * to_prev(downs, g)
            v = v + C[6, g] * roll(f, -1, 1) + C[7, g] * roll(f, 1, 1)
            s[g] = v
    for g in (1, 2):
        put(s[g, 0:NYL, :], g, s_nat)
    s_copy = pltpu.make_async_copy(s_nat, s_out, sem.at[1])
    s_copy.start()
    np_copy.wait()
    s_copy.wait()


def solution(mesh):
    n_gx, n_gy = mesh.shape["gx"], mesh.shape["gy"]
    vmem = pl.BlockSpec(memory_space=pltpu.VMEM)
    anywhere = pl.BlockSpec(memory_space=pltpu.HBM)

    def body(perm, facies, fpor, fmob, pressure, saturation, basis, bx_map, by_map, well_cells, well_rates):
        assert pressure.shape == (NZ, NXL, NYL) and n_gx % 2 == 0
        flat = [a.reshape(NZ * NXL, NYL) for a in (perm, facies, pressure, saturation, basis)]
        sizes = (n_gx, n_gy, by_map.shape[0])
        wide = pltpu.VMEM((GROUPS, EXT, 128), f32)
        cells_in = lambda kind=f32: pltpu.VMEM((NZ * NXL, NYL), kind)
        natural = [cells_in(), cells_in(jnp.int32), cells_in(), cells_in(), cells_in()]
        facies_tables = [pltpu.SMEM(fpor.shape, f32), pltpu.SMEM(fmob.shape, f32)]
        in_vmem = lambda v: pltpu.with_memory_space_constraint(v, pltpu.VMEM)
        in_hbm = lambda v: pltpu.with_memory_space_constraint(v, pltpu.HBM)
        block = pltpu.VMEM((5, NYL, 128), f32)
        edge = pltpu.VMEM((3 * NZ, NYL), f32)
        link = pl.pallas_call(
            lambda *refs: pair_kernel(n_gx, *refs),
            name="link",
            out_shape=[block, edge],
            in_specs=[anywhere] * 7,
            out_specs=[vmem] * 2,
            scratch_shapes=natural + facies_tables + [
                pltpu.SemaphoreType.DMA((7,)),
                cells_in(), cells_in(),
                block, edge, block, edge,
                pltpu.SemaphoreType.DMA((2,)),
                pltpu.SemaphoreType.DMA((2,)),
            ],
            compiler_params=pltpu.CompilerParams(collective_id=1, has_side_effects=True, vmem_limit_bytes=16 << 20),
        )(*[in_hbm(v) for v in (*flat, fpor, fmob)])
        results = pl.pallas_call(
            lambda *refs: comm_kernel(sizes, *refs),
            name="exchange",
            out_shape=[wide] * 7,
            in_specs=[vmem] * 7 + [anywhere] * 6,
            out_specs=[vmem] * 7,
            scratch_shapes=[
                pltpu.VMEM((n_gy, NYL), jnp.int32),
                pltpu.VMEM((1, well_cells.shape[0]), jnp.int32),
                pltpu.VMEM((1, well_cells.shape[0]), f32),
                pltpu.SMEM(bx_map.shape, jnp.int32),
            ] + facies_tables + [
                pltpu.SemaphoreType.DMA((6,)),
                cells_in(), cells_in(),
                pltpu.VMEM((5, GROUPS, EXT, 128), f32),
                pltpu.VMEM((2, 5, GROUPS, 8, 128), f32),
                edge, edge,
                pltpu.VMEM((2, 8, 128), f32),
                pltpu.VMEM((2, 8, 128), f32),
                pltpu.VMEM((2 * REACH + 1, ROWS_C, 128), f32),
                pltpu.VMEM((2 * REACH + 1, 8, 128), f32),
                pltpu.VMEM((2 * REACH + 1, 8, 128), f32),
                pltpu.SemaphoreType.DMA((4,)),
                pltpu.SemaphoreType.DMA((4,)),
                pltpu.SemaphoreType.DMA((10,)),
                pltpu.SemaphoreType.DMA((10,)),
                pltpu.SemaphoreType.DMA((27,)),
                pltpu.SemaphoreType.DMA((27,)),
            ],
            compiler_params=pltpu.CompilerParams(collective_id=0, has_side_effects=True, vmem_limit_bytes=32 << 20),
        )(
            *[in_vmem(v) for v in flat], *[in_vmem(v) for v in link],
            *[in_hbm(v) for v in (by_map.reshape(n_gy, NYL), well_cells.reshape(1, -1), well_rates.reshape(1, -1), bx_map)],
            fpor, fmob,
        )
        shape = jax.ShapeDtypeStruct((NZ * NXL, NYL), f32)
        new_pressure, water = pl.pallas_call(
            transport_kernel,
            name="transport",
            out_shape=[shape, shape],
            in_specs=[vmem] * 7,
            out_specs=[anywhere] * 2,
            scratch_shapes=[
                pltpu.VMEM((GROUPS, EXT, 128), f32),
                pltpu.VMEM((GROUPS, EXT + 16, 128), f32),
                pltpu.VMEM((8, GROUPS, EXT, 128), f32),
                cells_in(), cells_in(),
                pltpu.SemaphoreType.DMA((2,)),
            ],
            compiler_params=pltpu.CompilerParams(vmem_limit_bytes=32 << 20),
        )(*[in_vmem(v) for v in results])
        return new_pressure.reshape(pressure.shape), water.reshape(pressure.shape)

    cells = P("member", "gx", "gy")
    return jax.shard_map(
        body,
        mesh=mesh,
        in_specs=(cells, cells, P(), P(), cells, cells, cells, P("member"), P("member"), P("member"), P("member")),
        out_specs=(cells, cells),
        check_vma=False,
    )
```

```python
import jax
import jax.numpy as jnp
from jax import lax
from jax.experimental import pallas as pl
from jax.experimental.pallas import tpu as pltpu
from jax.sharding import PartitionSpec as P

NZ = 32
BX = 8
BY = 8
BZ = 4
NSWEEP = 3
NSUB = 4
NFAC = 4
NXL = 8
NYL = 128
EXT = NYL + 8
GROUPS = 4
ROWS_C = 24
REACH = 4
CHUNK = 16

time_step = 0.005
f32 = jnp.float32
bf16 = jnp.bfloat16
M, PR, B, PHI, S = range(5)


def iota(shape, dim):
    return lax.broadcasted_iota(jnp.int32, shape, dim)


def harmonic(left, right):
    total = left + right
    return 2.0 * left * right / jnp.where(total > 0, total, 1.0)


def split2(v):
    hi = v.astype(bf16)
    return hi, (v - hi.astype(f32)).astype(bf16)


def split3(v):
    hi = v.astype(bf16)
    rest = v - hi.astype(f32)
    mid = rest.astype(bf16)
    return hi, mid, (rest - mid.astype(f32)).astype(bf16)


def nn(a, b):
    return lax.dot_general(a, b, (((1,), (0,)), ((), ())), preferred_element_type=f32)


def nt(a, b):
    return lax.dot_general(a, b, (((1,), (1,)), ((), ())), preferred_element_type=f32)


def roll(v, shift, axis):
    return pltpu.roll(v, shift % v.shape[axis], axis)


def next_x(here, after):
    lane = iota(here.shape, 1)
    return jnp.where(lane < 96, roll(here, -32, 1), roll(after, -32, 1))


def prev_x(here, before):
    lane = iota(here.shape, 1)
    return jnp.where(lane >= 32, roll(here, 32, 1), roll(before, 32, 1))


def fetch_properties(perm, fac, sat, fpor, fmob, mob, por):
    region = fac[...]
    s_nat = sat[...]
    fm = jnp.zeros(region.shape, f32)
    fp = jnp.zeros(region.shape, f32)
    for level in range(NFAC):
        fm = jnp.where(region == level, fmob[level], fm)
        fp = jnp.where(region == level, fpor[level], fp)
    mob[...] = perm[...] * fm * (s_nat * s_nat + (1.0 - s_nat) * (1.0 - s_nat) * 0.25)
    por[...] = fp


def turned(ref, g):
    block = jnp.concatenate([ref[pl.ds(4 * (g - 1) + i, NZ, NXL), :] for i in range(4)], axis=0)
    return block.T


def edge_rows(ref, x):
    return jnp.concatenate([ref[pl.ds(x + NXL * i, NZ // BZ, NXL * BZ), :] for i in range(BZ)], axis=0)


class Copy:
    def __init__(self, src, dst, send, recv, target, goes, comes):
        self.goes, self.comes = goes, comes
        self.copy = pltpu.make_async_remote_copy(
            src_ref=src, dst_ref=dst, send_sem=send, recv_sem=recv, device_id=target, device_id_type=pl.DeviceIdType.MESH
        )

    def start(self):
        pl.when(self.goes)(lambda: self.copy.start())

    def wait_send(self):
        pl.when(self.goes)(lambda: self.copy.wait_send())

    def wait_recv(self):
        pl.when(self.comes)(lambda: self.copy.wait_recv())


def comm_kernel(
    sizes,
    perm_h, fac_h, pres_h, sat_h, bas_h, bymap_h, wells_h, rates_h, bxmap_h, fpor_h, fmob_h,
    tx_out, ty_out, tz_out, s_out, w_out, src_out, newp,
    perm, fac, pres, sat, bas, bymap, wells, rates, bxmap, fpor, fmob, in_sem,
    mob, por, E, yh, xs, xr, ys, yr, ps, low, high,
    send_a, recv_a, send_h, recv_h, send_c, recv_c,
):
    n_gx, n_gy, full_y = sizes
    gx = lax.axis_index("gx")
    gy = lax.axis_index("gy")

    def there(dx, dy):
        ok = jnp.bool_(True)
        if dx:
            ok = ok & (gx + dx >= 0) & (gx + dx < n_gx)
        if dy:
            ok = ok & (gy + dy >= 0) & (gy + dy < n_gy)
        return ok

    def where_is(dx, dy):
        return {"gx": gx + dx, "gy": gy + dy}

    partners = [(dx, dy) for dx in range(-REACH, REACH + 1) for dy in (-1, 0, 1) if (dx, dy) != (0, 0)]
    partners.sort(key=lambda d: -abs(d[0]) - abs(d[1]))

    inputs = [
        pltpu.make_async_copy(src, dst, in_sem.at[i])
        for i, (src, dst) in enumerate(zip(
            (sat_h, fac_h, perm_h, fpor_h, fmob_h, pres_h, bas_h, bxmap_h, bymap_h, wells_h, rates_h),
            (sat, fac, perm, fpor, fmob, pres, bas, bxmap, bymap, wells, rates),
        ))
    ]
    for copy in inputs:
        copy.start()

    barrier = pltpu.get_barrier_semaphore()
    for dx, dy in partners:
        @pl.when(there(dx, dy))
        def _(dx=dx, dy=dy):
            pl.semaphore_signal(barrier, inc=1, device_id=where_is(dx, dy), device_id_type=pl.DeviceIdType.MESH)

    for copy in inputs[:5]:
        copy.wait()
    fetch_properties(perm, fac, sat, fpor, fmob, mob, por)
    for copy in inputs[5:7]:
        copy.wait()

    def turn(pairs):
        for f, ref in pairs:
            for g in (1, 2):
                E[f, g, 0:NYL, :] = turned(ref, g)

    turn(((M, mob), (PR, pres), (B, bas)))
    ys[...] = jnp.zeros_like(ys)
    for side, y in ((0, 0), (1, NYL - 1)):
        for k, f in enumerate((M, PR, B)):
            for g in (1, 2):
                ys[side, 2 * k + g - 1 : 2 * k + g, :] = E[f, g, y : y + 1, :]
    own_edge = []
    for x in (0, NXL - 1):
        own_edge.append([edge_rows(ref, x) for ref in (mob, pres, bas)])
    for side in (0, 1):
        for k in range(3):
            xs[side, NZ * k : NZ * (k + 1)] = own_edge[side][k]

    span_x = lax.min(gx, REACH) + lax.min(n_gx - 1 - gx, REACH) + 1
    span_y = lax.min(gy, 1) + lax.min(n_gy - 1 - gy, 1) + 1
    pl.semaphore_wait(barrier, span_x * span_y - 1)

    def to(src, dst, sends, recvs, slot_out, slot_in, dx, dy):
        return Copy(src, dst, sends.at[slot_out], recvs.at[slot_in], where_is(dx, dy), there(dx, dy), there(-dx, -dy))

    edges = [
        to(ys.at[1], yr.at[0], send_a, recv_a, 2, 2, 0, 1),
        to(ys.at[0], yr.at[1], send_a, recv_a, 3, 3, 0, -1),
        to(xs.at[1], xr.at[0], send_a, recv_a, 0, 0, 1, 0),
        to(xs.at[0], xr.at[1], send_a, recv_a, 1, 1, -1, 0),
    ]
    for copy in edges:
        copy.start()
    turn(((PHI, por),))

    up, down = slice(NYL - 8, NYL), slice(0, 8)
    every = slice(0, 5)
    halo = [
        to(E.at[every, 1:3, up], yh.at[0, every, 1:3], send_h, recv_h, 4, 4, 0, 1),
        to(E.at[every, 1:3, down], yh.at[1, every, 1:3], send_h, recv_h, 5, 5, 0, -1),
        to(E.at[every, 2, up], yh.at[0, every, 0], send_h, recv_h, 6, 6, 1, 1),
        to(E.at[every, 1, up], yh.at[0, every, 3], send_h, recv_h, 7, 7, -1, 1),
        to(E.at[every, 2, down], yh.at[1, every, 0], send_h, recv_h, 8, 8, 1, -1),
        to(E.at[every, 1, down], yh.at[1, every, 3], send_h, recv_h, 9, 9, -1, -1),
    ]

    def halo_x(k, fields):
        return [
            to(E.at[fields, 2, 0:NYL], E.at[fields, 0, 0:NYL], send_h, recv_h, 2 * k, 2 * k, 1, 0),
            to(E.at[fields, 1, 0:NYL], E.at[fields, 3, 0:NYL], send_h, recv_h, 2 * k + 1, 2 * k + 1, -1, 0),
        ]

    halo_early = halo_x(0, slice(0, 4))
    halo_late = halo_x(1, slice(4, 5))
    for copy in halo_early:
        copy.start()
    turn(((S, sat),))
    for copy in halo:
        copy.start()
    for copy in inputs[7:]:
        copy.wait()

    def clear_if(missing, *parts):
        @pl.when(missing)
        def _():
            for ref, where in parts:
                ref[where] = jnp.zeros(ref.at[where].shape, f32)

    whole = slice(None)
    clear_if(gx == 0, (xr, 0), (E, (whole, 0)), (yh, (whole, whole, 0)))
    clear_if(gx == n_gx - 1, (xr, 1), (E, (whole, 3)), (yh, (whole, whole, 3)))
    clear_if(gy == 0, (yr, 0), (yh, 0), (low, whole))
    clear_if(gy == n_gy - 1, (yr, 1), (yh, 1), (high, whole))
    for dx in range(1, REACH + 1):
        for k, missing in ((REACH - dx, gx - dx < 0), (REACH + dx, gx + dx >= n_gx)):
            clear_if(missing, (ps, k), (low, k), (high, k))

    well_y = wells[...] % full_y
    well_x = wells[...] // full_y
    n_wells = wells.shape[1]
    row = iota((EXT, 1), 0)
    y_here = gy * NYL + jnp.where(row < NYL + 4, row, row - EXT)
    hits_y = (y_here == well_y).astype(f32).astype(bf16)
    x_here = gx * NXL - 4 + iota((16, 1), 0)
    hits_x = jnp.where(x_here == well_x, rates[...], 0.0)
    col = nt(hits_y, jnp.concatenate(split3(hits_x), axis=0))
    col = (col[:, 0:16] + col[:, 16:32] + col[:, 32:48]) * (1.0 / NZ)
    lane = iota((16, 512), 1)
    spread = (lane // NZ == iota((16, 512), 0)).astype(f32).astype(bf16)
    src = nn(jnp.concatenate(split3(col), axis=1), jnp.concatenate([spread] * 3, axis=0))
    for g in range(GROUPS):
        src_out[g] = src[:, 128 * g : 128 * (g + 1)]

    blocks_y = NYL // BY
    map_own = bymap[pl.ds(gy, 1), :] - (gy * blocks_y - 4)
    map_up = bymap[pl.ds(lax.min(gy + 1, n_gy - 1), 1), :] - (gy * blocks_y - 4)
    map_down = bymap[pl.ds(lax.max(gy - 1, 0), 1), :] - (gy * blocks_y - 4)
    sum_y = (iota((ROWS_C, NYL), 0) == map_own).astype(f32).astype(bf16)
    sum_y = jnp.concatenate([sum_y, sum_y], axis=1)

    def column_of(values):
        return jnp.broadcast_to(values.astype(f32), (128, 128)).T

    by_row = column_of(map_own)
    by_up = column_of(map_up)[0:8]
    by_down = column_of(map_down)[120:128]
    by_ext = jnp.concatenate([by_row, jnp.where(iota((8, 128), 0) < 4, by_up, by_down)], axis=0)
    spread_y = (by_ext[:, 0:ROWS_C] == iota((EXT, ROWS_C), 1).astype(f32)).astype(f32).astype(bf16)
    same_y = (by_row == jnp.concatenate([by_row[1:], by_row[:1]], axis=0)).astype(f32)

    kx = [bxmap[lax.clamp(0, gx * NXL - 4 + i, n_gx * NXL - 1)] - gx for i in range(16)]

    def lanes_of(values, shape):
        which = iota(shape, 1) // NZ
        total = jnp.zeros(shape, jnp.int32)
        for i, value in enumerate(values):
            total = jnp.where(which == i, value, total)
        return total

    z_block = (iota((1, 256), 1) % NZ) // BZ
    target = (lanes_of(kx[4:12], (1, 256)) + 1) * 8 + z_block
    sum_xz = (iota((128, 256), 0) == target).astype(f32).astype(bf16)
    sum_xz = jnp.concatenate([sum_xz, sum_xz], axis=1)

    lane128 = iota((NYL, 128), 1)
    row128 = iota((NYL, 128), 0)
    z_of = lane128 % NZ
    m = [E[M, g, 0:NYL, :] for g in (1, 2)]
    p = [E[PR, g, 0:NYL, :] for g in (1, 2)]
    b = [E[B, g, 0:NYL, :] for g in (1, 2)]
    phi = [E[PHI, g, 0:NYL, :] for g in (1, 2)]
    own_src = [src[0:NYL, 128 * g : 128 * (g + 1)] for g in (1, 2)]
    same_x = [lanes_of([(kx[4 + 4 * g + i] == kx[5 + 4 * g + i]).astype(jnp.int32) for i in range(4)], (1, 128)) for g in (0, 1)]

    def nx_(v, g):
        return next_x(v[0], v[1]) if g == 0 else roll(v[1], -32, 1)

    def ny_(v):
        return roll(v, -1, 0)

    def nz_(v):
        return roll(v, -1, 1)

    tx = [harmonic(m[0], nx_(m, 0)), jnp.where(lane128 < 96, harmonic(m[1], nx_(m, 1)), 0.0)]
    ty = [jnp.where(row128 < NYL - 1, harmonic(v, ny_(v)), 0.0) for v in m]
    tz = [jnp.where(z_of < NZ - 1, 0.1 * harmonic(v, nz_(v)), 0.0) for v in m]
    qx = [tx[g] * (p[g] - nx_(p, g)) for g in (0, 1)]
    sums = []
    for g in (0, 1):
        qy = ty[g] * (p[g] - ny_(p[g]))
        qz = tz[g] * (p[g] - nz_(p[g]))
        in_x = prev_x(qx[g], qx[0]) if g == 1 else jnp.where(lane128 >= 32, roll(qx[0], 32, 1), 0.0)
        t_in_x = prev_x(tx[g], tx[0]) if g == 1 else jnp.where(lane128 >= 32, roll(tx[0], 32, 1), 0.0)
        out = qx[g] - in_x + qy - roll(qy, 1, 0) + qz - roll(qz, 1, 1)
        resid = b[g] * (own_src[g] - out)
        cond = tx[g] + t_in_x + ty[g] + roll(ty[g], 1, 0) + tz[g] + roll(tz[g], 1, 1)
        cx = tx[g] * b[g] * nx_(b, g)
        cy = ty[g] * b[g] * ny_(b[g])
        cz = tz[g] * b[g] * nz_(b[g])
        keep_x = same_x[g].astype(f32)
        keep_z = (z_of % BZ != BZ - 1).astype(f32)
        diag = b[g] * b[g] * (0.5 * phi[g] + cond) - 2.0 * (cx * keep_x + cy * same_y + cz * keep_z)
        sums.append((resid, diag, cz * (1.0 - keep_z), cx * (1.0 - keep_x), cy * (1.0 - same_y)))
    inner = []
    for q in range(5):
        hi, mid = split2(jnp.concatenate([sums[0][q], sums[1][q]], axis=1))
        inner.append(nn(sum_y, jnp.concatenate([hi, mid], axis=0)))

    k_low, k_high, k_next = kx[4], kx[11], kx[12]
    together = k_high == k_next
    for copy in edges:
        copy.wait_recv()

    m0, p0, b0 = [xr[0, NZ * k : NZ * (k + 1)] for k in range(3)]
    m1, p1, b1 = [xr[1, NZ * k : NZ * (k + 1)] for k in range(3)]
    (om0, op0, ob0), (om1, op1, ob1) = own_edge
    t1 = harmonic(om1, m1)
    t0 = harmonic(om0, m0)

    def layers(v):
        return v[0:8] + v[8:16] + v[16:24] + v[24:32]

    r1, d1, c1 = layers(-ob1 * t1 * (op1 - p1)), layers(ob1 * ob1 * t1), layers(ob1 * b1 * t1)
    r0, d0 = layers(-ob0 * t0 * (op0 - p0)), layers(ob0 * ob0 * t0)
    nothing = jnp.zeros((8, 128), f32)
    d1 = d1 - 2.0 * jnp.where(together, c1, nothing)
    c1 = jnp.where(together, nothing, c1)
    placed = []
    for high_part, low_part in ((r1, r0), (d1, d0), (nothing, nothing), (c1, nothing), (nothing, nothing)):
        for k in (-1, 0, 1):
            placed.append(jnp.where(k_high == k, high_part, nothing) + jnp.where(k_low == k, low_part, nothing))
    hi, mid = split2(jnp.concatenate(placed + [nothing], axis=0))
    mine = nt(sum_y, jnp.concatenate([hi, mid], axis=1))

    def wide(ref, side, k):
        return jnp.concatenate([ref[side, 2 * k : 2 * k + 1, :], ref[side, 2 * k + 1 : 2 * k + 2, :]], axis=1)

    um, up_, ub = [wide(yr, 1, k) for k in range(3)]
    dm, dp, db = [wide(yr, 0, k) for k in range(3)]
    om1, op1, ob1 = [wide(ys, 1, k) for k in range(3)]
    om0, op0, ob0 = [wide(ys, 0, k) for k in range(3)]
    t1 = harmonic(om1, um)
    t0 = harmonic(om0, dm)
    rows = iota((ROWS_C, 1), 0)
    r_high = by_row[NYL - 1 : NYL, 0:1].astype(jnp.int32)
    r_low = by_row[0:1, 0:1].astype(jnp.int32)
    r_next = by_up[0:1, 0:1].astype(jnp.int32)
    at_high = rows == r_high
    at_low = rows == r_low
    same = r_high == r_next
    couple = ob1 * ub * t1
    zero = jnp.zeros_like(couple)
    inner[0] = inner[0] + jnp.where(at_high, -ob1 * t1 * (op1 - up_), 0.0) + jnp.where(at_low, -ob0 * t0 * (op0 - dp), 0.0)
    inner[1] = (
        inner[1] + jnp.where(at_high, ob1 * ob1 * t1 - 2.0 * jnp.where(same, couple, zero), 0.0)
        + jnp.where(at_low, ob0 * ob0 * t0, 0.0)
    )
    inner[4] = inner[4] + jnp.where(at_high, jnp.where(same, zero, couple), 0.0)
    hi, mid = split2(jnp.concatenate(inner, axis=0))
    partial = nt(jnp.concatenate([hi, mid], axis=1), sum_xz)
    for q in range(5):
        mine = mine + roll(partial[ROWS_C * q : ROWS_C * (q + 1)], 24 * q, 1)
    ps[REACH] = mine

    def slot(dx):
        return REACH + dx

    coarse = {}
    for dx in range(-REACH, REACH + 1):
        if dx:
            coarse[dx, 0] = to(ps.at[slot(0)], ps.at[slot(-dx)], send_c, recv_c, slot(dx), slot(-dx), dx, 0)
        coarse[dx, 1] = to(
            ps.at[slot(0), 16:24], low.at[slot(-dx)], send_c, recv_c, 9 + slot(dx), 9 + slot(-dx), dx, 1
        )
        coarse[dx, -1] = to(
            ps.at[slot(0), 0:8], high.at[slot(-dx)], send_c, recv_c, 18 + slot(dx), 18 + slot(-dx), dx, -1
        )
    for dx in (4, -4, 3, -3, 2, -2, 1, -1, 0):
        for dy in (1, -1, 0):
            if (dx, dy) in coarse:
                coarse[dx, dy].start()
    for copy in halo_late:
        copy.start()

    target = (lanes_of(kx, (1, 512)) + 3) * 8 + (iota((1, 512), 1) % NZ) // BZ
    spread_xz = (iota((64, 512), 0) == target).astype(f32).astype(bf16)
    spread_xz = jnp.concatenate([spread_xz] * 3, axis=0)

    for copy in halo_early + halo:
        copy.wait_recv()
    take_up = iota((8, 128), 0) < 4
    for f in range(5):
        for g in range(GROUPS):
            E[f, g, NYL:EXT, :] = jnp.where(take_up, yh[1, f, g], yh[0, f, g])

    z_ext = iota((EXT, 128), 1) % NZ
    for g in range(GROUPS):
        after = min(g + 1, GROUPS - 1)
        here = E[M, g]
        tx_out[g] = harmonic(here, next_x(here, E[M, after]))
        ty_out[g] = harmonic(here, roll(here, -1, 0))
        tz_out[g] = jnp.where(z_ext < NZ - 1, 0.1 * harmonic(here, roll(here, -1, 1)), 0.0)
        phi_here = E[PHI, g]
        w_out[g] = time_step / jnp.where(phi_here > 0, phi_here, 1.0)

    lane24 = iota((ROWS_C, 128), 1)
    system = [jnp.zeros((ROWS_C, 128), f32) for _ in range(5)]
    for dx in sorted(range(-REACH, REACH + 1), key=abs):
        if dx == REACH - 1:
            for copy in halo_late:
                copy.wait_recv()
            for g in range(GROUPS):
                s_out[g] = E[S, g]
        for dy in (-1, 0, 1):
            if (dx, dy) in coarse:
                coarse[-dx, -dy].wait_recv()
        k = slot(dx)
        part = jnp.concatenate([ps[k, 0:8] + low[k], ps[k, 8:16], ps[k, 16:24] + high[k]], axis=0)
        first = (dx + 2) * 8
        take = (lane24 >= max(first, 0)) & (lane24 < min(first + 24, 56))
        for q in range(2 if abs(dx) == REACH else 5):
            system[q] = system[q] + jnp.where(take, roll(part, first - 24 * q, 1), 0.0)
    resid, diag, cz, cx, cy = system
    diag = jnp.where(diag > 0, diag, 1.0)
    half = 0.5 / diag
    fixed = half * resid
    estimate = fixed
    for _ in range(NSWEEP - 1):
        flow = (
            cz * roll(estimate, -1, 1) + roll(cz * estimate, 1, 1)
            + cx * roll(estimate, -8, 1) + roll(cx * estimate, 8, 1)
            + cy * roll(estimate, -1, 0) + roll(cy * estimate, 1, 0)
        )
        estimate = 0.5 * estimate + fixed + half * flow
    row24 = iota((ROWS_C, 128), 0)
    wanted = (row24 >= 3) & (row24 < 21) & (lane24 >= 16) & (lane24 < 40)
    estimate = jnp.where(wanted, estimate, 0.0)[:, 0:64]
    spread1 = nn(jnp.concatenate(split3(estimate), axis=1), spread_xz)
    fine = nn(jnp.concatenate([spread_y] * 3, axis=1), jnp.concatenate(split3(spread1), axis=0))

    for g in range(GROUPS):
        newp[g] = E[PR, g] + E[B, g] * fine[:, 128 * g : 128 * (g + 1)]
    for copy in edges + halo + halo_early + halo_late + list(coarse.values()):
        copy.wait_send()


def transport_kernel(tx, ty, tz, s_in, w_in, src, newp, np_out, s_out, s, F, C, np_nat, s_nat, sem):
    first, last_row = 8, 8 + EXT - 1
    lane = iota((EXT, 128), 1)

    def to_next(rolled, g):
        return jnp.where(lane < 96, rolled[g], rolled[min(g + 1, GROUPS - 1)])

    def to_prev(rolled, g):
        return jnp.where(lane >= 32, rolled[g], rolled[max(g - 1, 0)])

    def put(block, g, dst):
        back = block.T
        for i in range(4):
            dst[pl.ds(4 * (g - 1) + i, NZ, NXL), :] = back[NZ * i : NZ * (i + 1)]

    for g in (1, 2):
        put(newp[g, 0:NYL, :], g, np_nat)
    np_copy = pltpu.make_async_copy(np_nat, np_out, sem.at[0])
    np_copy.start()

    rolled = [roll(newp[g], -32, 1) for g in range(GROUPS)]
    fx = [tx[g] * (newp[g] - to_next(rolled, g)) for g in range(GROUPS)]
    rolled = [roll(v, 32, 1) for v in fx]
    for g in range(GROUPS):
        here = newp[g]
        w = w_in[g]
        source = src[g]
        fx_up = fx[g]
        fx_down = to_prev(rolled, g)
        fy_up = ty[g] * (here - roll(here, -1, 0))
        fy_down = roll(fy_up, 1, 0)
        fz_up = tz[g] * (here - roll(here, -1, 1))
        fz_down = roll(fz_up, 1, 1)
        C[0, g] = w * jnp.maximum(source, 0.0)
        leaves = jnp.minimum(source, 0.0)
        for k, (up, down) in enumerate(((fx_up, fx_down), (fy_up, fy_down), (fz_up, fz_down))):
            from_up = jnp.maximum(-up, 0.0)
            from_down = jnp.maximum(down, 0.0)
            C[2 + 2 * k, g] = w * from_up
            C[3 + 2 * k, g] = w * from_down
            leaves = leaves - (up + from_up) + (down - from_down)
        C[1, g] = w * leaves

    for step in range(NSUB):
        last = step == NSUB - 1
        for g in range(GROUPS):
            for a in range(0, EXT, CHUNK):
                b = min(a + CHUNK, EXT)
                v = s_in[g, a:b] if step == 0 else s[g, a:b]
                wet = v * v
                F[g, first + a : first + b] = wet / (wet + (1.0 - v) * (1.0 - v) * 0.25)
            F[g, first - 1 : first] = F[g, last_row : last_row + 1]
            F[g, last_row + 1 : last_row + 2] = F[g, first : first + 1]
        end = NYL if last else EXT
        for a in range(0, end, CHUNK):
            b = min(a + CHUNK, end)
            here = [F[g, first + a : first + b] for g in range(GROUPS)]
            mask_next, mask_prev = lane[a:b] < 96, lane[a:b] >= 32
            ups = [None if last and g == 0 else roll(f, -32, 1) for g, f in enumerate(here)]
            downs = [None if last and g == 3 else roll(f, 32, 1) for g, f in enumerate(here)]
            for g in (1, 2) if last else range(GROUPS):
                v = s_in[g, a:b] if step == 0 else s[g, a:b]
                v = v + C[0, g, a:b] + C[1, g, a:b] * here[g]
                v = v + C[4, g, a:b] * F[g, first + a + 1 : first + b + 1]
                v = v + C[5, g, a:b] * F[g, first + a - 1 : first + b - 1]
                v = v + C[2, g, a:b] * jnp.where(mask_next, ups[g], ups[min(g + 1, GROUPS - 1)])
                v = v + C[3, g, a:b] * jnp.where(mask_prev, downs[g], downs[max(g - 1, 0)])
                v = v + C[6, g, a:b] * roll(here[g], -1, 1) + C[7, g, a:b] * roll(here[g], 1, 1)
                s[g, a:b] = v
    for g in (1, 2):
        put(s[g, 0:NYL, :], g, s_nat)
    s_copy = pltpu.make_async_copy(s_nat, s_out, sem.at[1])
    s_copy.start()
    np_copy.wait()
    s_copy.wait()


def solution(mesh):
    n_gx, n_gy = mesh.shape["gx"], mesh.shape["gy"]
    vmem = pl.BlockSpec(memory_space=pltpu.VMEM)
    anywhere = pl.BlockSpec(memory_space=pltpu.HBM)

    def body(perm, facies, fpor, fmob, pressure, saturation, basis, bx_map, by_map, well_cells, well_rates):
        assert pressure.shape == (NZ, NXL, NYL)
        flat = [a.reshape(NZ * NXL, NYL) for a in (perm, facies, pressure, saturation, basis)]
        sizes = (n_gx, n_gy, by_map.shape[0])
        wide = pltpu.VMEM((GROUPS, EXT, 128), f32)
        cells_in = lambda kind=f32: pltpu.VMEM((NZ * NXL, NYL), kind)
        natural = [cells_in(), cells_in(jnp.int32), cells_in(), cells_in(), cells_in()]
        facies_tables = [pltpu.SMEM(fpor.shape, f32), pltpu.SMEM(fmob.shape, f32)]
        in_vmem = lambda v: pltpu.with_memory_space_constraint(v, pltpu.VMEM)
        in_hbm = lambda v: pltpu.with_memory_space_constraint(v, pltpu.HBM)
        edge = pltpu.VMEM((2, 3 * NZ, NYL), f32)
        results = pl.pallas_call(
            lambda *refs: comm_kernel(sizes, *refs),
            name="exchange",
            out_shape=[wide] * 7,
            in_specs=[anywhere] * 11,
            out_specs=[vmem] * 7,
            scratch_shapes=natural + [
                pltpu.VMEM((n_gy, NYL), jnp.int32),
                pltpu.VMEM((1, well_cells.shape[0]), jnp.int32),
                pltpu.VMEM((1, well_cells.shape[0]), f32),
                pltpu.SMEM(bx_map.shape, jnp.int32),
            ] + facies_tables + [
                pltpu.SemaphoreType.DMA((11,)),
                cells_in(), cells_in(),
                pltpu.VMEM((5, GROUPS, EXT, 128), f32),
                pltpu.VMEM((2, 5, GROUPS, 8, 128), f32),
                edge, edge,
                pltpu.VMEM((2, 8, 128), f32),
                pltpu.VMEM((2, 8, 128), f32),
                pltpu.VMEM((2 * REACH + 1, ROWS_C, 128), f32),
                pltpu.VMEM((2 * REACH + 1, 8, 128), f32),
                pltpu.VMEM((2 * REACH + 1, 8, 128), f32),
                pltpu.SemaphoreType.DMA((4,)),
                pltpu.SemaphoreType.DMA((4,)),
                pltpu.SemaphoreType.DMA((10,)),
                pltpu.SemaphoreType.DMA((10,)),
                pltpu.SemaphoreType.DMA((27,)),
                pltpu.SemaphoreType.DMA((27,)),
            ],
            compiler_params=pltpu.CompilerParams(collective_id=0, has_side_effects=True, vmem_limit_bytes=32 << 20),
        )(
            *[in_hbm(v) for v in (
                *flat, by_map.reshape(n_gy, NYL), well_cells.reshape(1, -1), well_rates.reshape(1, -1), bx_map, fpor, fmob
            )]
        )
        shape = jax.ShapeDtypeStruct((NZ * NXL, NYL), f32)
        new_pressure, water = pl.pallas_call(
            transport_kernel,
            name="transport",
            out_shape=[shape, shape],
            in_specs=[vmem] * 7,
            out_specs=[anywhere] * 2,
            scratch_shapes=[
                pltpu.VMEM((GROUPS, EXT, 128), f32),
                pltpu.VMEM((GROUPS, EXT + 16, 128), f32),
                pltpu.VMEM((8, GROUPS, EXT, 128), f32),
                cells_in(), cells_in(),
                pltpu.SemaphoreType.DMA((2,)),
            ],
            compiler_params=pltpu.CompilerParams(vmem_limit_bytes=32 << 20),
        )(*[in_vmem(v) for v in results])
        return new_pressure.reshape(pressure.shape), water.reshape(pressure.shape)

    cells = P("member", "gx", "gy")
    return jax.shard_map(
        body,
        mesh=mesh,
        in_specs=(cells, cells, P(), P(), cells, cells, cells, P("member"), P("member"), P("member"), P("member")),
        out_specs=(cells, cells),
        check_vma=False,
    )
```

```python
import jax
import jax.numpy as jnp
from jax import lax
from jax.experimental import pallas as pl
from jax.experimental.pallas import tpu as pltpu
from jax.sharding import PartitionSpec as P

NZ = 32
BX = 8
BY = 8
BZ = 4
NSWEEP = 3
NSUB = 4
NFAC = 4
NXL = 8
NYL = 128
EXT = NYL + 8
GROUPS = 4
ROWS_C = 24
REACH = 4
CHUNK = 16

time_step = 0.005
f32 = jnp.float32
bf16 = jnp.bfloat16
M, PR, B, PHI, S = range(5)


def iota(shape, dim):
    return lax.broadcasted_iota(jnp.int32, shape, dim)


def harmonic(left, right):
    total = left + right
    return 2.0 * left * right / jnp.where(total > 0, total, 1.0)


def split2(v):
    hi = v.astype(bf16)
    return hi, (v - hi.astype(f32)).astype(bf16)


def split3(v):
    hi = v.astype(bf16)
    rest = v - hi.astype(f32)
    mid = rest.astype(bf16)
    return hi, mid, (rest - mid.astype(f32)).astype(bf16)


def nn(a, b):
    return lax.dot_general(a, b, (((1,), (0,)), ((), ())), preferred_element_type=f32)


def nt(a, b):
    return lax.dot_general(a, b, (((1,), (1,)), ((), ())), preferred_element_type=f32)


def roll(v, shift, axis):
    return pltpu.roll(v, shift % v.shape[axis], axis)


def next_x(here, after):
    lane = iota(here.shape, 1)
    return jnp.where(lane < 96, roll(here, -32, 1), roll(after, -32, 1))


def prev_x(here, before):
    lane = iota(here.shape, 1)
    return jnp.where(lane >= 32, roll(here, 32, 1), roll(before, 32, 1))


def fetch_properties(perm, fac, sat, fpor, fmob, mob, por):
    region = fac[...]
    s_nat = sat[...]
    fm = jnp.zeros(region.shape, f32)
    fp = jnp.zeros(region.shape, f32)
    for level in range(NFAC):
        fm = jnp.where(region == level, fmob[level], fm)
        fp = jnp.where(region == level, fpor[level], fp)
    mob[...] = perm[...] * fm * (s_nat * s_nat + (1.0 - s_nat) * (1.0 - s_nat) * 0.25)
    por[...] = fp


def turned(ref, g):
    block = jnp.concatenate([ref[pl.ds(4 * (g - 1) + i, NZ, NXL), :] for i in range(4)], axis=0)
    return block.T


def edge_rows(ref, x):
    return jnp.concatenate([ref[pl.ds(x + NXL * i, NZ // BZ, NXL * BZ), :] for i in range(BZ)], axis=0)


class Copy:
    def __init__(self, src, dst, send, recv, target, goes, comes):
        self.goes, self.comes = goes, comes
        self.copy = pltpu.make_async_remote_copy(
            src_ref=src, dst_ref=dst, send_sem=send, recv_sem=recv, device_id=target, device_id_type=pl.DeviceIdType.MESH
        )

    def start(self):
        pl.when(self.goes)(lambda: self.copy.start())

    def wait_send(self):
        pl.when(self.goes)(lambda: self.copy.wait_send())

    def wait_recv(self):
        pl.when(self.comes)(lambda: self.copy.wait_recv())


def comm_kernel(
    sizes,
    perm_h, fac_h, pres_h, sat_h, bas_h, bymap_h, wells_h, rates_h, bxmap_h, fpor_h, fmob_h,
    tx_out, ty_out, tz_out, s_out, w_out, src_out, newp,
    perm, fac, pres, sat, bas, bymap, wells, rates, bxmap, fpor, fmob, in_sem,
    mob, por, E, yh, xs, xr, ys, yr, ps, low, high,
    send_a, recv_a, send_h, recv_h, send_c, recv_c,
):
    n_gx, n_gy, full_y = sizes
    gx = lax.axis_index("gx")
    gy = lax.axis_index("gy")

    def there(dx, dy):
        ok = jnp.bool_(True)
        if dx:
            ok = ok & (gx + dx >= 0) & (gx + dx < n_gx)
        if dy:
            ok = ok & (gy + dy >= 0) & (gy + dy < n_gy)
        return ok

    def where_is(dx, dy):
        return {"gx": gx + dx, "gy": gy + dy}

    partners = [(dx, dy) for dx in range(-REACH, REACH + 1) for dy in (-1, 0, 1) if (dx, dy) != (0, 0)]
    partners.sort(key=lambda d: (0, abs(d[0]) + 2 * abs(d[1])) if abs(d[0]) + 2 * abs(d[1]) < 4 else (1, -abs(d[0]) - abs(d[1])))

    inputs = [
        pltpu.make_async_copy(src, dst, in_sem.at[i])
        for i, (src, dst) in enumerate(zip(
            (sat_h, fac_h, perm_h, fpor_h, fmob_h, pres_h, bas_h, bxmap_h, bymap_h, wells_h, rates_h),
            (sat, fac, perm, fpor, fmob, pres, bas, bxmap, bymap, wells, rates),
        ))
    ]
    for copy in inputs:
        copy.start()

    barrier = pltpu.get_barrier_semaphore()
    for dx, dy in partners:
        @pl.when(there(dx, dy))
        def _(dx=dx, dy=dy):
            pl.semaphore_signal(barrier, inc=1, device_id=where_is(dx, dy), device_id_type=pl.DeviceIdType.MESH)

    for copy in inputs[:5]:
        copy.wait()
    fetch_properties(perm, fac, sat, fpor, fmob, mob, por)
    for copy in inputs[5:7]:
        copy.wait()

    def turn(pairs):
        for f, ref in pairs:
            for g in (1, 2):
                E[f, g, 0:NYL, :] = turned(ref, g)

    turn(((M, mob), (PR, pres), (B, bas)))
    ys[...] = jnp.zeros_like(ys)
    for side, y in ((0, 0), (1, NYL - 1)):
        for k, f in enumerate((M, PR, B)):
            for g in (1, 2):
                ys[side, 2 * k + g - 1 : 2 * k + g, :] = E[f, g, y : y + 1, :]
    own_edge = []
    for x in (0, NXL - 1):
        own_edge.append([edge_rows(ref, x) for ref in (mob, pres, bas)])
    for side in (0, 1):
        for k in range(3):
            xs[side, NZ * k : NZ * (k + 1)] = own_edge[side][k]

    span_x = lax.min(gx, REACH) + lax.min(n_gx - 1 - gx, REACH) + 1
    span_y = lax.min(gy, 1) + lax.min(n_gy - 1 - gy, 1) + 1
    pl.semaphore_wait(barrier, span_x * span_y - 1)

    def to(src, dst, sends, recvs, slot_out, slot_in, dx, dy):
        return Copy(src, dst, sends.at[slot_out], recvs.at[slot_in], where_is(dx, dy), there(dx, dy), there(-dx, -dy))

    edges = [
        to(ys.at[1], yr.at[0], send_a, recv_a, 2, 2, 0, 1),
        to(ys.at[0], yr.at[1], send_a, recv_a, 3, 3, 0, -1),
        to(xs.at[1], xr.at[0], send_a, recv_a, 0, 0, 1, 0),
        to(xs.at[0], xr.at[1], send_a, recv_a, 1, 1, -1, 0),
    ]
    for copy in edges:
        copy.start()

    up, down = slice(NYL - 8, NYL), slice(0, 8)
    every = slice(0, 5)
    halo = [
        to(E.at[every, 1:3, up], yh.at[0, every, 1:3], send_h, recv_h, 4, 4, 0, 1),
        to(E.at[every, 1:3, down], yh.at[1, every, 1:3], send_h, recv_h, 5, 5, 0, -1),
        to(E.at[every, 2, up], yh.at[0, every, 0], send_h, recv_h, 6, 6, 1, 1),
        to(E.at[every, 1, up], yh.at[0, every, 3], send_h, recv_h, 7, 7, -1, 1),
        to(E.at[every, 2, down], yh.at[1, every, 0], send_h, recv_h, 8, 8, 1, -1),
        to(E.at[every, 1, down], yh.at[1, every, 3], send_h, recv_h, 9, 9, -1, -1),
    ]

    def halo_x(k, fields):
        return [
            to(E.at[fields, 2, 0:NYL], E.at[fields, 0, 0:NYL], send_h, recv_h, 2 * k, 2 * k, 1, 0),
            to(E.at[fields, 1, 0:NYL], E.at[fields, 3, 0:NYL], send_h, recv_h, 2 * k + 1, 2 * k + 1, -1, 0),
        ]

    halo_first = halo_x(0, slice(M, M + 1))
    halo_next = halo_x(1, slice(PR, B + 1))
    halo_last = halo_x(5, slice(PHI, S + 1))
    for copy in halo_first + halo_next:
        copy.start()
    turn(((S, sat), (PHI, por)))
    for copy in halo:
        copy.start()
    for copy in inputs[7:]:
        copy.wait()

    def clear_if(missing, *parts):
        @pl.when(missing)
        def _():
            for ref, where in parts:
                ref[where] = jnp.zeros(ref.at[where].shape, f32)

    whole = slice(None)
    clear_if(gx == 0, (xr, 0), (E, (whole, 0)), (yh, (whole, whole, 0)))
    clear_if(gx == n_gx - 1, (xr, 1), (E, (whole, 3)), (yh, (whole, whole, 3)))
    clear_if(gy == 0, (yr, 0), (yh, 0), (low, whole))
    clear_if(gy == n_gy - 1, (yr, 1), (yh, 1), (high, whole))
    for dx in range(1, REACH + 1):
        for k, missing in ((REACH - dx, gx - dx < 0), (REACH + dx, gx + dx >= n_gx)):
            clear_if(missing, (ps, k), (low, k), (high, k))

    well_y = wells[...] % full_y
    well_x = wells[...] // full_y
    n_wells = wells.shape[1]
    row = iota((EXT, 1), 0)
    y_here = gy * NYL + jnp.where(row < NYL + 4, row, row - EXT)
    hits_y = (y_here == well_y).astype(f32).astype(bf16)
    x_here = gx * NXL - 4 + iota((16, 1), 0)
    hits_x = jnp.where(x_here == well_x, rates[...], 0.0)
    col = nt(hits_y, jnp.concatenate(split3(hits_x), axis=0))
    col = (col[:, 0:16] + col[:, 16:32] + col[:, 32:48]) * (1.0 / NZ)
    lane = iota((16, 512), 1)
    spread = (lane // NZ == iota((16, 512), 0)).astype(f32).astype(bf16)
    src = nn(jnp.concatenate(split3(col), axis=1), jnp.concatenate([spread] * 3, axis=0))
    for g in range(GROUPS):
        src_out[g] = src[:, 128 * g : 128 * (g + 1)]

    blocks_y = NYL // BY
    map_own = bymap[pl.ds(gy, 1), :] - (gy * blocks_y - 4)
    map_up = bymap[pl.ds(lax.min(gy + 1, n_gy - 1), 1), :] - (gy * blocks_y - 4)
    map_down = bymap[pl.ds(lax.max(gy - 1, 0), 1), :] - (gy * blocks_y - 4)
    sum_y = (iota((ROWS_C, NYL), 0) == map_own).astype(f32).astype(bf16)
    sum_y = jnp.concatenate([sum_y, sum_y], axis=1)

    def column_of(values):
        return jnp.broadcast_to(values.astype(f32), (128, 128)).T

    by_row = column_of(map_own)
    by_up = column_of(map_up)[0:8]
    by_down = column_of(map_down)[120:128]
    by_ext = jnp.concatenate([by_row, jnp.where(iota((8, 128), 0) < 4, by_up, by_down)], axis=0)
    spread_y = (by_ext[:, 0:ROWS_C] == iota((EXT, ROWS_C), 1).astype(f32)).astype(f32).astype(bf16)
    same_y = (by_row == jnp.concatenate([by_row[1:], by_row[:1]], axis=0)).astype(f32)

    kx = [bxmap[lax.clamp(0, gx * NXL - 4 + i, n_gx * NXL - 1)] - gx for i in range(16)]

    def lanes_of(values, shape):
        which = iota(shape, 1) // NZ
        total = jnp.zeros(shape, jnp.int32)
        for i, value in enumerate(values):
            total = jnp.where(which == i, value, total)
        return total

    z_block = (iota((1, 256), 1) % NZ) // BZ
    target = (lanes_of(kx[4:12], (1, 256)) + 1) * 8 + z_block
    sum_xz = (iota((128, 256), 0) == target).astype(f32).astype(bf16)
    sum_xz = jnp.concatenate([sum_xz, sum_xz], axis=1)

    lane128 = iota((NYL, 128), 1)
    row128 = iota((NYL, 128), 0)
    z_of = lane128 % NZ
    m = [E[M, g, 0:NYL, :] for g in (1, 2)]
    p = [E[PR, g, 0:NYL, :] for g in (1, 2)]
    b = [E[B, g, 0:NYL, :] for g in (1, 2)]
    phi = [E[PHI, g, 0:NYL, :] for g in (1, 2)]
    own_src = [src[0:NYL, 128 * g : 128 * (g + 1)] for g in (1, 2)]
    same_x = [lanes_of([(kx[4 + 4 * g + i] == kx[5 + 4 * g + i]).astype(jnp.int32) for i in range(4)], (1, 128)) for g in (0, 1)]

    def nx_(v, g):
        return next_x(v[0], v[1]) if g == 0 else roll(v[1], -32, 1)

    def ny_(v):
        return roll(v, -1, 0)

    def nz_(v):
        return roll(v, -1, 1)

    tx = [harmonic(m[0], nx_(m, 0)), jnp.where(lane128 < 96, harmonic(m[1], nx_(m, 1)), 0.0)]
    ty = [jnp.where(row128 < NYL - 1, harmonic(v, ny_(v)), 0.0) for v in m]
    tz = [jnp.where(z_of < NZ - 1, 0.1 * harmonic(v, nz_(v)), 0.0) for v in m]
    qx = [tx[g] * (p[g] - nx_(p, g)) for g in (0, 1)]
    sums = []
    for g in (0, 1):
        qy = ty[g] * (p[g] - ny_(p[g]))
        qz = tz[g] * (p[g] - nz_(p[g]))
        in_x = prev_x(qx[g], qx[0]) if g == 1 else jnp.where(lane128 >= 32, roll(qx[0], 32, 1), 0.0)
        t_in_x = prev_x(tx[g], tx[0]) if g == 1 else jnp.where(lane128 >= 32, roll(tx[0], 32, 1), 0.0)
        out = qx[g] - in_x + qy - roll(qy, 1, 0) + qz - roll(qz, 1, 1)
        resid = b[g] * (own_src[g] - out)
        cond = tx[g] + t_in_x + ty[g] + roll(ty[g], 1, 0) + tz[g] + roll(tz[g], 1, 1)
        cx = tx[g] * b[g] * nx_(b, g)
        cy = ty[g] * b[g] * ny_(b[g])
        cz = tz[g] * b[g] * nz_(b[g])
        keep_x = same_x[g].astype(f32)
        keep_z = (z_of % BZ != BZ - 1).astype(f32)
        diag = b[g] * b[g] * (0.5 * phi[g] + cond) - 2.0 * (cx * keep_x + cy * same_y + cz * keep_z)
        sums.append((resid, diag, cz * (1.0 - keep_z), cx * (1.0 - keep_x), cy * (1.0 - same_y)))
    inner = []
    for q in range(5):
        hi, mid = split2(jnp.concatenate([sums[0][q], sums[1][q]], axis=1))
        inner.append(nn(sum_y, jnp.concatenate([hi, mid], axis=0)))

    k_low, k_high, k_next = kx[4], kx[11], kx[12]
    together = k_high == k_next
    for copy in edges:
        copy.wait_recv()

    m0, p0, b0 = [xr[0, NZ * k : NZ * (k + 1)] for k in range(3)]
    m1, p1, b1 = [xr[1, NZ * k : NZ * (k + 1)] for k in range(3)]
    (om0, op0, ob0), (om1, op1, ob1) = own_edge
    t1 = harmonic(om1, m1)
    t0 = harmonic(om0, m0)

    def layers(v):
        return v[0:8] + v[8:16] + v[16:24] + v[24:32]

    r1, d1, c1 = layers(-ob1 * t1 * (op1 - p1)), layers(ob1 * ob1 * t1), layers(ob1 * b1 * t1)
    r0, d0 = layers(-ob0 * t0 * (op0 - p0)), layers(ob0 * ob0 * t0)
    nothing = jnp.zeros((8, 128), f32)
    d1 = d1 - 2.0 * jnp.where(together, c1, nothing)
    c1 = jnp.where(together, nothing, c1)
    placed = []
    for high_part, low_part in ((r1, r0), (d1, d0), (nothing, nothing), (c1, nothing), (nothing, nothing)):
        for k in (-1, 0, 1):
            placed.append(jnp.where(k_high == k, high_part, nothing) + jnp.where(k_low == k, low_part, nothing))
    hi, mid = split2(jnp.concatenate(placed + [nothing], axis=0))
    mine = nt(sum_y, jnp.concatenate([hi, mid], axis=1))

    def wide(ref, side, k):
        return jnp.concatenate([ref[side, 2 * k : 2 * k + 1, :], ref[side, 2 * k + 1 : 2 * k + 2, :]], axis=1)

    um, up_, ub = [wide(yr, 1, k) for k in range(3)]
    dm, dp, db = [wide(yr, 0, k) for k in range(3)]
    om1, op1, ob1 = [wide(ys, 1, k) for k in range(3)]
    om0, op0, ob0 = [wide(ys, 0, k) for k in range(3)]
    t1 = harmonic(om1, um)
    t0 = harmonic(om0, dm)
    rows = iota((ROWS_C, 1), 0)
    r_high = by_row[NYL - 1 : NYL, 0:1].astype(jnp.int32)
    r_low = by_row[0:1, 0:1].astype(jnp.int32)
    r_next = by_up[0:1, 0:1].astype(jnp.int32)
    at_high = rows == r_high
    at_low = rows == r_low
    same = r_high == r_next
    couple = ob1 * ub * t1
    zero = jnp.zeros_like(couple)
    inner[0] = inner[0] + jnp.where(at_high, -ob1 * t1 * (op1 - up_), 0.0) + jnp.where(at_low, -ob0 * t0 * (op0 - dp), 0.0)
    inner[1] = (
        inner[1] + jnp.where(at_high, ob1 * ob1 * t1 - 2.0 * jnp.where(same, couple, zero), 0.0)
        + jnp.where(at_low, ob0 * ob0 * t0, 0.0)
    )
    inner[4] = inner[4] + jnp.where(at_high, jnp.where(same, zero, couple), 0.0)
    hi, mid = split2(jnp.concatenate(inner, axis=0))
    partial = nt(jnp.concatenate([hi, mid], axis=1), sum_xz)
    for q in range(5):
        mine = mine + roll(partial[ROWS_C * q : ROWS_C * (q + 1)], 24 * q, 1)
    ps[REACH] = mine

    def slot(dx):
        return REACH + dx

    coarse = {}
    for dx in range(-REACH, REACH + 1):
        if dx:
            coarse[dx, 0] = to(ps.at[slot(0)], ps.at[slot(-dx)], send_c, recv_c, slot(dx), slot(-dx), dx, 0)
        coarse[dx, 1] = to(
            ps.at[slot(0), 16:24], low.at[slot(-dx)], send_c, recv_c, 9 + slot(dx), 9 + slot(-dx), dx, 1
        )
        coarse[dx, -1] = to(
            ps.at[slot(0), 0:8], high.at[slot(-dx)], send_c, recv_c, 18 + slot(dx), 18 + slot(-dx), dx, -1
        )
    for dx in (4, -4, 3, -3, 2, -2, 1, -1, 0):
        for dy in (1, -1, 0):
            if (dx, dy) in coarse:
                coarse[dx, dy].start()
    for copy in halo_last:
        copy.start()

    target = (lanes_of(kx, (1, 512)) + 3) * 8 + (iota((1, 512), 1) % NZ) // BZ
    spread_xz = (iota((64, 512), 0) == target).astype(f32).astype(bf16)
    spread_xz = jnp.concatenate([spread_xz] * 3, axis=0)

    for copy in halo_first + halo:
        copy.wait_recv()
    take_up = iota((8, 128), 0) < 4
    for f in range(5):
        for g in range(GROUPS):
            E[f, g, NYL:EXT, :] = jnp.where(take_up, yh[1, f, g], yh[0, f, g])

    z_ext = iota((EXT, 128), 1) % NZ
    for g in range(GROUPS):
        after = min(g + 1, GROUPS - 1)
        here = E[M, g]
        tx_out[g] = harmonic(here, next_x(here, E[M, after]))
        ty_out[g] = harmonic(here, roll(here, -1, 0))
        tz_out[g] = jnp.where(z_ext < NZ - 1, 0.1 * harmonic(here, roll(here, -1, 1)), 0.0)

    def finish(g):
        s_out[g] = E[S, g]
        phi_here = E[PHI, g]
        w_out[g] = time_step / jnp.where(phi_here > 0, phi_here, 1.0)

    finish(1)
    finish(2)

    lane24 = iota((ROWS_C, 128), 1)
    system = [jnp.zeros((ROWS_C, 128), f32) for _ in range(5)]
    for dx in sorted(range(-REACH, REACH + 1), key=abs):
        for dy in (-1, 0, 1):
            if (dx, dy) in coarse:
                coarse[-dx, -dy].wait_recv()
        k = slot(dx)
        part = jnp.concatenate([ps[k, 0:8] + low[k], ps[k, 8:16], ps[k, 16:24] + high[k]], axis=0)
        first = (dx + 2) * 8
        take = (lane24 >= max(first, 0)) & (lane24 < min(first + 24, 56))
        for q in range(2 if abs(dx) == REACH else 5):
            system[q] = system[q] + jnp.where(take, roll(part, first - 24 * q, 1), 0.0)
    resid, diag, cz, cx, cy = system
    diag = jnp.where(diag > 0, diag, 1.0)
    half = 0.5 / diag
    fixed = half * resid
    estimate = fixed
    for _ in range(NSWEEP - 1):
        flow = (
            cz * roll(estimate, -1, 1) + roll(cz * estimate, 1, 1)
            + cx * roll(estimate, -8, 1) + roll(cx * estimate, 8, 1)
            + cy * roll(estimate, -1, 0) + roll(cy * estimate, 1, 0)
        )
        estimate = 0.5 * estimate + fixed + half * flow
    row24 = iota((ROWS_C, 128), 0)
    wanted = (row24 >= 3) & (row24 < 21) & (lane24 >= 16) & (lane24 < 40)
    estimate = jnp.where(wanted, estimate, 0.0)[:, 0:64]
    spread1 = nn(jnp.concatenate(split3(estimate), axis=1), spread_xz)
    fine = nn(jnp.concatenate([spread_y] * 3, axis=1), jnp.concatenate(split3(spread1), axis=0))

    for copy in halo_next:
        copy.wait_recv()
    for g in range(GROUPS):
        newp[g] = E[PR, g] + E[B, g] * fine[:, 128 * g : 128 * (g + 1)]
    for copy in halo_last:
        copy.wait_recv()
    finish(0)
    finish(3)
    for copy in edges + halo + halo_first + halo_next + halo_last + list(coarse.values()):
        copy.wait_send()


def transport_kernel(tx, ty, tz, s_in, w_in, src, newp, np_out, s_out, s, F, C, np_nat, s_nat, sem):
    first, last_row = 8, 8 + EXT - 1
    lane = iota((EXT, 128), 1)

    def to_next(rolled, g):
        return jnp.where(lane < 96, rolled[g], rolled[min(g + 1, GROUPS - 1)])

    def to_prev(rolled, g):
        return jnp.where(lane >= 32, rolled[g], rolled[max(g - 1, 0)])

    def put(block, g, dst):
        back = block.T
        for i in range(4):
            dst[pl.ds(4 * (g - 1) + i, NZ, NXL), :] = back[NZ * i : NZ * (i + 1)]

    for g in (1, 2):
        put(newp[g, 0:NYL, :], g, np_nat)
    np_copy = pltpu.make_async_copy(np_nat, np_out, sem.at[0])
    np_copy.start()

    rolled = [roll(newp[g], -32, 1) for g in range(GROUPS)]
    fx = [tx[g] * (newp[g] - to_next(rolled, g)) for g in range(GROUPS)]
    rolled = [roll(v, 32, 1) for v in fx]
    for g in range(GROUPS):
        here = newp[g]
        w = w_in[g]
        source = src[g]
        fx_up = fx[g]
        fx_down = to_prev(rolled, g)
        fy_up = ty[g] * (here - roll(here, -1, 0))
        fy_down = roll(fy_up, 1, 0)
        fz_up = tz[g] * (here - roll(here, -1, 1))
        fz_down = roll(fz_up, 1, 1)
        C[0, g] = w * jnp.maximum(source, 0.0)
        leaves = jnp.minimum(source, 0.0)
        for k, (up, down) in enumerate(((fx_up, fx_down), (fy_up, fy_down), (fz_up, fz_down))):
            from_up = jnp.maximum(-up, 0.0)
            from_down = jnp.maximum(down, 0.0)
            C[2 + 2 * k, g] = w * from_up
            C[3 + 2 * k, g] = w * from_down
            leaves = leaves - (up + from_up) + (down - from_down)
        C[1, g] = w * leaves

    for step in range(NSUB):
        last = step == NSUB - 1
        for g in range(GROUPS):
            for a in range(0, EXT, CHUNK):
                b = min(a + CHUNK, EXT)
                v = s_in[g, a:b] if step == 0 else s[g, a:b]
                wet = v * v
                F[g, first + a : first + b] = wet / (wet + (1.0 - v) * (1.0 - v) * 0.25)
            F[g, first - 1 : first] = F[g, last_row : last_row + 1]
            F[g, last_row + 1 : last_row + 2] = F[g, first : first + 1]
        end = NYL if last else EXT
        for a in range(0, end, CHUNK):
            b = min(a + CHUNK, end)
            here = [F[g, first + a : first + b] for g in range(GROUPS)]
            mask_next, mask_prev = lane[a:b] < 96, lane[a:b] >= 32
            ups = [None if last and g == 0 else roll(f, -32, 1) for g, f in enumerate(here)]
            downs = [None if last and g == 3 else roll(f, 32, 1) for g, f in enumerate(here)]
            for g in (1, 2) if last else range(GROUPS):
                v = s_in[g, a:b] if step == 0 else s[g, a:b]
                v = v + C[0, g, a:b] + C[1, g, a:b] * here[g]
                v = v + C[4, g, a:b] * F[g, first + a + 1 : first + b + 1]
                v = v + C[5, g, a:b] * F[g, first + a - 1 : first + b - 1]
                v = v + C[2, g, a:b] * jnp.where(mask_next, ups[g], ups[min(g + 1, GROUPS - 1)])
                v = v + C[3, g, a:b] * jnp.where(mask_prev, downs[g], downs[max(g - 1, 0)])
                v = v + C[6, g, a:b] * roll(here[g], -1, 1) + C[7, g, a:b] * roll(here[g], 1, 1)
                s[g, a:b] = v
    for g in (1, 2):
        put(s[g, 0:NYL, :], g, s_nat)
    s_copy = pltpu.make_async_copy(s_nat, s_out, sem.at[1])
    s_copy.start()
    np_copy.wait()
    s_copy.wait()


def solution(mesh):
    n_gx, n_gy = mesh.shape["gx"], mesh.shape["gy"]
    vmem = pl.BlockSpec(memory_space=pltpu.VMEM)
    anywhere = pl.BlockSpec(memory_space=pltpu.HBM)

    def body(perm, facies, fpor, fmob, pressure, saturation, basis, bx_map, by_map, well_cells, well_rates):
        assert pressure.shape == (NZ, NXL, NYL)
        flat = [a.reshape(NZ * NXL, NYL) for a in (perm, facies, pressure, saturation, basis)]
        sizes = (n_gx, n_gy, by_map.shape[0])
        wide = pltpu.VMEM((GROUPS, EXT, 128), f32)
        cells_in = lambda kind=f32: pltpu.VMEM((NZ * NXL, NYL), kind)
        natural = [cells_in(), cells_in(jnp.int32), cells_in(), cells_in(), cells_in()]
        facies_tables = [pltpu.SMEM(fpor.shape, f32), pltpu.SMEM(fmob.shape, f32)]
        in_vmem = lambda v: pltpu.with_memory_space_constraint(v, pltpu.VMEM)
        in_hbm = lambda v: pltpu.with_memory_space_constraint(v, pltpu.HBM)
        edge = pltpu.VMEM((2, 3 * NZ, NYL), f32)
        results = pl.pallas_call(
            lambda *refs: comm_kernel(sizes, *refs),
            name="exchange",
            out_shape=[wide] * 7,
            in_specs=[anywhere] * 11,
            out_specs=[vmem] * 7,
            scratch_shapes=natural + [
                pltpu.VMEM((n_gy, NYL), jnp.int32),
                pltpu.VMEM((1, well_cells.shape[0]), jnp.int32),
                pltpu.VMEM((1, well_cells.shape[0]), f32),
                pltpu.SMEM(bx_map.shape, jnp.int32),
            ] + facies_tables + [
                pltpu.SemaphoreType.DMA((11,)),
                cells_in(), cells_in(),
                pltpu.VMEM((5, GROUPS, EXT, 128), f32),
                pltpu.VMEM((2, 5, GROUPS, 8, 128), f32),
                edge, edge,
                pltpu.VMEM((2, 8, 128), f32),
                pltpu.VMEM((2, 8, 128), f32),
                pltpu.VMEM((2 * REACH + 1, ROWS_C, 128), f32),
                pltpu.VMEM((2 * REACH + 1, 8, 128), f32),
                pltpu.VMEM((2 * REACH + 1, 8, 128), f32),
                pltpu.SemaphoreType.DMA((4,)),
                pltpu.SemaphoreType.DMA((4,)),
                pltpu.SemaphoreType.DMA((12,)),
                pltpu.SemaphoreType.DMA((12,)),
                pltpu.SemaphoreType.DMA((27,)),
                pltpu.SemaphoreType.DMA((27,)),
            ],
            compiler_params=pltpu.CompilerParams(collective_id=0, has_side_effects=True, vmem_limit_bytes=32 << 20),
        )(
            *[in_hbm(v) for v in (
                *flat, by_map.reshape(n_gy, NYL), well_cells.reshape(1, -1), well_rates.reshape(1, -1), bx_map, fpor, fmob
            )]
        )
        shape = jax.ShapeDtypeStruct((NZ * NXL, NYL), f32)
        new_pressure, water = pl.pallas_call(
            transport_kernel,
            name="transport",
            out_shape=[shape, shape],
            in_specs=[vmem] * 7,
            out_specs=[anywhere] * 2,
            scratch_shapes=[
                pltpu.VMEM((GROUPS, EXT, 128), f32),
                pltpu.VMEM((GROUPS, EXT + 16, 128), f32),
                pltpu.VMEM((8, GROUPS, EXT, 128), f32),
                cells_in(), cells_in(),
                pltpu.SemaphoreType.DMA((2,)),
            ],
            compiler_params=pltpu.CompilerParams(vmem_limit_bytes=32 << 20),
        )(*[in_vmem(v) for v in results])
        return new_pressure.reshape(pressure.shape), water.reshape(pressure.shape)

    cells = P("member", "gx", "gy")
    return jax.shard_map(
        body,
        mesh=mesh,
        in_specs=(cells, cells, P(), P(), cells, cells, cells, P("member"), P("member"), P("member"), P("member")),
        out_specs=(cells, cells),
        check_vma=False,
    )
```

```python
import jax
import jax.numpy as jnp
from jax import lax
from jax.experimental import pallas as pl
from jax.experimental.pallas import tpu as pltpu
from jax.sharding import PartitionSpec as P

NZ = 32
BX = 8
BY = 8
BZ = 4
NSWEEP = 3
NSUB = 4
NFAC = 4
NXL = 8
NYL = 128
EXT = NYL + 8
GROUPS = 4
ROWS_C = 24
REACH = 4
CHUNK = 16

time_step = 0.005
f32 = jnp.float32
bf16 = jnp.bfloat16
M, PR, B, PHI, S = range(5)


def iota(shape, dim):
    return lax.broadcasted_iota(jnp.int32, shape, dim)


def harmonic(left, right):
    total = left + right
    return 2.0 * left * right / jnp.where(total > 0, total, 1.0)


def split2(v):
    hi = v.astype(bf16)
    return hi, (v - hi.astype(f32)).astype(bf16)


def split3(v):
    hi = v.astype(bf16)
    rest = v - hi.astype(f32)
    mid = rest.astype(bf16)
    return hi, mid, (rest - mid.astype(f32)).astype(bf16)


def nn(a, b):
    return lax.dot_general(a, b, (((1,), (0,)), ((), ())), preferred_element_type=f32)


def nt(a, b):
    return lax.dot_general(a, b, (((1,), (1,)), ((), ())), preferred_element_type=f32)


def roll(v, shift, axis):
    return pltpu.roll(v, shift % v.shape[axis], axis)


def next_x(here, after):
    lane = iota(here.shape, 1)
    return jnp.where(lane < 96, roll(here, -32, 1), roll(after, -32, 1))


def prev_x(here, before):
    lane = iota(here.shape, 1)
    return jnp.where(lane >= 32, roll(here, 32, 1), roll(before, 32, 1))


def fetch_properties(perm, fac, sat, fpor, fmob, mob, por):
    region = fac[...]
    s_nat = sat[...]
    fm = jnp.zeros(region.shape, f32)
    fp = jnp.zeros(region.shape, f32)
    for level in range(NFAC):
        fm = jnp.where(region == level, fmob[level], fm)
        fp = jnp.where(region == level, fpor[level], fp)
    mob[...] = perm[...] * fm * (s_nat * s_nat + (1.0 - s_nat) * (1.0 - s_nat) * 0.25)
    por[...] = fp


def turned(ref, g):
    block = jnp.concatenate([ref[pl.ds(4 * (g - 1) + i, NZ, NXL), :] for i in range(4)], axis=0)
    return block.T


def edge_rows(ref, x):
    return jnp.concatenate([ref[pl.ds(x + NXL * i, NZ // BZ, NXL * BZ), :] for i in range(BZ)], axis=0)


class Copy:
    def __init__(self, src, dst, send, recv, target, goes, comes):
        self.goes, self.comes = goes, comes
        self.copy = pltpu.make_async_remote_copy(
            src_ref=src, dst_ref=dst, send_sem=send, recv_sem=recv, device_id=target, device_id_type=pl.DeviceIdType.MESH
        )

    def start(self):
        pl.when(self.goes)(lambda: self.copy.start())

    def wait_send(self):
        pl.when(self.goes)(lambda: self.copy.wait_send())

    def wait_recv(self):
        pl.when(self.comes)(lambda: self.copy.wait_recv())


def comm_kernel(
    sizes,
    perm_h, fac_h, pres_h, sat_h, bas_h, bymap_h, wells_h, rates_h, bxmap_h, fpor_h, fmob_h,
    tx_out, ty_out, tz_out, s_out, w_out, src_out, newp,
    perm, fac, pres, sat, bas, bymap, wells, rates, bxmap, fpor, fmob, in_sem,
    mob, por, E, yh, xs, xr, ys, yr, ps, low, high,
    send_a, recv_a, send_h, recv_h, send_c, recv_c,
):
    n_gx, n_gy, full_y = sizes
    gx = lax.axis_index("gx")
    gy = lax.axis_index("gy")

    def there(dx, dy):
        ok = jnp.bool_(True)
        if dx:
            ok = ok & (gx + dx >= 0) & (gx + dx < n_gx)
        if dy:
            ok = ok & (gy + dy >= 0) & (gy + dy < n_gy)
        return ok

    def where_is(dx, dy):
        return {"gx": gx + dx, "gy": gy + dy}

    partners = [(dx, dy) for dx in range(-REACH, REACH + 1) for dy in (-1, 0, 1) if (dx, dy) != (0, 0)]
    partners.sort(key=lambda d: (0, abs(d[0]) + 2 * abs(d[1])) if abs(d[0]) + 2 * abs(d[1]) < 4 else (1, -abs(d[0]) - abs(d[1])))

    inputs = [
        pltpu.make_async_copy(src, dst, in_sem.at[i])
        for i, (src, dst) in enumerate(zip(
            (sat_h, fac_h, perm_h, fpor_h, fmob_h, pres_h, bas_h, bxmap_h, bymap_h, wells_h, rates_h),
            (sat, fac, perm, fpor, fmob, pres, bas, bxmap, bymap, wells, rates),
        ))
    ]
    for copy in inputs:
        copy.start()

    barrier = pltpu.get_barrier_semaphore()
    for dx, dy in partners:
        @pl.when(there(dx, dy))
        def _(dx=dx, dy=dy):
            pl.semaphore_signal(barrier, inc=1, device_id=where_is(dx, dy), device_id_type=pl.DeviceIdType.MESH)

    for copy in inputs[:5]:
        copy.wait()
    fetch_properties(perm, fac, sat, fpor, fmob, mob, por)
    for copy in inputs[5:7]:
        copy.wait()

    def turn(pairs):
        for f, ref in pairs:
            for g in (1, 2):
                E[f, g, 0:NYL, :] = turned(ref, g)

    turn(((M, mob), (PR, pres), (B, bas)))
    ys[...] = jnp.zeros_like(ys)
    for side, y in ((0, 0), (1, NYL - 1)):
        for k, f in enumerate((M, PR, B)):
            for g in (1, 2):
                ys[side, 2 * k + g - 1 : 2 * k + g, :] = E[f, g, y : y + 1, :]
    own_edge = []
    for x in (0, NXL - 1):
        own_edge.append([edge_rows(ref, x) for ref in (mob, pres, bas)])
    for side in (0, 1):
        for k in range(3):
            xs[side, NZ * k : NZ * (k + 1)] = own_edge[side][k]

    span_x = lax.min(gx, REACH) + lax.min(n_gx - 1 - gx, REACH) + 1
    span_y = lax.min(gy, 1) + lax.min(n_gy - 1 - gy, 1) + 1
    pl.semaphore_wait(barrier, span_x * span_y - 1)

    def to(src, dst, sends, recvs, slot_out, slot_in, dx, dy):
        return Copy(src, dst, sends.at[slot_out], recvs.at[slot_in], where_is(dx, dy), there(dx, dy), there(-dx, -dy))

    edges = [
        to(ys.at[0], yr.at[1], send_a, recv_a, 3, 3, 0, -1),
        to(xs.at[0], xr.at[1], send_a, recv_a, 1, 1, -1, 0),
        to(ys.at[1], yr.at[0], send_a, recv_a, 2, 2, 0, 1),
        to(xs.at[1], xr.at[0], send_a, recv_a, 0, 0, 1, 0),
    ]
    for copy in edges:
        copy.start()

    up, down = slice(NYL - 8, NYL), slice(0, 8)
    every = slice(0, 5)
    halo = [
        to(E.at[every, 1:3, up], yh.at[0, every, 1:3], send_h, recv_h, 4, 4, 0, 1),
        to(E.at[every, 1:3, down], yh.at[1, every, 1:3], send_h, recv_h, 5, 5, 0, -1),
        to(E.at[every, 2, up], yh.at[0, every, 0], send_h, recv_h, 6, 6, 1, 1),
        to(E.at[every, 1, up], yh.at[0, every, 3], send_h, recv_h, 7, 7, -1, 1),
        to(E.at[every, 2, down], yh.at[1, every, 0], send_h, recv_h, 8, 8, 1, -1),
        to(E.at[every, 1, down], yh.at[1, every, 3], send_h, recv_h, 9, 9, -1, -1),
    ]

    def halo_x(k, fields):
        return [
            to(E.at[fields, 2, 0:NYL], E.at[fields, 0, 0:NYL], send_h, recv_h, 2 * k, 2 * k, 1, 0),
            to(E.at[fields, 1, 0:NYL], E.at[fields, 3, 0:NYL], send_h, recv_h, 2 * k + 1, 2 * k + 1, -1, 0),
        ]

    halo_first = halo_x(0, slice(M, M + 1))
    halo_next = halo_x(1, slice(PR, B + 1))
    halo_last = halo_x(5, slice(PHI, S + 1))
    for copy in halo_first + halo_next:
        copy.start()
    turn(((S, sat), (PHI, por)))
    for copy in halo:
        copy.start()
    for copy in inputs[7:]:
        copy.wait()

    def clear_if(missing, *parts):
        @pl.when(missing)
        def _():
            for ref, where in parts:
                ref[where] = jnp.zeros(ref.at[where].shape, f32)

    whole = slice(None)
    clear_if(gx == 0, (xr, 0), (E, (whole, 0)), (yh, (whole, whole, 0)))
    clear_if(gx == n_gx - 1, (xr, 1), (E, (whole, 3)), (yh, (whole, whole, 3)))
    clear_if(gy == 0, (yr, 0), (yh, 0), (low, whole))
    clear_if(gy == n_gy - 1, (yr, 1), (yh, 1), (high, whole))
    for dx in range(1, REACH + 1):
        for k, missing in ((REACH - dx, gx - dx < 0), (REACH + dx, gx + dx >= n_gx)):
            clear_if(missing, (ps, k), (low, k), (high, k))

    well_y = wells[...] % full_y
    well_x = wells[...] // full_y
    n_wells = wells.shape[1]
    row = iota((EXT, 1), 0)
    y_here = gy * NYL + jnp.where(row < NYL + 4, row, row - EXT)
    hits_y = (y_here == well_y).astype(f32).astype(bf16)
    x_here = gx * NXL - 4 + iota((16, 1), 0)
    hits_x = jnp.where(x_here == well_x, rates[...], 0.0)
    col = nt(hits_y, jnp.concatenate(split3(hits_x), axis=0))
    col = (col[:, 0:16] + col[:, 16:32] + col[:, 32:48]) * (1.0 / NZ)
    lane = iota((16, 512), 1)
    spread = (lane // NZ == iota((16, 512), 0)).astype(f32).astype(bf16)
    src = nn(jnp.concatenate(split3(col), axis=1), jnp.concatenate([spread] * 3, axis=0))
    for g in range(GROUPS):
        src_out[g] = src[:, 128 * g : 128 * (g + 1)]

    blocks_y = NYL // BY
    map_own = bymap[pl.ds(gy, 1), :] - (gy * blocks_y - 4)
    map_up = bymap[pl.ds(lax.min(gy + 1, n_gy - 1), 1), :] - (gy * blocks_y - 4)
    map_down = bymap[pl.ds(lax.max(gy - 1, 0), 1), :] - (gy * blocks_y - 4)
    sum_y = (iota((ROWS_C, NYL), 0) == map_own).astype(f32).astype(bf16)
    sum_y = jnp.concatenate([sum_y, sum_y], axis=1)

    def column_of(values):
        return jnp.broadcast_to(values.astype(f32), (128, 128)).T

    by_row = column_of(map_own)
    by_up = column_of(map_up)[0:8]
    by_down = column_of(map_down)[120:128]
    by_ext = jnp.concatenate([by_row, jnp.where(iota((8, 128), 0) < 4, by_up, by_down)], axis=0)
    spread_y = (by_ext[:, 0:ROWS_C] == iota((EXT, ROWS_C), 1).astype(f32)).astype(f32).astype(bf16)
    same_y = (by_row == jnp.concatenate([by_row[1:], by_row[:1]], axis=0)).astype(f32)

    kx = [bxmap[lax.clamp(0, gx * NXL - 4 + i, n_gx * NXL - 1)] - gx for i in range(16)]

    def lanes_of(values, shape):
        which = iota(shape, 1) // NZ
        total = jnp.zeros(shape, jnp.int32)
        for i, value in enumerate(values):
            total = jnp.where(which == i, value, total)
        return total

    z_block = (iota((1, 256), 1) % NZ) // BZ
    target = (lanes_of(kx[4:12], (1, 256)) + 1) * 8 + z_block
    sum_xz = (iota((128, 256), 0) == target).astype(f32).astype(bf16)
    sum_xz = jnp.concatenate([sum_xz, sum_xz], axis=1)

    lane128 = iota((NYL, 128), 1)
    row128 = iota((NYL, 128), 0)
    z_of = lane128 % NZ
    m = [E[M, g, 0:NYL, :] for g in (1, 2)]
    p = [E[PR, g, 0:NYL, :] for g in (1, 2)]
    b = [E[B, g, 0:NYL, :] for g in (1, 2)]
    phi = [E[PHI, g, 0:NYL, :] for g in (1, 2)]
    own_src = [src[0:NYL, 128 * g : 128 * (g + 1)] for g in (1, 2)]
    same_x = [lanes_of([(kx[4 + 4 * g + i] == kx[5 + 4 * g + i]).astype(jnp.int32) for i in range(4)], (1, 128)) for g in (0, 1)]

    def nx_(v, g):
        return next_x(v[0], v[1]) if g == 0 else roll(v[1], -32, 1)

    def ny_(v):
        return roll(v, -1, 0)

    def nz_(v):
        return roll(v, -1, 1)

    tx = [harmonic(m[0], nx_(m, 0)), jnp.where(lane128 < 96, harmonic(m[1], nx_(m, 1)), 0.0)]
    ty = [jnp.where(row128 < NYL - 1, harmonic(v, ny_(v)), 0.0) for v in m]
    tz = [jnp.where(z_of < NZ - 1, 0.1 * harmonic(v, nz_(v)), 0.0) for v in m]
    qx = [tx[g] * (p[g] - nx_(p, g)) for g in (0, 1)]
    sums = []
    for g in (0, 1):
        qy = ty[g] * (p[g] - ny_(p[g]))
        qz = tz[g] * (p[g] - nz_(p[g]))
        in_x = prev_x(qx[g], qx[0]) if g == 1 else jnp.where(lane128 >= 32, roll(qx[0], 32, 1), 0.0)
        t_in_x = prev_x(tx[g], tx[0]) if g == 1 else jnp.where(lane128 >= 32, roll(tx[0], 32, 1), 0.0)
        out = qx[g] - in_x + qy - roll(qy, 1, 0) + qz - roll(qz, 1, 1)
        resid = b[g] * (own_src[g] - out)
        cond = tx[g] + t_in_x + ty[g] + roll(ty[g], 1, 0) + tz[g] + roll(tz[g], 1, 1)
        cx = tx[g] * b[g] * nx_(b, g)
        cy = ty[g] * b[g] * ny_(b[g])
        cz = tz[g] * b[g] * nz_(b[g])
        keep_x = same_x[g].astype(f32)
        keep_z = (z_of % BZ != BZ - 1).astype(f32)
        diag = b[g] * b[g] * (0.5 * phi[g] + cond) - 2.0 * (cx * keep_x + cy * same_y + cz * keep_z)
        sums.append((resid, diag, cz * (1.0 - keep_z), cx * (1.0 - keep_x), cy * (1.0 - same_y)))
    inner = []
    for q in range(5):
        hi, mid = split2(jnp.concatenate([sums[0][q], sums[1][q]], axis=1))
        inner.append(nn(sum_y, jnp.concatenate([hi, mid], axis=0)))

    hi, mid = split2(jnp.concatenate(inner, axis=0))
    partial = nt(jnp.concatenate([hi, mid], axis=1), sum_xz)
    inside = partial[0:ROWS_C]
    for q in range(1, 5):
        inside = inside + roll(partial[ROWS_C * q : ROWS_C * (q + 1)], 24 * q, 1)
    target = (lanes_of(kx[4:12], (1, 256)) + 1) * 8 + z_block
    sum_rows = jnp.concatenate(
        [(iota((128, 256), 0) == target + 24 * q).astype(f32).astype(bf16) for q in (0, 1, 4)] * 2, axis=1
    )

    k_low, k_high, k_next = kx[4], kx[11], kx[12]
    together = k_high == k_next
    for copy in edges:
        copy.wait_recv()

    m0, p0, b0 = [xr[0, NZ * k : NZ * (k + 1)] for k in range(3)]
    m1, p1, b1 = [xr[1, NZ * k : NZ * (k + 1)] for k in range(3)]
    (om0, op0, ob0), (om1, op1, ob1) = own_edge
    t1 = harmonic(om1, m1)
    t0 = harmonic(om0, m0)

    def layers(v):
        return v[0:8] + v[8:16] + v[16:24] + v[24:32]

    r1, d1, c1 = layers(-ob1 * t1 * (op1 - p1)), layers(ob1 * ob1 * t1), layers(ob1 * b1 * t1)
    r0, d0 = layers(-ob0 * t0 * (op0 - p0)), layers(ob0 * ob0 * t0)
    nothing = jnp.zeros((8, 128), f32)
    d1 = d1 - 2.0 * jnp.where(together, c1, nothing)
    c1 = jnp.where(together, nothing, c1)
    placed = []
    for high_part, low_part in ((r1, r0), (d1, d0), (nothing, nothing), (c1, nothing), (nothing, nothing)):
        for k in (-1, 0, 1):
            placed.append(jnp.where(k_high == k, high_part, nothing) + jnp.where(k_low == k, low_part, nothing))
    hi, mid = split2(jnp.concatenate(placed + [nothing], axis=0))
    mine = nt(sum_y, jnp.concatenate([hi, mid], axis=1))

    def wide(ref, side, k):
        return jnp.concatenate([ref[side, 2 * k : 2 * k + 1, :], ref[side, 2 * k + 1 : 2 * k + 2, :]], axis=1)

    um, up_, ub = [wide(yr, 1, k) for k in range(3)]
    dm, dp, db = [wide(yr, 0, k) for k in range(3)]
    om1, op1, ob1 = [wide(ys, 1, k) for k in range(3)]
    om0, op0, ob0 = [wide(ys, 0, k) for k in range(3)]
    t1 = harmonic(om1, um)
    t0 = harmonic(om0, dm)
    rows = iota((ROWS_C, 1), 0)
    r_high = by_row[NYL - 1 : NYL, 0:1].astype(jnp.int32)
    r_low = by_row[0:1, 0:1].astype(jnp.int32)
    r_next = by_up[0:1, 0:1].astype(jnp.int32)
    at_high = rows == r_high
    at_low = rows == r_low
    same = r_high == r_next
    couple = ob1 * ub * t1
    zero = jnp.zeros_like(couple)
    at_top = jnp.concatenate(
        [-ob1 * t1 * (op1 - up_), ob1 * ob1 * t1 - 2.0 * jnp.where(same, couple, zero), jnp.where(same, zero, couple)], axis=1
    )
    at_bottom = jnp.concatenate([-ob0 * t0 * (op0 - dp), ob0 * ob0 * t0, zero], axis=1)
    both = jnp.where(iota((8, 768), 0) == 0, at_top, at_bottom)
    hi, mid = split2(both)
    edge_y = nt(jnp.concatenate([hi, mid], axis=1), sum_rows)
    mine = mine + jnp.where(at_high, edge_y[0:1], 0.0) + jnp.where(at_low, edge_y[1:2], 0.0)
    mine = mine + inside
    ps[REACH] = mine

    def slot(dx):
        return REACH + dx

    coarse = {}
    for dx in range(-REACH, REACH + 1):
        if dx:
            coarse[dx, 0] = to(ps.at[slot(0)], ps.at[slot(-dx)], send_c, recv_c, slot(dx), slot(-dx), dx, 0)
        coarse[dx, 1] = to(
            ps.at[slot(0), 16:24], low.at[slot(-dx)], send_c, recv_c, 9 + slot(dx), 9 + slot(-dx), dx, 1
        )
        coarse[dx, -1] = to(
            ps.at[slot(0), 0:8], high.at[slot(-dx)], send_c, recv_c, 18 + slot(dx), 18 + slot(-dx), dx, -1
        )
    for dx in (-1, -2, -3, -4, 0, 1, 2, 3, 4):
        for dy in (0, -1, 1):
            if (dx, dy) in coarse:
                coarse[dx, dy].start()
    for copy in halo_last:
        copy.start()

    target = (lanes_of(kx, (1, 512)) + 3) * 8 + (iota((1, 512), 1) % NZ) // BZ
    spread_xz = (iota((64, 512), 0) == target).astype(f32).astype(bf16)
    spread_xz = jnp.concatenate([spread_xz] * 2, axis=0)

    for copy in halo_first + halo:
        copy.wait_recv()
    take_up = iota((8, 128), 0) < 4
    for f in range(5):
        for g in range(GROUPS):
            E[f, g, NYL:EXT, :] = jnp.where(take_up, yh[1, f, g], yh[0, f, g])

    z_ext = iota((EXT, 128), 1) % NZ
    for g in range(GROUPS):
        after = min(g + 1, GROUPS - 1)
        here = E[M, g]
        tx_out[g] = harmonic(here, next_x(here, E[M, after]))
        ty_out[g] = harmonic(here, roll(here, -1, 0))
        tz_out[g] = jnp.where(z_ext < NZ - 1, 0.1 * harmonic(here, roll(here, -1, 1)), 0.0)

    def finish(g):
        s_out[g] = E[S, g]
        phi_here = E[PHI, g]
        w_out[g] = time_step / jnp.where(phi_here > 0, phi_here, 1.0)

    finish(1)
    finish(2)

    lane24 = iota((ROWS_C, 128), 1)
    system = [jnp.zeros((ROWS_C, 128), f32) for _ in range(5)]
    for dx in sorted(range(-REACH, REACH + 1), key=abs):
        for dy in (-1, 0, 1):
            if (dx, dy) in coarse:
                coarse[-dx, -dy].wait_recv()
        k = slot(dx)
        part = jnp.concatenate([ps[k, 0:8] + low[k], ps[k, 8:16], ps[k, 16:24] + high[k]], axis=0)
        first = (dx + 2) * 8
        take = (lane24 >= max(first, 0)) & (lane24 < min(first + 24, 56))
        for q in range(2 if abs(dx) == REACH else 5):
            system[q] = system[q] + jnp.where(take, roll(part, first - 24 * q, 1), 0.0)
    resid, diag, cz, cx, cy = system
    diag = jnp.where(diag > 0, diag, 1.0)
    half = 0.5 / diag
    fixed = half * resid
    estimate = fixed
    for _ in range(NSWEEP - 1):
        flow = (
            cz * roll(estimate, -1, 1) + roll(cz * estimate, 1, 1)
            + cx * roll(estimate, -8, 1) + roll(cx * estimate, 8, 1)
            + cy * roll(estimate, -1, 0) + roll(cy * estimate, 1, 0)
        )
        estimate = 0.5 * estimate + fixed + half * flow
    row24 = iota((ROWS_C, 128), 0)
    wanted = (row24 >= 3) & (row24 < 21) & (lane24 >= 16) & (lane24 < 40)
    estimate = jnp.where(wanted, estimate, 0.0)[:, 0:64]
    spread1 = nn(jnp.concatenate(split2(estimate), axis=1), spread_xz)
    fine = nn(jnp.concatenate([spread_y] * 2, axis=1), jnp.concatenate(split2(spread1), axis=0))

    for copy in halo_next:
        copy.wait_recv()
    for g in range(GROUPS):
        newp[g] = E[PR, g] + E[B, g] * fine[:, 128 * g : 128 * (g + 1)]
    for copy in halo_last:
        copy.wait_recv()
    finish(0)
    finish(3)
    for copy in edges + halo + halo_first + halo_next + halo_last + list(coarse.values()):
        copy.wait_send()


def transport_kernel(tx, ty, tz, s_in, w_in, src, newp, np_out, s_out, s, F, C, np_nat, s_nat, sem):
    first, last_row = 8, 8 + EXT - 1
    lane = iota((EXT, 128), 1)

    def to_next(rolled, g):
        return jnp.where(lane < 96, rolled[g], rolled[min(g + 1, GROUPS - 1)])

    def to_prev(rolled, g):
        return jnp.where(lane >= 32, rolled[g], rolled[max(g - 1, 0)])

    def put(block, g, dst):
        back = block.T
        for i in range(4):
            dst[pl.ds(4 * (g - 1) + i, NZ, NXL), :] = back[NZ * i : NZ * (i + 1)]

    for g in (1, 2):
        put(newp[g, 0:NYL, :], g, np_nat)
    np_copy = pltpu.make_async_copy(np_nat, np_out, sem.at[0])
    np_copy.start()

    rolled = [roll(newp[g], -32, 1) for g in range(GROUPS)]
    fx = [tx[g] * (newp[g] - to_next(rolled, g)) for g in range(GROUPS)]
    rolled = [roll(v, 32, 1) for v in fx]
    for g in range(GROUPS):
        here = newp[g]
        w = w_in[g]
        source = src[g]
        fx_up = fx[g]
        fx_down = to_prev(rolled, g)
        fy_up = ty[g] * (here - roll(here, -1, 0))
        fy_down = roll(fy_up, 1, 0)
        fz_up = tz[g] * (here - roll(here, -1, 1))
        fz_down = roll(fz_up, 1, 1)
        C[0, g] = w * jnp.maximum(source, 0.0)
        leaves = jnp.minimum(source, 0.0)
        for k, (up, down) in enumerate(((fx_up, fx_down), (fy_up, fy_down), (fz_up, fz_down))):
            from_up = jnp.maximum(-up, 0.0)
            from_down = jnp.maximum(down, 0.0)
            C[2 + 2 * k, g] = w * from_up
            C[3 + 2 * k, g] = w * from_down
            leaves = leaves - (up + from_up) + (down - from_down)
        C[1, g] = w * leaves

    for step in range(NSUB):
        last = step == NSUB - 1
        for g in range(GROUPS):
            for a in range(0, EXT, CHUNK):
                b = min(a + CHUNK, EXT)
                v = s_in[g, a:b] if step == 0 else s[g, a:b]
                wet = v * v
                F[g, first + a : first + b] = wet / (wet + (1.0 - v) * (1.0 - v) * 0.25)
            F[g, first - 1 : first] = F[g, last_row : last_row + 1]
            F[g, last_row + 1 : last_row + 2] = F[g, first : first + 1]
        end = NYL if last else EXT
        for a in range(0, end, CHUNK):
            b = min(a + CHUNK, end)
            here = [F[g, first + a : first + b] for g in range(GROUPS)]
            mask_next, mask_prev = lane[a:b] < 96, lane[a:b] >= 32
            ups = [None if last and g == 0 else roll(f, -32, 1) for g, f in enumerate(here)]
            downs = [None if last and g == 3 else roll(f, 32, 1) for g, f in enumerate(here)]
            for g in (1, 2) if last else range(GROUPS):
                v = s_in[g, a:b] if step == 0 else s[g, a:b]
                v = v + C[0, g, a:b] + C[1, g, a:b] * here[g]
                v = v + C[4, g, a:b] * F[g, first + a + 1 : first + b + 1]
                v = v + C[5, g, a:b] * F[g, first + a - 1 : first + b - 1]
                v = v + C[2, g, a:b] * jnp.where(mask_next, ups[g], ups[min(g + 1, GROUPS - 1)])
                v = v + C[3, g, a:b] * jnp.where(mask_prev, downs[g], downs[max(g - 1, 0)])
                v = v + C[6, g, a:b] * roll(here[g], -1, 1) + C[7, g, a:b] * roll(here[g], 1, 1)
                s[g, a:b] = v
    for g in (1, 2):
        put(s[g, 0:NYL, :], g, s_nat)
    s_copy = pltpu.make_async_copy(s_nat, s_out, sem.at[1])
    s_copy.start()
    np_copy.wait()
    s_copy.wait()


def solution(mesh):
    n_gx, n_gy = mesh.shape["gx"], mesh.shape["gy"]
    vmem = pl.BlockSpec(memory_space=pltpu.VMEM)
    anywhere = pl.BlockSpec(memory_space=pltpu.HBM)

    def body(perm, facies, fpor, fmob, pressure, saturation, basis, bx_map, by_map, well_cells, well_rates):
        assert pressure.shape == (NZ, NXL, NYL)
        flat = [a.reshape(NZ * NXL, NYL) for a in (perm, facies, pressure, saturation, basis)]
        sizes = (n_gx, n_gy, by_map.shape[0])
        wide = pltpu.VMEM((GROUPS, EXT, 128), f32)
        cells_in = lambda kind=f32: pltpu.VMEM((NZ * NXL, NYL), kind)
        natural = [cells_in(), cells_in(jnp.int32), cells_in(), cells_in(), cells_in()]
        facies_tables = [pltpu.SMEM(fpor.shape, f32), pltpu.SMEM(fmob.shape, f32)]
        in_vmem = lambda v: pltpu.with_memory_space_constraint(v, pltpu.VMEM)
        in_hbm = lambda v: pltpu.with_memory_space_constraint(v, pltpu.HBM)
        edge = pltpu.VMEM((2, 3 * NZ, NYL), f32)
        results = pl.pallas_call(
            lambda *refs: comm_kernel(sizes, *refs),
            name="exchange",
            out_shape=[wide] * 7,
            in_specs=[anywhere] * 11,
            out_specs=[vmem] * 7,
            scratch_shapes=natural + [
                pltpu.VMEM((n_gy, NYL), jnp.int32),
                pltpu.VMEM((1, well_cells.shape[0]), jnp.int32),
                pltpu.VMEM((1, well_cells.shape[0]), f32),
                pltpu.SMEM(bx_map.shape, jnp.int32),
            ] + facies_tables + [
                pltpu.SemaphoreType.DMA((11,)),
                cells_in(), cells_in(),
                pltpu.VMEM((5, GROUPS, EXT, 128), f32),
                pltpu.VMEM((2, 5, GROUPS, 8, 128), f32),
                edge, edge,
                pltpu.VMEM((2, 8, 128), f32),
                pltpu.VMEM((2, 8, 128), f32),
                pltpu.VMEM((2 * REACH + 1, ROWS_C, 128), f32),
                pltpu.VMEM((2 * REACH + 1, 8, 128), f32),
                pltpu.VMEM((2 * REACH + 1, 8, 128), f32),
                pltpu.SemaphoreType.DMA((4,)),
                pltpu.SemaphoreType.DMA((4,)),
                pltpu.SemaphoreType.DMA((12,)),
                pltpu.SemaphoreType.DMA((12,)),
                pltpu.SemaphoreType.DMA((27,)),
                pltpu.SemaphoreType.DMA((27,)),
            ],
            compiler_params=pltpu.CompilerParams(collective_id=0, has_side_effects=True, vmem_limit_bytes=32 << 20),
        )(
            *[in_hbm(v) for v in (
                *flat, by_map.reshape(n_gy, NYL), well_cells.reshape(1, -1), well_rates.reshape(1, -1), bx_map, fpor, fmob
            )]
        )
        shape = jax.ShapeDtypeStruct((NZ * NXL, NYL), f32)
        new_pressure, water = pl.pallas_call(
            transport_kernel,
            name="transport",
            out_shape=[shape, shape],
            in_specs=[vmem] * 7,
            out_specs=[anywhere] * 2,
            scratch_shapes=[
                pltpu.VMEM((GROUPS, EXT, 128), f32),
                pltpu.VMEM((GROUPS, EXT + 16, 128), f32),
                pltpu.VMEM((8, GROUPS, EXT, 128), f32),
                cells_in(), cells_in(),
                pltpu.SemaphoreType.DMA((2,)),
            ],
            compiler_params=pltpu.CompilerParams(vmem_limit_bytes=32 << 20),
        )(*[in_vmem(v) for v in results])
        return new_pressure.reshape(pressure.shape), water.reshape(pressure.shape)

    cells = P("member", "gx", "gy")
    return jax.shard_map(
        body,
        mesh=mesh,
        in_specs=(cells, cells, P(), P(), cells, cells, cells, P("member"), P("member"), P("member"), P("member")),
        out_specs=(cells, cells),
        check_vma=False,
    )
```

```python
import jax
import jax.numpy as jnp
from jax import lax
from jax.experimental import pallas as pl
from jax.experimental.pallas import tpu as pltpu
from jax.sharding import PartitionSpec as P

NZ = 32
BX = 8
BY = 8
BZ = 4
NSWEEP = 3
NSUB = 4
NFAC = 4
NXL = 8
NYL = 128
EXT = NYL + 8
GROUPS = 4
ROWS_C = 24
REACH = 4
CHUNK = 16

time_step = 0.005
f32 = jnp.float32
bf16 = jnp.bfloat16
M, PR, B, PHI, S = range(5)


def iota(shape, dim):
    return lax.broadcasted_iota(jnp.int32, shape, dim)


def harmonic(left, right):
    total = left + right
    return 2.0 * left * right / jnp.where(total > 0, total, 1.0)


def split2(v):
    hi = v.astype(bf16)
    return hi, (v - hi.astype(f32)).astype(bf16)


def split3(v):
    hi = v.astype(bf16)
    rest = v - hi.astype(f32)
    mid = rest.astype(bf16)
    return hi, mid, (rest - mid.astype(f32)).astype(bf16)


def nn(a, b):
    return lax.dot_general(a, b, (((1,), (0,)), ((), ())), preferred_element_type=f32)


def nt(a, b):
    return lax.dot_general(a, b, (((1,), (1,)), ((), ())), preferred_element_type=f32)


def roll(v, shift, axis):
    return pltpu.roll(v, shift % v.shape[axis], axis)


def next_x(here, after):
    lane = iota(here.shape, 1)
    return jnp.where(lane < 96, roll(here, -32, 1), roll(after, -32, 1))


def prev_x(here, before):
    lane = iota(here.shape, 1)
    return jnp.where(lane >= 32, roll(here, 32, 1), roll(before, 32, 1))


def fetch_properties(perm, fac, sat, fpor, fmob, mob, por):
    region = fac[...]
    s_nat = sat[...]
    fm = jnp.zeros(region.shape, f32)
    fp = jnp.zeros(region.shape, f32)
    for level in range(NFAC):
        fm = jnp.where(region == level, fmob[level], fm)
        fp = jnp.where(region == level, fpor[level], fp)
    mob[...] = perm[...] * fm * (s_nat * s_nat + (1.0 - s_nat) * (1.0 - s_nat) * 0.25)
    por[...] = fp


def turned(ref, g):
    block = jnp.concatenate([ref[pl.ds(4 * (g - 1) + i, NZ, NXL), :] for i in range(4)], axis=0)
    return block.T


def edge_rows(ref, x):
    return jnp.concatenate([ref[pl.ds(x + NXL * i, NZ // BZ, NXL * BZ), :] for i in range(BZ)], axis=0)


class Copy:
    def __init__(self, src, dst, send, recv, target, goes, comes):
        self.goes, self.comes = goes, comes
        self.copy = pltpu.make_async_remote_copy(
            src_ref=src, dst_ref=dst, send_sem=send, recv_sem=recv, device_id=target, device_id_type=pl.DeviceIdType.MESH
        )

    def start(self):
        pl.when(self.goes)(lambda: self.copy.start())

    def wait_send(self):
        pl.when(self.goes)(lambda: self.copy.wait_send())

    def wait_recv(self):
        pl.when(self.comes)(lambda: self.copy.wait_recv())


def comm_kernel(
    sizes,
    perm_h, fac_h, pres_h, sat_h, bas_h, bymap_h, wells_h, rates_h, bxmap_h, fpor_h, fmob_h,
    tx_out, ty_out, tz_out, s_out, w_out, src_out, newp,
    perm, fac, pres, sat, bas, bymap, wells, rates, bxmap, fpor, fmob, in_sem,
    mob, por, E, yh, xs, xr, ys, yr, ps, low, high,
    send_a, recv_a, send_h, recv_h, send_c, recv_c,
):
    n_gx, n_gy, full_y = sizes
    gx = lax.axis_index("gx")
    gy = lax.axis_index("gy")

    def there(dx, dy):
        ok = jnp.bool_(True)
        if dx:
            ok = ok & (gx + dx >= 0) & (gx + dx < n_gx)
        if dy:
            ok = ok & (gy + dy >= 0) & (gy + dy < n_gy)
        return ok

    def where_is(dx, dy):
        return {"gx": gx + dx, "gy": gy + dy}

    partners = [(dx, dy) for dx in range(-REACH, REACH + 1) for dy in (-1, 0, 1) if (dx, dy) != (0, 0)]
    partners.sort(key=lambda d: -abs(d[0]) - abs(d[1]))

    inputs = [
        pltpu.make_async_copy(src, dst, in_sem.at[i])
        for i, (src, dst) in enumerate(zip(
            (sat_h, fac_h, perm_h, fpor_h, fmob_h, pres_h, bas_h, bxmap_h, bymap_h, wells_h, rates_h),
            (sat, fac, perm, fpor, fmob, pres, bas, bxmap, bymap, wells, rates),
        ))
    ]
    for copy in inputs:
        copy.start()

    barrier = pltpu.get_barrier_semaphore()
    for dx, dy in partners:
        @pl.when(there(dx, dy))
        def _(dx=dx, dy=dy):
            pl.semaphore_signal(barrier, inc=1, device_id=where_is(dx, dy), device_id_type=pl.DeviceIdType.MESH)

    for copy in inputs[:5]:
        copy.wait()
    fetch_properties(perm, fac, sat, fpor, fmob, mob, por)
    for copy in inputs[5:7]:
        copy.wait()

    def turn(pairs):
        for f, ref in pairs:
            for g in (1, 2):
                E[f, g, 0:NYL, :] = turned(ref, g)

    turn(((M, mob), (PR, pres), (B, bas)))
    ys[...] = jnp.zeros_like(ys)
    for side, y in ((0, 0), (1, NYL - 1)):
        for k, f in enumerate((M, PR, B)):
            for g in (1, 2):
                ys[side, 2 * k + g - 1 : 2 * k + g, :] = E[f, g, y : y + 1, :]
    own_edge = []
    for x in (0, NXL - 1):
        own_edge.append([edge_rows(ref, x) for ref in (mob, pres, bas)])
    for side in (0, 1):
        for k in range(3):
            xs[side, NZ * k : NZ * (k + 1)] = own_edge[side][k]

    span_x = lax.min(gx, REACH) + lax.min(n_gx - 1 - gx, REACH) + 1
    span_y = lax.min(gy, 1) + lax.min(n_gy - 1 - gy, 1) + 1
    pl.semaphore_wait(barrier, span_x * span_y - 1)

    def to(src, dst, sends, recvs, slot_out, slot_in, dx, dy):
        return Copy(src, dst, sends.at[slot_out], recvs.at[slot_in], where_is(dx, dy), there(dx, dy), there(-dx, -dy))

    edges = [
        to(ys.at[0], yr.at[1], send_a, recv_a, 3, 3, 0, -1),
        to(xs.at[0], xr.at[1], send_a, recv_a, 1, 1, -1, 0),
        to(ys.at[1], yr.at[0], send_a, recv_a, 2, 2, 0, 1),
        to(xs.at[1], xr.at[0], send_a, recv_a, 0, 0, 1, 0),
    ]
    for copy in edges:
        copy.start()

    up, down = slice(NYL - 8, NYL), slice(0, 8)
    every = slice(0, 5)
    halo = [
        to(E.at[every, 1:3, up], yh.at[0, every, 1:3], send_h, recv_h, 4, 4, 0, 1),
        to(E.at[every, 1:3, down], yh.at[1, every, 1:3], send_h, recv_h, 5, 5, 0, -1),
        to(E.at[every, 2, up], yh.at[0, every, 0], send_h, recv_h, 6, 6, 1, 1),
        to(E.at[every, 1, up], yh.at[0, every, 3], send_h, recv_h, 7, 7, -1, 1),
        to(E.at[every, 2, down], yh.at[1, every, 0], send_h, recv_h, 8, 8, 1, -1),
        to(E.at[every, 1, down], yh.at[1, every, 3], send_h, recv_h, 9, 9, -1, -1),
    ]

    def halo_x(k, fields):
        return [
            to(E.at[fields, 2, 0:NYL], E.at[fields, 0, 0:NYL], send_h, recv_h, 2 * k, 2 * k, 1, 0),
            to(E.at[fields, 1, 0:NYL], E.at[fields, 3, 0:NYL], send_h, recv_h, 2 * k + 1, 2 * k + 1, -1, 0),
        ]

    halo_first = halo_x(0, slice(M, M + 1))
    halo_next = halo_x(1, slice(PR, B + 1))
    halo_last = halo_x(5, slice(PHI, S + 1))
    for copy in halo_first + halo_next:
        copy.start()
    turn(((S, sat), (PHI, por)))
    for copy in halo:
        copy.start()
    for copy in inputs[7:]:
        copy.wait()

    def clear_if(missing, *parts):
        @pl.when(missing)
        def _():
            for ref, where in parts:
                ref[where] = jnp.zeros(ref.at[where].shape, f32)

    whole = slice(None)
    clear_if(gx == 0, (xr, 0), (E, (whole, 0)), (yh, (whole, whole, 0)))
    clear_if(gx == n_gx - 1, (xr, 1), (E, (whole, 3)), (yh, (whole, whole, 3)))
    clear_if(gy == 0, (yr, 0), (yh, 0), (low, whole))
    clear_if(gy == n_gy - 1, (yr, 1), (yh, 1), (high, whole))
    for dx in range(1, REACH + 1):
        for k, missing in ((REACH - dx, gx - dx < 0), (REACH + dx, gx + dx >= n_gx)):
            clear_if(missing, (ps, k), (low, k), (high, k))

    well_y = wells[...] % full_y
    well_x = wells[...] // full_y
    n_wells = wells.shape[1]
    row = iota((EXT, 1), 0)
    y_here = gy * NYL + jnp.where(row < NYL + 4, row, row - EXT)
    hits_y = (y_here == well_y).astype(f32).astype(bf16)
    x_here = gx * NXL - 4 + iota((16, 1), 0)
    hits_x = jnp.where(x_here == well_x, rates[...], 0.0)
    col = nt(hits_y, jnp.concatenate(split3(hits_x), axis=0))
    col = (col[:, 0:16] + col[:, 16:32] + col[:, 32:48]) * (1.0 / NZ)
    lane = iota((16, 512), 1)
    spread = (lane // NZ == iota((16, 512), 0)).astype(f32).astype(bf16)
    src = nn(jnp.concatenate(split3(col), axis=1), jnp.concatenate([spread] * 3, axis=0))
    for g in range(GROUPS):
        src_out[g] = src[:, 128 * g : 128 * (g + 1)]

    blocks_y = NYL // BY
    map_own = bymap[pl.ds(gy, 1), :] - (gy * blocks_y - 4)
    map_up = bymap[pl.ds(lax.min(gy + 1, n_gy - 1), 1), :] - (gy * blocks_y - 4)
    map_down = bymap[pl.ds(lax.max(gy - 1, 0), 1), :] - (gy * blocks_y - 4)
    sum_y = (iota((ROWS_C, NYL), 0) == map_own).astype(f32).astype(bf16)
    sum_y = jnp.concatenate([sum_y, sum_y], axis=1)

    def column_of(values):
        return jnp.broadcast_to(values.astype(f32), (128, 128)).T

    by_row = column_of(map_own)
    by_up = column_of(map_up)[0:8]
    by_down = column_of(map_down)[120:128]
    by_ext = jnp.concatenate([by_row, jnp.where(iota((8, 128), 0) < 4, by_up, by_down)], axis=0)
    spread_y = (by_ext[:, 0:ROWS_C] == iota((EXT, ROWS_C), 1).astype(f32)).astype(f32).astype(bf16)
    same_y = (by_row == jnp.concatenate([by_row[1:], by_row[:1]], axis=0)).astype(f32)

    kx = [bxmap[lax.clamp(0, gx * NXL - 4 + i, n_gx * NXL - 1)] - gx for i in range(16)]

    def lanes_of(values, shape):
        which = iota(shape, 1) // NZ
        total = jnp.zeros(shape, jnp.int32)
        for i, value in enumerate(values):
            total = jnp.where(which == i, value, total)
        return total

    z_block = (iota((1, 256), 1) % NZ) // BZ
    target = (lanes_of(kx[4:12], (1, 256)) + 1) * 8 + z_block
    sum_xz = (iota((128, 256), 0) == target).astype(f32).astype(bf16)
    sum_xz = jnp.concatenate([sum_xz, sum_xz], axis=1)

    lane128 = iota((NYL, 128), 1)
    row128 = iota((NYL, 128), 0)
    z_of = lane128 % NZ
    m = [E[M, g, 0:NYL, :] for g in (1, 2)]
    p = [E[PR, g, 0:NYL, :] for g in (1, 2)]
    b = [E[B, g, 0:NYL, :] for g in (1, 2)]
    phi = [E[PHI, g, 0:NYL, :] for g in (1, 2)]
    own_src = [src[0:NYL, 128 * g : 128 * (g + 1)] for g in (1, 2)]
    same_x = [lanes_of([(kx[4 + 4 * g + i] == kx[5 + 4 * g + i]).astype(jnp.int32) for i in range(4)], (1, 128)) for g in (0, 1)]

    def nx_(v, g):
        return next_x(v[0], v[1]) if g == 0 else roll(v[1], -32, 1)

    def ny_(v):
        return roll(v, -1, 0)

    def nz_(v):
        return roll(v, -1, 1)

    tx = [harmonic(m[0], nx_(m, 0)), jnp.where(lane128 < 96, harmonic(m[1], nx_(m, 1)), 0.0)]
    ty = [jnp.where(row128 < NYL - 1, harmonic(v, ny_(v)), 0.0) for v in m]
    tz = [jnp.where(z_of < NZ - 1, 0.1 * harmonic(v, nz_(v)), 0.0) for v in m]
    qx = [tx[g] * (p[g] - nx_(p, g)) for g in (0, 1)]
    sums = []
    for g in (0, 1):
        qy = ty[g] * (p[g] - ny_(p[g]))
        qz = tz[g] * (p[g] - nz_(p[g]))
        in_x = prev_x(qx[g], qx[0]) if g == 1 else jnp.where(lane128 >= 32, roll(qx[0], 32, 1), 0.0)
        t_in_x = prev_x(tx[g], tx[0]) if g == 1 else jnp.where(lane128 >= 32, roll(tx[0], 32, 1), 0.0)
        out = qx[g] - in_x + qy - roll(qy, 1, 0) + qz - roll(qz, 1, 1)
        resid = b[g] * (own_src[g] - out)
        cond = tx[g] + t_in_x + ty[g] + roll(ty[g], 1, 0) + tz[g] + roll(tz[g], 1, 1)
        cx = tx[g] * b[g] * nx_(b, g)
        cy = ty[g] * b[g] * ny_(b[g])
        cz = tz[g] * b[g] * nz_(b[g])
        keep_x = same_x[g].astype(f32)
        keep_z = (z_of % BZ != BZ - 1).astype(f32)
        diag = b[g] * b[g] * (0.5 * phi[g] + cond) - 2.0 * (cx * keep_x + cy * same_y + cz * keep_z)
        sums.append((resid, diag, cz * (1.0 - keep_z), cx * (1.0 - keep_x), cy * (1.0 - same_y)))
    inner = []
    for q in range(5):
        hi, mid = split2(jnp.concatenate([sums[0][q], sums[1][q]], axis=1))
        inner.append(nn(sum_y, jnp.concatenate([hi, mid], axis=0)))

    hi, mid = split2(jnp.concatenate(inner, axis=0))
    partial = nt(jnp.concatenate([hi, mid], axis=1), sum_xz)
    inside = partial[0:ROWS_C]
    for q in range(1, 5):
        inside = inside + roll(partial[ROWS_C * q : ROWS_C * (q + 1)], 24 * q, 1)
    target = (lanes_of(kx[4:12], (1, 256)) + 1) * 8 + z_block
    sum_rows = jnp.concatenate(
        [(iota((128, 256), 0) == target + 24 * q).astype(f32).astype(bf16) for q in (0, 1, 4)] * 2, axis=1
    )

    k_low, k_high, k_next = kx[4], kx[11], kx[12]
    together = k_high == k_next
    for copy in edges:
        copy.wait_recv()

    m0, p0, b0 = [xr[0, NZ * k : NZ * (k + 1)] for k in range(3)]
    m1, p1, b1 = [xr[1, NZ * k : NZ * (k + 1)] for k in range(3)]
    (om0, op0, ob0), (om1, op1, ob1) = own_edge
    t1 = harmonic(om1, m1)
    t0 = harmonic(om0, m0)

    def layers(v):
        return v[0:8] + v[8:16] + v[16:24] + v[24:32]

    r1, d1, c1 = layers(-ob1 * t1 * (op1 - p1)), layers(ob1 * ob1 * t1), layers(ob1 * b1 * t1)
    r0, d0 = layers(-ob0 * t0 * (op0 - p0)), layers(ob0 * ob0 * t0)
    nothing = jnp.zeros((8, 128), f32)
    d1 = d1 - 2.0 * jnp.where(together, c1, nothing)
    c1 = jnp.where(together, nothing, c1)
    placed = []
    for high_part, low_part in ((r1, r0), (d1, d0), (nothing, nothing), (c1, nothing), (nothing, nothing)):
        for k in (-1, 0, 1):
            placed.append(jnp.where(k_high == k, high_part, nothing) + jnp.where(k_low == k, low_part, nothing))
    hi, mid = split2(jnp.concatenate(placed + [nothing], axis=0))
    mine = nt(sum_y, jnp.concatenate([hi, mid], axis=1))

    def wide(ref, side, k):
        return jnp.concatenate([ref[side, 2 * k : 2 * k + 1, :], ref[side, 2 * k + 1 : 2 * k + 2, :]], axis=1)

    um, up_, ub = [wide(yr, 1, k) for k in range(3)]
    dm, dp, db = [wide(yr, 0, k) for k in range(3)]
    om1, op1, ob1 = [wide(ys, 1, k) for k in range(3)]
    om0, op0, ob0 = [wide(ys, 0, k) for k in range(3)]
    t1 = harmonic(om1, um)
    t0 = harmonic(om0, dm)
    rows = iota((ROWS_C, 1), 0)
    r_high = by_row[NYL - 1 : NYL, 0:1].astype(jnp.int32)
    r_low = by_row[0:1, 0:1].astype(jnp.int32)
    r_next = by_up[0:1, 0:1].astype(jnp.int32)
    at_high = rows == r_high
    at_low = rows == r_low
    same = r_high == r_next
    couple = ob1 * ub * t1
    zero = jnp.zeros_like(couple)
    at_top = jnp.concatenate(
        [-ob1 * t1 * (op1 - up_), ob1 * ob1 * t1 - 2.0 * jnp.where(same, couple, zero), jnp.where(same, zero, couple)], axis=1
    )
    at_bottom = jnp.concatenate([-ob0 * t0 * (op0 - dp), ob0 * ob0 * t0, zero], axis=1)
    both = jnp.where(iota((8, 768), 0) == 0, at_top, at_bottom)
    hi, mid = split2(both)
    edge_y = nt(jnp.concatenate([hi, mid], axis=1), sum_rows)
    mine = mine + jnp.where(at_high, edge_y[0:1], 0.0) + jnp.where(at_low, edge_y[1:2], 0.0)
    mine = mine + inside
    ps[REACH] = mine

    def slot(dx):
        return REACH + dx

    coarse = {}
    for dx in range(-REACH, REACH + 1):
        if dx:
            coarse[dx, 0] = to(ps.at[slot(0)], ps.at[slot(-dx)], send_c, recv_c, slot(dx), slot(-dx), dx, 0)
        coarse[dx, 1] = to(
            ps.at[slot(0), 16:24], low.at[slot(-dx)], send_c, recv_c, 9 + slot(dx), 9 + slot(-dx), dx, 1
        )
        coarse[dx, -1] = to(
            ps.at[slot(0), 0:8], high.at[slot(-dx)], send_c, recv_c, 18 + slot(dx), 18 + slot(-dx), dx, -1
        )
    for dx in (-1, -2, -3, -4, 0, 1, 2, 3, 4):
        for dy in (0, -1, 1):
            if (dx, dy) in coarse:
                coarse[dx, dy].start()
    for copy in halo_last:
        copy.start()

    target = (lanes_of(kx, (1, 512)) + 3) * 8 + (iota((1, 512), 1) % NZ) // BZ
    spread_xz = (iota((64, 512), 0) == target).astype(f32).astype(bf16)
    spread_xz = jnp.concatenate([spread_xz] * 2, axis=0)

    for copy in halo_first + halo:
        copy.wait_recv()
    take_up = iota((8, 128), 0) < 4
    for f in range(5):
        for g in range(GROUPS):
            E[f, g, NYL:EXT, :] = jnp.where(take_up, yh[1, f, g], yh[0, f, g])

    z_ext = iota((EXT, 128), 1) % NZ
    for g in range(GROUPS):
        after = min(g + 1, GROUPS - 1)
        here = E[M, g]
        tx_out[g] = harmonic(here, next_x(here, E[M, after]))
        ty_out[g] = harmonic(here, roll(here, -1, 0))
        tz_out[g] = jnp.where(z_ext < NZ - 1, 0.1 * harmonic(here, roll(here, -1, 1)), 0.0)

    def finish(g):
        s_out[g] = E[S, g]
        phi_here = E[PHI, g]
        w_out[g] = time_step / jnp.where(phi_here > 0, phi_here, 1.0)

    finish(1)
    finish(2)

    lane24 = iota((ROWS_C, 128), 1)
    system = [jnp.zeros((ROWS_C, 128), f32) for _ in range(5)]
    for dx in sorted(range(-REACH, REACH + 1), key=abs):
        for dy in (-1, 0, 1):
            if (dx, dy) in coarse:
                coarse[-dx, -dy].wait_recv()
        k = slot(dx)
        part = jnp.concatenate([ps[k, 0:8] + low[k], ps[k, 8:16], ps[k, 16:24] + high[k]], axis=0)
        first = (dx + 2) * 8
        take = (lane24 >= max(first, 0)) & (lane24 < min(first + 24, 56))
        for q in range(2 if abs(dx) == REACH else 5):
            system[q] = system[q] + jnp.where(take, roll(part, first - 24 * q, 1), 0.0)
    resid, diag, cz, cx, cy = system
    diag = jnp.where(diag > 0, diag, 1.0)
    half = 0.5 / diag
    fixed = half * resid
    estimate = fixed
    for _ in range(NSWEEP - 1):
        flow = (
            cz * roll(estimate, -1, 1) + roll(cz * estimate, 1, 1)
            + cx * roll(estimate, -8, 1) + roll(cx * estimate, 8, 1)
            + cy * roll(estimate, -1, 0) + roll(cy * estimate, 1, 0)
        )
        estimate = 0.5 * estimate + fixed + half * flow
    row24 = iota((ROWS_C, 128), 0)
    wanted = (row24 >= 3) & (row24 < 21) & (lane24 >= 16) & (lane24 < 40)
    estimate = jnp.where(wanted, estimate, 0.0)[:, 0:64]
    spread1 = nn(jnp.concatenate(split2(estimate), axis=1), spread_xz)
    fine = nn(jnp.concatenate([spread_y] * 2, axis=1), jnp.concatenate(split2(spread1), axis=0))

    for copy in halo_next:
        copy.wait_recv()
    for g in range(GROUPS):
        newp[g] = E[PR, g] + E[B, g] * fine[:, 128 * g : 128 * (g + 1)]
    for copy in halo_last:
        copy.wait_recv()
    finish(0)
    finish(3)
    for copy in edges + halo + halo_first + halo_next + halo_last + list(coarse.values()):
        copy.wait_send()


def transport_kernel(tx, ty, tz, s_in, w_in, src, newp, np_out, s_out, s, F, C, np_nat, s_nat, sem):
    first, last_row = 8, 8 + EXT - 1
    lane = iota((EXT, 128), 1)

    def to_next(rolled, g):
        return jnp.where(lane < 96, rolled[g], rolled[min(g + 1, GROUPS - 1)])

    def to_prev(rolled, g):
        return jnp.where(lane >= 32, rolled[g], rolled[max(g - 1, 0)])

    def put(block, g, dst):
        back = block.T
        for i in range(4):
            dst[pl.ds(4 * (g - 1) + i, NZ, NXL), :] = back[NZ * i : NZ * (i + 1)]

    for g in (1, 2):
        put(newp[g, 0:NYL, :], g, np_nat)
    np_copy = pltpu.make_async_copy(np_nat, np_out, sem.at[0])
    np_copy.start()

    rolled = [roll(newp[g], -32, 1) for g in range(GROUPS)]
    fx = [tx[g] * (newp[g] - to_next(rolled, g)) for g in range(GROUPS)]
    rolled = [roll(v, 32, 1) for v in fx]
    for g in range(GROUPS):
        here = newp[g]
        w = w_in[g]
        source = src[g]
        fx_up = fx[g]
        fx_down = to_prev(rolled, g)
        fy_up = ty[g] * (here - roll(here, -1, 0))
        fy_down = roll(fy_up, 1, 0)
        fz_up = tz[g] * (here - roll(here, -1, 1))
        fz_down = roll(fz_up, 1, 1)
        C[0, g] = w * jnp.maximum(source, 0.0)
        leaves = jnp.minimum(source, 0.0)
        for k, (up, down) in enumerate(((fx_up, fx_down), (fy_up, fy_down), (fz_up, fz_down))):
            from_up = jnp.maximum(-up, 0.0)
            from_down = jnp.maximum(down, 0.0)
            C[2 + 2 * k, g] = w * from_up
            C[3 + 2 * k, g] = w * from_down
            leaves = leaves - (up + from_up) + (down - from_down)
        C[1, g] = w * leaves

    for step in range(NSUB):
        last = step == NSUB - 1
        for g in range(GROUPS):
            for a in range(0, EXT, CHUNK):
                b = min(a + CHUNK, EXT)
                v = s_in[g, a:b] if step == 0 else s[g, a:b]
                wet = v * v
                F[g, first + a : first + b] = wet / (wet + (1.0 - v) * (1.0 - v) * 0.25)
            F[g, first - 1 : first] = F[g, last_row : last_row + 1]
            F[g, last_row + 1 : last_row + 2] = F[g, first : first + 1]
        end = NYL if last else EXT
        for a in range(0, end, CHUNK):
            b = min(a + CHUNK, end)
            here = [F[g, first + a : first + b] for g in range(GROUPS)]
            mask_next, mask_prev = lane[a:b] < 96, lane[a:b] >= 32
            ups = [None if last and g == 0 else roll(f, -32, 1) for g, f in enumerate(here)]
            downs = [None if last and g == 3 else roll(f, 32, 1) for g, f in enumerate(here)]
            for g in (1, 2) if last else range(GROUPS):
                v = s_in[g, a:b] if step == 0 else s[g, a:b]
                v = v + C[0, g, a:b] + C[1, g, a:b] * here[g]
                v = v + C[4, g, a:b] * F[g, first + a + 1 : first + b + 1]
                v = v + C[5, g, a:b] * F[g, first + a - 1 : first + b - 1]
                v = v + C[2, g, a:b] * jnp.where(mask_next, ups[g], ups[min(g + 1, GROUPS - 1)])
                v = v + C[3, g, a:b] * jnp.where(mask_prev, downs[g], downs[max(g - 1, 0)])
                v = v + C[6, g, a:b] * roll(here[g], -1, 1) + C[7, g, a:b] * roll(here[g], 1, 1)
                s[g, a:b] = v
    for g in (1, 2):
        put(s[g, 0:NYL, :], g, s_nat)
    s_copy = pltpu.make_async_copy(s_nat, s_out, sem.at[1])
    s_copy.start()
    np_copy.wait()
    s_copy.wait()


def solution(mesh):
    n_gx, n_gy = mesh.shape["gx"], mesh.shape["gy"]
    vmem = pl.BlockSpec(memory_space=pltpu.VMEM)
    anywhere = pl.BlockSpec(memory_space=pltpu.HBM)

    def body(perm, facies, fpor, fmob, pressure, saturation, basis, bx_map, by_map, well_cells, well_rates):
        assert pressure.shape == (NZ, NXL, NYL)
        flat = [a.reshape(NZ * NXL, NYL) for a in (perm, facies, pressure, saturation, basis)]
        sizes = (n_gx, n_gy, by_map.shape[0])
        wide = pltpu.VMEM((GROUPS, EXT, 128), f32)
        cells_in = lambda kind=f32: pltpu.VMEM((NZ * NXL, NYL), kind)
        natural = [cells_in(), cells_in(jnp.int32), cells_in(), cells_in(), cells_in()]
        facies_tables = [pltpu.SMEM(fpor.shape, f32), pltpu.SMEM(fmob.shape, f32)]
        in_vmem = lambda v: pltpu.with_memory_space_constraint(v, pltpu.VMEM)
        in_hbm = lambda v: pltpu.with_memory_space_constraint(v, pltpu.HBM)
        edge = pltpu.VMEM((2, 3 * NZ, NYL), f32)
        results = pl.pallas_call(
            lambda *refs: comm_kernel(sizes, *refs),
            name="exchange",
            out_shape=[wide] * 7,
            in_specs=[anywhere] * 11,
            out_specs=[vmem] * 7,
            scratch_shapes=natural + [
                pltpu.VMEM((n_gy, NYL), jnp.int32),
                pltpu.VMEM((1, well_cells.shape[0]), jnp.int32),
                pltpu.VMEM((1, well_cells.shape[0]), f32),
                pltpu.SMEM(bx_map.shape, jnp.int32),
            ] + facies_tables + [
                pltpu.SemaphoreType.DMA((11,)),
                cells_in(), cells_in(),
                pltpu.VMEM((5, GROUPS, EXT, 128), f32),
                pltpu.VMEM((2, 5, GROUPS, 8, 128), f32),
                edge, edge,
                pltpu.VMEM((2, 8, 128), f32),
                pltpu.VMEM((2, 8, 128), f32),
                pltpu.VMEM((2 * REACH + 1, ROWS_C, 128), f32),
                pltpu.VMEM((2 * REACH + 1, 8, 128), f32),
                pltpu.VMEM((2 * REACH + 1, 8, 128), f32),
                pltpu.SemaphoreType.DMA((4,)),
                pltpu.SemaphoreType.DMA((4,)),
                pltpu.SemaphoreType.DMA((12,)),
                pltpu.SemaphoreType.DMA((12,)),
                pltpu.SemaphoreType.DMA((27,)),
                pltpu.SemaphoreType.DMA((27,)),
            ],
            compiler_params=pltpu.CompilerParams(collective_id=0, has_side_effects=True, vmem_limit_bytes=32 << 20),
        )(
            *[in_hbm(v) for v in (
                *flat, by_map.reshape(n_gy, NYL), well_cells.reshape(1, -1), well_rates.reshape(1, -1), bx_map, fpor, fmob
            )]
        )
        shape = jax.ShapeDtypeStruct((NZ * NXL, NYL), f32)
        new_pressure, water = pl.pallas_call(
            transport_kernel,
            name="transport",
            out_shape=[shape, shape],
            in_specs=[vmem] * 7,
            out_specs=[anywhere] * 2,
            scratch_shapes=[
                pltpu.VMEM((GROUPS, EXT, 128), f32),
                pltpu.VMEM((GROUPS, EXT + 16, 128), f32),
                pltpu.VMEM((8, GROUPS, EXT, 128), f32),
                cells_in(), cells_in(),
                pltpu.SemaphoreType.DMA((2,)),
            ],
            compiler_params=pltpu.CompilerParams(vmem_limit_bytes=32 << 20),
        )(*[in_vmem(v) for v in results])
        return new_pressure.reshape(pressure.shape), water.reshape(pressure.shape)

    cells = P("member", "gx", "gy")
    return jax.shard_map(
        body,
        mesh=mesh,
        in_specs=(cells, cells, P(), P(), cells, cells, cells, P("member"), P("member"), P("member"), P("member")),
        out_specs=(cells, cells),
        check_vma=False,
    )
```

```python
import jax
import jax.numpy as jnp
from jax import lax
from jax.experimental import pallas as pl
from jax.experimental.pallas import tpu as pltpu
from jax.sharding import PartitionSpec as P

NZ = 32
BX = 8
BY = 8
BZ = 4
NSWEEP = 3
NSUB = 4
NFAC = 4
NXL = 8
NYL = 128
EXT = NYL + 8
GROUPS = 4
ROWS_C = 24
REACH = 4
CHUNK = 16

time_step = 0.005
f32 = jnp.float32
bf16 = jnp.bfloat16
M, PR, B, PHI, S = range(5)


def iota(shape, dim):
    return lax.broadcasted_iota(jnp.int32, shape, dim)


def harmonic(left, right):
    total = left + right
    return 2.0 * left * right / jnp.where(total > 0, total, 1.0)


def split2(v):
    hi = v.astype(bf16)
    return hi, (v - hi.astype(f32)).astype(bf16)


def split3(v):
    hi = v.astype(bf16)
    rest = v - hi.astype(f32)
    mid = rest.astype(bf16)
    return hi, mid, (rest - mid.astype(f32)).astype(bf16)


def nn(a, b):
    return lax.dot_general(a, b, (((1,), (0,)), ((), ())), preferred_element_type=f32)


def nt(a, b):
    return lax.dot_general(a, b, (((1,), (1,)), ((), ())), preferred_element_type=f32)


def roll(v, shift, axis):
    return pltpu.roll(v, shift % v.shape[axis], axis)


def next_x(here, after):
    lane = iota(here.shape, 1)
    return jnp.where(lane < 96, roll(here, -32, 1), roll(after, -32, 1))


def prev_x(here, before):
    lane = iota(here.shape, 1)
    return jnp.where(lane >= 32, roll(here, 32, 1), roll(before, 32, 1))


def fetch_properties(perm, fac, sat, fpor, fmob, mob, por):
    region = fac[...]
    s_nat = sat[...]
    fm = jnp.zeros(region.shape, f32)
    fp = jnp.zeros(region.shape, f32)
    for level in range(NFAC):
        fm = jnp.where(region == level, fmob[level], fm)
        fp = jnp.where(region == level, fpor[level], fp)
    mob[...] = perm[...] * fm * (s_nat * s_nat + (1.0 - s_nat) * (1.0 - s_nat) * 0.25)
    por[...] = fp


def turned(ref, g):
    block = jnp.concatenate([ref[pl.ds(4 * (g - 1) + i, NZ, NXL), :] for i in range(4)], axis=0)
    return block.T


def edge_rows(ref, x):
    return jnp.concatenate([ref[pl.ds(x + NXL * i, NZ // BZ, NXL * BZ), :] for i in range(BZ)], axis=0)


class Copy:
    def __init__(self, src, dst, send, recv, target, goes, comes):
        self.goes, self.comes = goes, comes
        self.copy = pltpu.make_async_remote_copy(
            src_ref=src, dst_ref=dst, send_sem=send, recv_sem=recv, device_id=target, device_id_type=pl.DeviceIdType.MESH
        )

    def start(self):
        pl.when(self.goes)(lambda: self.copy.start())

    def wait_send(self):
        pl.when(self.goes)(lambda: self.copy.wait_send())

    def wait_recv(self):
        pl.when(self.comes)(lambda: self.copy.wait_recv())


def comm_kernel(
    sizes,
    perm_h, fac_h, pres_h, sat_h, bas_h, bymap_h, wells_h, rates_h, bxmap_h, fpor_h, fmob_h,
    tx_out, ty_out, tz_out, s_out, w_out, src_out, newp,
    perm, fac, pres, sat, bas, bymap, wells, rates, bxmap, fpor, fmob, in_sem,
    mob, por, E, yh, xs, xr, ys, yr, ps, low, high,
    send_a, recv_a, send_h, recv_h, send_c, recv_c,
):
    n_gx, n_gy, full_y = sizes
    gx = lax.axis_index("gx")
    gy = lax.axis_index("gy")

    def there(dx, dy):
        ok = jnp.bool_(True)
        if dx:
            ok = ok & (gx + dx >= 0) & (gx + dx < n_gx)
        if dy:
            ok = ok & (gy + dy >= 0) & (gy + dy < n_gy)
        return ok

    def where_is(dx, dy):
        return {"gx": gx + dx, "gy": gy + dy}

    partners = [(dx, dy) for dx in range(-REACH, REACH + 1) for dy in (-1, 0, 1) if (dx, dy) != (0, 0)]
    partners.sort(key=lambda d: -abs(d[0]) - abs(d[1]))

    inputs = [
        pltpu.make_async_copy(src, dst, in_sem.at[i])
        for i, (src, dst) in enumerate(zip(
            (sat_h, fac_h, perm_h, fpor_h, fmob_h, pres_h, bas_h, bxmap_h, bymap_h, wells_h, rates_h),
            (sat, fac, perm, fpor, fmob, pres, bas, bxmap, bymap, wells, rates),
        ))
    ]
    for copy in inputs:
        copy.start()

    barrier = pltpu.get_barrier_semaphore()
    for dx, dy in partners:
        @pl.when(there(dx, dy))
        def _(dx=dx, dy=dy):
            pl.semaphore_signal(barrier, inc=1, device_id=where_is(dx, dy), device_id_type=pl.DeviceIdType.MESH)

    for copy in inputs[:5]:
        copy.wait()
    fetch_properties(perm, fac, sat, fpor, fmob, mob, por)
    for copy in inputs[5:7]:
        copy.wait()

    def turn(pairs):
        for f, ref in pairs:
            for g in (1, 2):
                E[f, g, 0:NYL, :] = turned(ref, g)

    turn(((M, mob), (PR, pres), (B, bas)))
    ys[...] = jnp.zeros_like(ys)
    for side, y in ((0, 0), (1, NYL - 1)):
        for k, f in enumerate((M, PR, B)):
            for g in (1, 2):
                ys[side, 2 * k + g - 1 : 2 * k + g, :] = E[f, g, y : y + 1, :]
    own_edge = []
    for x in (0, NXL - 1):
        own_edge.append([edge_rows(ref, x) for ref in (mob, pres, bas)])
    for side in (0, 1):
        for k in range(3):
            xs[side, NZ * k : NZ * (k + 1)] = own_edge[side][k]

    span_x = lax.min(gx, REACH) + lax.min(n_gx - 1 - gx, REACH) + 1
    span_y = lax.min(gy, 1) + lax.min(n_gy - 1 - gy, 1) + 1
    pl.semaphore_wait(barrier, span_x * span_y - 1)

    def to(src, dst, sends, recvs, slot_out, slot_in, dx, dy):
        return Copy(src, dst, sends.at[slot_out], recvs.at[slot_in], where_is(dx, dy), there(dx, dy), there(-dx, -dy))

    edges = [
        to(ys.at[0], yr.at[1], send_a, recv_a, 3, 3, 0, -1),
        to(xs.at[0], xr.at[1], send_a, recv_a, 1, 1, -1, 0),
        to(ys.at[1], yr.at[0], send_a, recv_a, 2, 2, 0, 1),
        to(xs.at[1], xr.at[0], send_a, recv_a, 0, 0, 1, 0),
    ]
    for copy in edges:
        copy.start()

    up, down = slice(NYL - 8, NYL), slice(0, 8)
    every = slice(0, 5)
    halo = [
        to(E.at[every, 1:3, up], yh.at[0, every, 1:3], send_h, recv_h, 4, 4, 0, 1),
        to(E.at[every, 1:3, down], yh.at[1, every, 1:3], send_h, recv_h, 5, 5, 0, -1),
        to(E.at[every, 2, up], yh.at[0, every, 0], send_h, recv_h, 6, 6, 1, 1),
        to(E.at[every, 1, up], yh.at[0, every, 3], send_h, recv_h, 7, 7, -1, 1),
        to(E.at[every, 2, down], yh.at[1, every, 0], send_h, recv_h, 8, 8, 1, -1),
        to(E.at[every, 1, down], yh.at[1, every, 3], send_h, recv_h, 9, 9, -1, -1),
    ]

    def halo_x(k, fields):
        return [
            to(E.at[fields, 2, 0:NYL], E.at[fields, 0, 0:NYL], send_h, recv_h, 2 * k, 2 * k, 1, 0),
            to(E.at[fields, 1, 0:NYL], E.at[fields, 3, 0:NYL], send_h, recv_h, 2 * k + 1, 2 * k + 1, -1, 0),
        ]

    halo_first = halo_x(0, slice(M, M + 1))
    halo_next = halo_x(1, slice(PR, B + 1))
    halo_last = halo_x(5, slice(PHI, S + 1))
    for copy in halo_first + halo_next:
        copy.start()
    turn(((S, sat), (PHI, por)))
    for copy in halo:
        copy.start()
    for copy in inputs[7:]:
        copy.wait()

    def clear_if(missing, *parts):
        @pl.when(missing)
        def _():
            for ref, where in parts:
                ref[where] = jnp.zeros(ref.at[where].shape, f32)

    whole = slice(None)
    clear_if(gx == 0, (xr, 0), (E, (whole, 0)), (yh, (whole, whole, 0)))
    clear_if(gx == n_gx - 1, (xr, 1), (E, (whole, 3)), (yh, (whole, whole, 3)))
    clear_if(gy == 0, (yr, 0), (yh, 0), (low, whole))
    clear_if(gy == n_gy - 1, (yr, 1), (yh, 1), (high, whole))
    for dx in range(1, REACH + 1):
        for k, missing in ((REACH - dx, gx - dx < 0), (REACH + dx, gx + dx >= n_gx)):
            clear_if(missing, (ps, k), (low, k), (high, k))

    well_y = wells[...] % full_y
    well_x = wells[...] // full_y
    n_wells = wells.shape[1]
    row = iota((EXT, 1), 0)
    y_here = gy * NYL + jnp.where(row < NYL + 4, row, row - EXT)
    hits_y = (y_here == well_y).astype(f32).astype(bf16)
    x_here = gx * NXL - 4 + iota((16, 1), 0)
    hits_x = jnp.where(x_here == well_x, rates[...], 0.0)
    col = nt(hits_y, jnp.concatenate(split3(hits_x), axis=0))
    col = (col[:, 0:16] + col[:, 16:32] + col[:, 32:48]) * (1.0 / NZ)
    lane = iota((16, 512), 1)
    spread = (lane // NZ == iota((16, 512), 0)).astype(f32).astype(bf16)
    src = nn(jnp.concatenate(split3(col), axis=1), jnp.concatenate([spread] * 3, axis=0))
    for g in range(GROUPS):
        src_out[g] = src[:, 128 * g : 128 * (g + 1)]

    blocks_y = NYL // BY
    map_own = bymap[pl.ds(gy, 1), :] - (gy * blocks_y - 4)
    map_up = bymap[pl.ds(lax.min(gy + 1, n_gy - 1), 1), :] - (gy * blocks_y - 4)
    map_down = bymap[pl.ds(lax.max(gy - 1, 0), 1), :] - (gy * blocks_y - 4)
    sum_y = (iota((ROWS_C, NYL), 0) == map_own).astype(f32).astype(bf16)
    sum_y = jnp.concatenate([sum_y, sum_y], axis=1)

    def column_of(values):
        return jnp.broadcast_to(values.astype(f32), (128, 128)).T

    by_row = column_of(map_own)
    by_up = column_of(map_up)[0:8]
    by_down = column_of(map_down)[120:128]
    by_ext = jnp.concatenate([by_row, jnp.where(iota((8, 128), 0) < 4, by_up, by_down)], axis=0)
    spread_y = (by_ext[:, 0:ROWS_C] == iota((EXT, ROWS_C), 1).astype(f32)).astype(f32).astype(bf16)
    same_y = (by_row == jnp.concatenate([by_row[1:], by_row[:1]], axis=0)).astype(f32)

    kx = [bxmap[lax.clamp(0, gx * NXL - 4 + i, n_gx * NXL - 1)] - gx for i in range(16)]

    def lanes_of(values, shape):
        which = iota(shape, 1) // NZ
        total = jnp.zeros(shape, jnp.int32)
        for i, value in enumerate(values):
            total = jnp.where(which == i, value, total)
        return total

    z_block = (iota((1, 256), 1) % NZ) // BZ
    target = (lanes_of(kx[4:12], (1, 256)) + 1) * 8 + z_block
    sum_xz = (iota((128, 256), 0) == target).astype(f32).astype(bf16)
    sum_xz = jnp.concatenate([sum_xz, sum_xz], axis=1)

    lane128 = iota((NYL, 128), 1)
    row128 = iota((NYL, 128), 0)
    z_of = lane128 % NZ
    m = [E[M, g, 0:NYL, :] for g in (1, 2)]
    p = [E[PR, g, 0:NYL, :] for g in (1, 2)]
    b = [E[B, g, 0:NYL, :] for g in (1, 2)]
    phi = [E[PHI, g, 0:NYL, :] for g in (1, 2)]
    own_src = [src[0:NYL, 128 * g : 128 * (g + 1)] for g in (1, 2)]
    same_x = [lanes_of([(kx[4 + 4 * g + i] == kx[5 + 4 * g + i]).astype(jnp.int32) for i in range(4)], (1, 128)) for g in (0, 1)]

    def nx_(v, g):
        return next_x(v[0], v[1]) if g == 0 else roll(v[1], -32, 1)

    def ny_(v):
        return roll(v, -1, 0)

    def nz_(v):
        return roll(v, -1, 1)

    tx = [harmonic(m[0], nx_(m, 0)), jnp.where(lane128 < 96, harmonic(m[1], nx_(m, 1)), 0.0)]
    ty = [jnp.where(row128 < NYL - 1, harmonic(v, ny_(v)), 0.0) for v in m]
    tz = [jnp.where(z_of < NZ - 1, 0.1 * harmonic(v, nz_(v)), 0.0) for v in m]
    qx = [tx[g] * (p[g] - nx_(p, g)) for g in (0, 1)]
    sums = []
    for g in (0, 1):
        qy = ty[g] * (p[g] - ny_(p[g]))
        qz = tz[g] * (p[g] - nz_(p[g]))
        in_x = prev_x(qx[g], qx[0]) if g == 1 else jnp.where(lane128 >= 32, roll(qx[0], 32, 1), 0.0)
        t_in_x = prev_x(tx[g], tx[0]) if g == 1 else jnp.where(lane128 >= 32, roll(tx[0], 32, 1), 0.0)
        out = qx[g] - in_x + qy - roll(qy, 1, 0) + qz - roll(qz, 1, 1)
        resid = b[g] * (own_src[g] - out)
        cond = tx[g] + t_in_x + ty[g] + roll(ty[g], 1, 0) + tz[g] + roll(tz[g], 1, 1)
        cx = tx[g] * b[g] * nx_(b, g)
        cy = ty[g] * b[g] * ny_(b[g])
        cz = tz[g] * b[g] * nz_(b[g])
        keep_x = same_x[g].astype(f32)
        keep_z = (z_of % BZ != BZ - 1).astype(f32)
        diag = b[g] * b[g] * (0.5 * phi[g] + cond) - 2.0 * (cx * keep_x + cy * same_y + cz * keep_z)
        sums.append((resid, diag, cz * (1.0 - keep_z), cx * (1.0 - keep_x), cy * (1.0 - same_y)))
    inner = []
    for q in range(5):
        hi, mid = split2(jnp.concatenate([sums[0][q], sums[1][q]], axis=1))
        inner.append(nn(sum_y, jnp.concatenate([hi, mid], axis=0)))

    hi, mid = split2(jnp.concatenate(inner, axis=0))
    partial = nt(jnp.concatenate([hi, mid], axis=1), sum_xz)
    inside = partial[0:ROWS_C]
    for q in range(1, 5):
        inside = inside + roll(partial[ROWS_C * q : ROWS_C * (q + 1)], 24 * q, 1)
    target = (lanes_of(kx[4:12], (1, 256)) + 1) * 8 + z_block
    sum_rows = jnp.concatenate(
        [(iota((128, 256), 0) == target + 24 * q).astype(f32).astype(bf16) for q in (0, 1, 4)] * 2, axis=1
    )

    k_low, k_high, k_next = kx[4], kx[11], kx[12]
    together = k_high == k_next
    for copy in edges:
        copy.wait_recv()

    m0, p0, b0 = [xr[0, NZ * k : NZ * (k + 1)] for k in range(3)]
    m1, p1, b1 = [xr[1, NZ * k : NZ * (k + 1)] for k in range(3)]
    (om0, op0, ob0), (om1, op1, ob1) = own_edge
    t1 = harmonic(om1, m1)
    t0 = harmonic(om0, m0)

    def layers(v):
        return v[0:8] + v[8:16] + v[16:24] + v[24:32]

    r1, d1, c1 = layers(-ob1 * t1 * (op1 - p1)), layers(ob1 * ob1 * t1), layers(ob1 * b1 * t1)
    r0, d0 = layers(-ob0 * t0 * (op0 - p0)), layers(ob0 * ob0 * t0)
    nothing = jnp.zeros((8, 128), f32)
    d1 = d1 - 2.0 * jnp.where(together, c1, nothing)
    c1 = jnp.where(together, nothing, c1)
    placed = []
    for high_part, low_part in ((r1, r0), (d1, d0), (nothing, nothing), (c1, nothing), (nothing, nothing)):
        for k in (-1, 0, 1):
            placed.append(jnp.where(k_high == k, high_part, nothing) + jnp.where(k_low == k, low_part, nothing))
    hi, mid = split2(jnp.concatenate(placed + [nothing], axis=0))
    mine = nt(sum_y, jnp.concatenate([hi, mid], axis=1))

    def wide(ref, side, k):
        return jnp.concatenate([ref[side, 2 * k : 2 * k + 1, :], ref[side, 2 * k + 1 : 2 * k + 2, :]], axis=1)

    um, up_, ub = [wide(yr, 1, k) for k in range(3)]
    dm, dp, db = [wide(yr, 0, k) for k in range(3)]
    om1, op1, ob1 = [wide(ys, 1, k) for k in range(3)]
    om0, op0, ob0 = [wide(ys, 0, k) for k in range(3)]
    t1 = harmonic(om1, um)
    t0 = harmonic(om0, dm)
    rows = iota((ROWS_C, 1), 0)
    r_high = by_row[NYL - 1 : NYL, 0:1].astype(jnp.int32)
    r_low = by_row[0:1, 0:1].astype(jnp.int32)
    r_next = by_up[0:1, 0:1].astype(jnp.int32)
    at_high = rows == r_high
    at_low = rows == r_low
    same = r_high == r_next
    couple = ob1 * ub * t1
    zero = jnp.zeros_like(couple)
    at_top = jnp.concatenate(
        [-ob1 * t1 * (op1 - up_), ob1 * ob1 * t1 - 2.0 * jnp.where(same, couple, zero), jnp.where(same, zero, couple)], axis=1
    )
    at_bottom = jnp.concatenate([-ob0 * t0 * (op0 - dp), ob0 * ob0 * t0, zero], axis=1)
    both = jnp.where(iota((8, 768), 0) == 0, at_top, at_bottom)
    hi, mid = split2(both)
    edge_y = nt(jnp.concatenate([hi, mid], axis=1), sum_rows)
    mine = mine + jnp.where(at_high, edge_y[0:1], 0.0) + jnp.where(at_low, edge_y[1:2], 0.0)
    mine = mine + inside
    ps[REACH] = mine

    def slot(dx):
        return REACH + dx

    coarse = {}
    for dx in range(-REACH, REACH + 1):
        if dx:
            coarse[dx, 0] = to(ps.at[slot(0)], ps.at[slot(-dx)], send_c, recv_c, slot(dx), slot(-dx), dx, 0)
        coarse[dx, 1] = to(
            ps.at[slot(0), 16:24], low.at[slot(-dx)], send_c, recv_c, 9 + slot(dx), 9 + slot(-dx), dx, 1
        )
        coarse[dx, -1] = to(
            ps.at[slot(0), 0:8], high.at[slot(-dx)], send_c, recv_c, 18 + slot(dx), 18 + slot(-dx), dx, -1
        )
    for dx in (-3, -2, -4, -1, 0, 1, 2, 3, 4):
        for dy in (-1, 0, 1):
            if (dx, dy) in coarse:
                coarse[dx, dy].start()
    for copy in halo_last:
        copy.start()

    target = (lanes_of(kx, (1, 512)) + 3) * 8 + (iota((1, 512), 1) % NZ) // BZ
    spread_xz = (iota((64, 512), 0) == target).astype(f32).astype(bf16)
    spread_xz = jnp.concatenate([spread_xz] * 2, axis=0)

    for copy in halo_first + halo:
        copy.wait_recv()
    take_up = iota((8, 128), 0) < 4
    for f in range(5):
        for g in range(GROUPS):
            E[f, g, NYL:EXT, :] = jnp.where(take_up, yh[1, f, g], yh[0, f, g])

    z_ext = iota((EXT, 128), 1) % NZ
    for g in range(GROUPS):
        after = min(g + 1, GROUPS - 1)
        here = E[M, g]
        tx_out[g] = harmonic(here, next_x(here, E[M, after]))
        ty_out[g] = harmonic(here, roll(here, -1, 0))
        tz_out[g] = jnp.where(z_ext < NZ - 1, 0.1 * harmonic(here, roll(here, -1, 1)), 0.0)

    def finish(g):
        s_out[g] = E[S, g]
        phi_here = E[PHI, g]
        w_out[g] = time_step / jnp.where(phi_here > 0, phi_here, 1.0)

    finish(1)
    finish(2)

    lane24 = iota((ROWS_C, 128), 1)
    system = [jnp.zeros((ROWS_C, 128), f32) for _ in range(5)]
    for group in ((0, -1, 1), (-2, 2), (-3, 3, -4, 4)):
        for dx in group:
            for dy in (-1, 0, 1):
                if (dx, dy) in coarse:
                    coarse[-dx, -dy].wait_recv()
        for dx in group:
            k = slot(dx)
            part = jnp.concatenate([ps[k, 0:8] + low[k], ps[k, 8:16], ps[k, 16:24] + high[k]], axis=0)
            first = (dx + 2) * 8
            take = (lane24 >= max(first, 0)) & (lane24 < min(first + 24, 56))
            for q in range(2 if abs(dx) == REACH else 5):
                system[q] = system[q] + jnp.where(take, roll(part, first - 24 * q, 1), 0.0)
    resid, diag, cz, cx, cy = system
    diag = jnp.where(diag > 0, diag, 1.0)
    half = 0.5 / diag
    fixed = half * resid
    estimate = fixed
    for _ in range(NSWEEP - 1):
        flow = (
            cz * roll(estimate, -1, 1) + roll(cz * estimate, 1, 1)
            + cx * roll(estimate, -8, 1) + roll(cx * estimate, 8, 1)
            + cy * roll(estimate, -1, 0) + roll(cy * estimate, 1, 0)
        )
        estimate = 0.5 * estimate + fixed + half * flow
    row24 = iota((ROWS_C, 128), 0)
    wanted = (row24 >= 3) & (row24 < 21) & (lane24 >= 16) & (lane24 < 40)
    estimate = jnp.where(wanted, estimate, 0.0)[:, 0:64]
    spread1 = nn(jnp.concatenate(split2(estimate), axis=1), spread_xz)
    fine = nn(jnp.concatenate([spread_y] * 2, axis=1), jnp.concatenate(split2(spread1), axis=0))

    for copy in halo_next:
        copy.wait_recv()
    for g in range(GROUPS):
        newp[g] = E[PR, g] + E[B, g] * fine[:, 128 * g : 128 * (g + 1)]
    for copy in halo_last:
        copy.wait_recv()
    finish(0)
    finish(3)
    for copy in edges + halo + halo_first + halo_next + halo_last + list(coarse.values()):
        copy.wait_send()


def transport_kernel(tx, ty, tz, s_in, w_in, src, newp, np_out, s_out, s, F, C, np_nat, s_nat, sem):
    first, last_row = 8, 8 + EXT - 1
    lane = iota((EXT, 128), 1)

    def to_next(rolled, g):
        return jnp.where(lane < 96, rolled[g], rolled[min(g + 1, GROUPS - 1)])

    def to_prev(rolled, g):
        return jnp.where(lane >= 32, rolled[g], rolled[max(g - 1, 0)])

    def put(block, g, dst):
        back = block.T
        for i in range(4):
            dst[pl.ds(4 * (g - 1) + i, NZ, NXL), :] = back[NZ * i : NZ * (i + 1)]

    for g in (1, 2):
        put(newp[g, 0:NYL, :], g, np_nat)
    np_copy = pltpu.make_async_copy(np_nat, np_out, sem.at[0])
    np_copy.start()

    rolled = [roll(newp[g], -32, 1) for g in range(GROUPS)]
    fx = [tx[g] * (newp[g] - to_next(rolled, g)) for g in range(GROUPS)]
    rolled = [roll(v, 32, 1) for v in fx]
    for g in range(GROUPS):
        here = newp[g]
        w = w_in[g]
        source = src[g]
        fx_up = fx[g]
        fx_down = to_prev(rolled, g)
        fy_up = ty[g] * (here - roll(here, -1, 0))
        fy_down = roll(fy_up, 1, 0)
        fz_up = tz[g] * (here - roll(here, -1, 1))
        fz_down = roll(fz_up, 1, 1)
        C[0, g] = w * jnp.maximum(source, 0.0)
        leaves = jnp.minimum(source, 0.0)
        for k, (up, down) in enumerate(((fx_up, fx_down), (fy_up, fy_down), (fz_up, fz_down))):
            from_up = jnp.maximum(-up, 0.0)
            from_down = jnp.maximum(down, 0.0)
            C[2 + 2 * k, g] = w * from_up
            C[3 + 2 * k, g] = w * from_down
            leaves = leaves - (up + from_up) + (down - from_down)
        C[1, g] = w * leaves

    for step in range(NSUB):
        last = step == NSUB - 1
        for g in range(GROUPS):
            for a in range(0, EXT, CHUNK):
                b = min(a + CHUNK, EXT)
                v = s_in[g, a:b] if step == 0 else s[g, a:b]
                wet = v * v
                F[g, first + a : first + b] = wet / (wet + (1.0 - v) * (1.0 - v) * 0.25)
            F[g, first - 1 : first] = F[g, last_row : last_row + 1]
            F[g, last_row + 1 : last_row + 2] = F[g, first : first + 1]
        end = NYL if last else EXT
        for a in range(0, end, CHUNK):
            b = min(a + CHUNK, end)
            here = [F[g, first + a : first + b] for g in range(GROUPS)]
            mask_next, mask_prev = lane[a:b] < 96, lane[a:b] >= 32
            ups = [None if last and g == 0 else roll(f, -32, 1) for g, f in enumerate(here)]
            downs = [None if last and g == 3 else roll(f, 32, 1) for g, f in enumerate(here)]
            for g in (1, 2) if last else range(GROUPS):
                v = s_in[g, a:b] if step == 0 else s[g, a:b]
                v = v + C[0, g, a:b] + C[1, g, a:b] * here[g]
                v = v + C[4, g, a:b] * F[g, first + a + 1 : first + b + 1]
                v = v + C[5, g, a:b] * F[g, first + a - 1 : first + b - 1]
                v = v + C[2, g, a:b] * jnp.where(mask_next, ups[g], ups[min(g + 1, GROUPS - 1)])
                v = v + C[3, g, a:b] * jnp.where(mask_prev, downs[g], downs[max(g - 1, 0)])
                v = v + C[6, g, a:b] * roll(here[g], -1, 1) + C[7, g, a:b] * roll(here[g], 1, 1)
                s[g, a:b] = v
    for g in (1, 2):
        put(s[g, 0:NYL, :], g, s_nat)
    s_copy = pltpu.make_async_copy(s_nat, s_out, sem.at[1])
    s_copy.start()
    np_copy.wait()
    s_copy.wait()


def solution(mesh):
    n_gx, n_gy = mesh.shape["gx"], mesh.shape["gy"]
    vmem = pl.BlockSpec(memory_space=pltpu.VMEM)
    anywhere = pl.BlockSpec(memory_space=pltpu.HBM)

    def body(perm, facies, fpor, fmob, pressure, saturation, basis, bx_map, by_map, well_cells, well_rates):
        assert pressure.shape == (NZ, NXL, NYL)
        flat = [a.reshape(NZ * NXL, NYL) for a in (perm, facies, pressure, saturation, basis)]
        sizes = (n_gx, n_gy, by_map.shape[0])
        wide = pltpu.VMEM((GROUPS, EXT, 128), f32)
        cells_in = lambda kind=f32: pltpu.VMEM((NZ * NXL, NYL), kind)
        natural = [cells_in(), cells_in(jnp.int32), cells_in(), cells_in(), cells_in()]
        facies_tables = [pltpu.SMEM(fpor.shape, f32), pltpu.SMEM(fmob.shape, f32)]
        in_vmem = lambda v: pltpu.with_memory_space_constraint(v, pltpu.VMEM)
        in_hbm = lambda v: pltpu.with_memory_space_constraint(v, pltpu.HBM)
        edge = pltpu.VMEM((2, 3 * NZ, NYL), f32)
        results = pl.pallas_call(
            lambda *refs: comm_kernel(sizes, *refs),
            name="exchange",
            out_shape=[wide] * 7,
            in_specs=[anywhere] * 11,
            out_specs=[vmem] * 7,
            scratch_shapes=natural + [
                pltpu.VMEM((n_gy, NYL), jnp.int32),
                pltpu.VMEM((1, well_cells.shape[0]), jnp.int32),
                pltpu.VMEM((1, well_cells.shape[0]), f32),
                pltpu.SMEM(bx_map.shape, jnp.int32),
            ] + facies_tables + [
                pltpu.SemaphoreType.DMA((11,)),
                cells_in(), cells_in(),
                pltpu.VMEM((5, GROUPS, EXT, 128), f32),
                pltpu.VMEM((2, 5, GROUPS, 8, 128), f32),
                edge, edge,
                pltpu.VMEM((2, 8, 128), f32),
                pltpu.VMEM((2, 8, 128), f32),
                pltpu.VMEM((2 * REACH + 1, ROWS_C, 128), f32),
                pltpu.VMEM((2 * REACH + 1, 8, 128), f32),
                pltpu.VMEM((2 * REACH + 1, 8, 128), f32),
                pltpu.SemaphoreType.DMA((4,)),
                pltpu.SemaphoreType.DMA((4,)),
                pltpu.SemaphoreType.DMA((12,)),
                pltpu.SemaphoreType.DMA((12,)),
                pltpu.SemaphoreType.DMA((27,)),
                pltpu.SemaphoreType.DMA((27,)),
            ],
            compiler_params=pltpu.CompilerParams(collective_id=0, has_side_effects=True, vmem_limit_bytes=32 << 20),
        )(
            *[in_hbm(v) for v in (
                *flat, by_map.reshape(n_gy, NYL), well_cells.reshape(1, -1), well_rates.reshape(1, -1), bx_map, fpor, fmob
            )]
        )
        shape = jax.ShapeDtypeStruct((NZ * NXL, NYL), f32)
        new_pressure, water = pl.pallas_call(
            transport_kernel,
            name="transport",
            out_shape=[shape, shape],
            in_specs=[vmem] * 7,
            out_specs=[anywhere] * 2,
            scratch_shapes=[
                pltpu.VMEM((GROUPS, EXT, 128), f32),
                pltpu.VMEM((GROUPS, EXT + 16, 128), f32),
                pltpu.VMEM((8, GROUPS, EXT, 128), f32),
                cells_in(), cells_in(),
                pltpu.SemaphoreType.DMA((2,)),
            ],
            compiler_params=pltpu.CompilerParams(vmem_limit_bytes=32 << 20),
        )(*[in_vmem(v) for v in results])
        return new_pressure.reshape(pressure.shape), water.reshape(pressure.shape)

    cells = P("member", "gx", "gy")
    return jax.shard_map(
        body,
        mesh=mesh,
        in_specs=(cells, cells, P(), P(), cells, cells, cells, P("member"), P("member"), P("member"), P("member")),
        out_specs=(cells, cells),
        check_vma=False,
    )
```
